128 devices in a mesh: rep: 2 (over core), dp: 64 (over x, y, z).
Axes of the slice: x: 4, y: 4, z: 4, core: 2. Of those that a mesh axis runs over, the one named last changes fastest.
Arguments:
- x: bfloat16 [128, 1024, 1280], P(('rep', 'dp')), parts along dimension 0
- dy: bfloat16 [128, 1024, 1280], P(('rep', 'dp')), parts along dimension 0
- w_gate: bfloat16 [2, 1280, 4096], replicated
- w_up: bfloat16 [2, 1280, 4096], replicated
- w_down: bfloat16 [2, 4096, 1280], replicated
- m_w_gate: float32 [2, 1280, 4096], P(None, 'dp')
- m_w_up: float32 [2, 1280, 4096], P(None, 'dp')
- m_w_down: float32 [2, 4096, 1280], P(None, 'dp')
- v_w_gate: float32 [2, 1280, 4096], P(None, 'dp')
- v_w_up: float32 [2, 1280, 4096], P(None, 'dp')
- v_w_down: float32 [2, 4096, 1280], P(None, 'dp')
Outputs:
- output 1: bfloat16 [4, 1280, 4096], P('rep'), parts along dimension 0
- output 2: bfloat16 [4, 1280, 4096], P('rep'), parts along dimension 0
- output 3: bfloat16 [4, 4096, 1280], P('rep'), parts along dimension 0
- output 4: float32 [4, 1280, 4096], P('rep', 'dp'), parts along dimension 0
- output 5: float32 [4, 1280, 4096], P('rep', 'dp'), parts along dimension 0
- output 6: float32 [4, 4096, 1280], P('rep', 'dp'), parts along dimension 0
- output 7: float32 [4, 1280, 4096], P('rep', 'dp'), parts along dimension 0
- output 8: float32 [4, 1280, 4096], P('rep', 'dp'), parts along dimension 0
- output 9: float32 [4, 4096, 1280], P('rep', 'dp'), parts along dimension 0
There are 2 independent parts. The reference program is written for one: setup_inputs(seed, part) draws one part's arguments, and reference() takes and returns one part's arrays. A program takes and returns all parts, laid end to end along the dimension named above; an argument that names none is the same for every part.
All inputs are finite; a program needn't handle non-finite values.
Results may differ from the reference program's by a relative error of at most 0.022.
Values are sent between devices in bfloat16 or wider.
A program may use at most 1.5 GiB of HBM per device.

```python
import jax
import jax.numpy as jnp
from jax import lax

SEQUENCES = 64
TOKENS = 1024
D = 1280
FF = 4096
LAYERS = 2
NAMES = ("w_gate", "w_up", "w_down")
SHAPES = {"w_gate": (LAYERS, D, FF), "w_up": (LAYERS, D, FF), "w_down": (LAYERS, FF, D)}


def bump(key, n, height):
    away = (jnp.arange(n, dtype=jnp.int32) - jax.random.randint(key, (), 0, n, jnp.int32)) % n
    return jnp.where(away < n // 8, height, 1.0)


def together(key, own, strength):
    shared = jax.random.normal(key, own.shape[1:], jnp.float32)
    return (own + strength * shared) * lax.rsqrt(1 + strength * strength)


def setup_inputs(seed: int = 0, part: int = 0) -> dict:
    kx, kdy, ka, kb, kz, kf, kh, kl, *keys = jax.random.split(jax.random.key(seed), 8 + 3 * len(NAMES))
    kx, kdy, ka, kb = (jax.random.fold_in(k, part) for k in (kx, kdy, ka, kb))
    kw, km, kv = (keys[i::3] for i in range(3))
    shape = (SEQUENCES, TOKENS, D)
    much_x, much_dy = jax.random.uniform(kz, (2,), jnp.float32, 0.0, 1.0)
    loud = 2.0 ** jax.random.uniform(jax.random.fold_in(kz, 1), (), jnp.float32, -1.0, 2.0)
    layers = 2.0 ** jax.random.uniform(kl, (LAYERS, 1, 1), jnp.float32, -1.0, 1.0)
    x = together(ka, jax.random.normal(kx, shape, jnp.float32), much_x) * bump(kf, D, 4.0)
    dy = together(kb, jax.random.normal(kdy, shape, jnp.float32), much_dy)
    drawn = {"x": x.astype(jnp.bfloat16), "dy": (loud * dy * (SEQUENCES * TOKENS) ** -0.5).astype(jnp.bfloat16)}
    for key, name in zip(kw, NAMES, strict=True):
        w = jax.random.normal(key, SHAPES[name], jnp.float32) * SHAPES[name][1] ** -0.5
        drawn[name] = (w * {"w_gate": 1.0, "w_up": bump(kh, FF, 4.0), "w_down": layers}[name]).astype(jnp.bfloat16)
    for key, name in zip(km, NAMES, strict=True):
        drawn[f"m_{name}"] = 0.1 * jax.random.normal(key, SHAPES[name], jnp.float32)
    for key, name in zip(kv, NAMES, strict=True):
        drawn[f"v_{name}"] = loud * loud * jax.random.uniform(key, SHAPES[name], jnp.float32, 0.05, 0.15)
    return drawn


def matmul(a, w):
    return jnp.dot(a, w, preferred_element_type=jnp.float32).astype(jnp.bfloat16)


def normed(h):
    wide = h.astype(jnp.float32)
    scale = lax.rsqrt(jnp.mean(wide**2, -1, keepdims=True) + 1e-6)
    return (wide * scale).astype(jnp.bfloat16)


def layer(h, w):
    a = normed(h)
    gate = jnp.dot(a, w["w_gate"], preferred_element_type=jnp.float32)
    up = jnp.dot(a, w["w_up"], preferred_element_type=jnp.float32)
    return h + matmul((jax.nn.silu(gate) * up).astype(jnp.bfloat16), w["w_down"])


def adamw(w, m, v, g):
    m = 0.9 * m + 0.1 * g
    v = 0.95 * v + 0.05 * g * g
    step = m * lax.rsqrt(v + 1e-8) + 0.1 * w
    return (w - 0.02 * step).astype(jnp.bfloat16), m, v


def stack(weights, h):
    return lax.scan(lambda h, w: (layer(h, w), None), h, weights)[0]


def reference(x, dy, w_gate, w_up, w_down, m_w_gate, m_w_up, m_w_down, v_w_gate, v_w_up, v_w_down):
    weights = dict(zip(NAMES, (w_gate, w_up, w_down), strict=True))

    def take(so_far, sequence):
        h, by_y = sequence
        _, back = jax.vjp(lambda w: stack(w, h), weights)
        return jax.tree.map(lambda total, term: total + term.astype(jnp.float32), so_far, back(by_y)[0]), None

    none_yet = {name: jnp.zeros(w.shape, jnp.float32) for name, w in weights.items()}
    by_weights, _ = lax.scan(take, none_yet, (x, dy))
    gradients = [by_weights[name].astype(jnp.bfloat16).astype(jnp.float32) for name in NAMES]
    new = [
        adamw(w.astype(jnp.float32), m, v, g)
        for w, m, v, g in zip((w_gate, w_up, w_down), (m_w_gate, m_w_up, m_w_down), (v_w_gate, v_w_up, v_w_down), gradients, strict=True)
    ]
    return tuple(one[which] for which in range(3) for one in new)
```

```python
import jax
import jax.numpy as jnp
from jax import lax
from jax.sharding import PartitionSpec as P

NAMES = ("w_gate", "w_up", "w_down")


def dot(a, b, dims):
    return lax.dot_general(a, b, (dims, ((), ())), preferred_element_type=jnp.float32)


def scale_of(h):
    wide = h.astype(jnp.float32)
    return lax.rsqrt(jnp.mean(wide**2, -1, keepdims=True) + 1e-6)


def hidden(a, w_gate, w_up):
    gate, up = dot(a, w_gate, ((1,), (0,))), dot(a, w_up, ((1,), (0,)))
    return gate, up, (jax.nn.silu(gate) * up).astype(jnp.bfloat16)


def of_hidden(d, gate, up):
    d = d.astype(jnp.float32)
    s = jax.nn.sigmoid(gate)
    d_gate = d * up * (s * (1 + gate * (1 - s)))
    return d_gate.astype(jnp.bfloat16), (d * (gate * s)).astype(jnp.bfloat16)


def of_norm(h, scale, d):
    wide, d = h.astype(jnp.float32), d.astype(jnp.float32)
    along = jnp.mean(wide * d, -1, keepdims=True)
    return (scale * d - wide * (scale * scale * scale) * along).astype(jnp.bfloat16)


def adamw(w, m, v, g):
    m = 0.9 * m + 0.1 * g
    v = 0.95 * v + 0.05 * g * g
    step = m * lax.rsqrt(v + 1e-8) + 0.1 * w
    return (w - 0.02 * step).astype(jnp.bfloat16), m, v


def solution(mesh):
    n = mesh.shape["dp"]

    def step(x, dy, wg, wu, wd, mg, mu, md, vg, vu, vd):
        bf = jnp.bfloat16
        h0, dy = x[0], dy[0]
        s0 = scale_of(h0)
        a0 = (h0.astype(jnp.float32) * s0).astype(bf)
        g0, u0, p0 = hidden(a0, wg[0], wu[0])
        h1 = h0 + dot(p0, wd[0], ((1,), (0,))).astype(bf)
        s1 = scale_of(h1)
        a1 = (h1.astype(jnp.float32) * s1).astype(bf)
        g1, u1, p1 = hidden(a1, wg[1], wu[1])
        down1 = dot(p1, dy, ((0,), (0,))).astype(bf)
        dg1, du1 = of_hidden(dot(dy, wd[1], ((1,), (1,))).astype(bf), g1, u1)
        gate1 = dot(a1, dg1, ((0,), (0,))).astype(bf)
        up1 = dot(a1, du1, ((0,), (0,))).astype(bf)
        da1 = dot(dg1, wg[1], ((1,), (1,))) + dot(du1, wu[1], ((1,), (1,)))
        dh1 = dy + of_norm(h1, s1, da1)
        down0 = dot(p0, dh1, ((0,), (0,))).astype(bf)
        dg0, du0 = of_hidden(dot(dh1, wd[0], ((1,), (1,))).astype(bf), g0, u0)
        gate0 = dot(a0, dg0, ((0,), (0,))).astype(bf)
        up0 = dot(a0, du0, ((0,), (0,))).astype(bf)

        def summed(gate, up, down):
            parts = [t.reshape(n, -1, 1280) for t in (gate, up, down)]
            return lax.psum_scatter(jnp.concatenate(parts, 1), "dp", scatter_dimension=0, tiled=True)[0]

        me = lax.axis_index("dp")
        news = [None, None]
        for layer, grads in ((1, (gate1, up1, down1)), (0, (gate0, up0, down0))):
            total = summed(*grads).astype(jnp.float32)
            out = []
            for i, (w, m, v) in enumerate(((wg, mg, vg), (wu, mu, vu), (wd, md, vd))):
                rows, cols = m.shape[1:]
                g = total[64 * i : 64 * i + 64].reshape(rows, cols)
                mine = lax.dynamic_slice(w[layer], (me * rows, 0), (rows, cols)).astype(jnp.float32)
                out.append(adamw(mine, m[layer], v[layer], g))
            whole = lax.all_gather(jnp.concatenate([o[0].reshape(64, 1280) for o in out]), "dp")
            news[layer] = [(whole[:, 64 * i : 64 * i + 64].reshape(w.shape[1:]), *out[i][1:]) for i, w in enumerate((wg, wu, wd))]
        return tuple(jnp.stack([news[0][i][which], news[1][i][which]]) for which in range(3) for i in range(3))

    seq, whole, rows = P(("rep", "dp")), P(), P(None, "dp", None)
    return jax.shard_map(
        step,
        mesh=mesh,
        in_specs=(seq, seq) + (whole,) * 3 + (rows,) * 6,
        out_specs=(P("rep"),) * 3 + (P("rep", "dp", None),) * 6,
        check_vma=False,
    )
```

```python
import functools
import jax, jax.numpy as jnp
from jax import lax
from jax.experimental import pallas as pl
from jax.experimental.pallas import tpu as pltpu
from jax.sharding import PartitionSpec as P

AXES = ("x", "y", "z")
STRIDE = {"x": 16, "y": 4, "z": 1}
ORDERS = (("x", "y", "z"), ("y", "z", "x"), ("z", "x", "y"))
BF, F32 = jnp.bfloat16, jnp.float32
ROWS = 3840


def comm_kernel(n_super, U, g, m, v, w, wall, m_out, v_out,
                recv1, send2, recv2, own, sa, b1s, b1r, b2s, b2r, sb, c1s, c1r, c2s, c2r,
                mb, vb, wb, mo, vo, wn, ssem, rsem, lsem):
    me = lax.axis_index("dp")
    pos = {"x": me // 16, "y": (me // 4) % 4, "z": me % 4}
    low = (U // 2 + 15) // 16 * 16
    halves = (pl.ds(0, 2), pl.ds(2, 2))
    row_halves = (pl.ds(0, low), pl.ds(low, U - low))

    def peer(axis, by):
        return {"dp": me + ((pos[axis] + by) % 4 - pos[axis]) * STRIDE[axis]}

    barrier = pltpu.get_barrier_semaphore()
    for axis in AXES:
        for by in (1, 3):
            pl.semaphore_signal(barrier, inc=1, device_id=peer(axis, by), device_id_type=pl.DeviceIdType.MESH)
    pl.semaphore_wait(barrier, 6)

    def part(ref, fixed, rows):
        return ref.at[tuple(fixed.get(axis, slice(None)) for axis in AXES) + (rows, slice(None))]

    def remote(kind, slot, c, way, src, dst, axis):
        return pltpu.make_async_remote_copy(
            src_ref=src, dst_ref=dst, send_sem=ssem.at[kind, slot, c, way], recv_sem=rsem.at[kind, slot, c, way],
            device_id=peer(axis, (1, 3)[way]), device_id_type=pl.DeviceIdType.MESH)

    def local(kind, slot, c, src, dst):
        return pltpu.make_async_copy(src, dst, lsem.at[kind, slot, c])

    class Chunk:
        def __init__(self, c, j):
            self.c, self.slot = c, j % 2
            self.A, self.B, self.C = ORDERS[c]
            self.rest = tuple(axis for axis in AXES if axis != self.A)
            self.ib = self.rest.index(self.B)
            self.rows = pl.ds(pl.multiple_of((3 * j + c) * U, 16), U)
            self.a, self.b, self.c3 = (pos[axis] for axis in ORDERS[c])

        def unit(self, b, i):
            return (b, i) if self.ib == 0 else (i, b)

        def row_part(self, rows):
            return pl.ds(self.rows.start + rows.start, rows.size)

        def a1(self):
            s, c = self.slot, self.c
            return [remote(0, s, c, way, part(g, {self.A: (self.a + 2) % 4, self.rest[0]: halves[way]}, self.rows),
                           recv1.at[s, c, halves[way]], self.A) for way in (0, 1)]

        def load2(self):
            s, c = self.slot, self.c
            return [local(way, s, c, part(g, {self.A: (self.a + (1, 3)[way]) % 4}, self.rows), send2.at[s, c, way]) for way in (0, 1)]

        def load_own(self):
            return [local(2, self.slot, self.c, part(g, {self.A: self.a}, self.rows), own.at[self.slot, self.c])]

        def a2(self):
            s, c = self.slot, self.c
            return [remote(1, s, c, way, send2.at[s, c, way], recv2.at[s, c, way], self.A) for way in (0, 1)]

        def b1(self):
            s, c = self.slot, self.c
            return [remote(2, s, c, way, b1s.at[s, c, halves[way]], b1r.at[s, c, halves[way]], self.B) for way in (0, 1)]

        def b2(self):
            s, c = self.slot, self.c
            return [remote(3, s, c, way, b2s.at[s, c, way], b2r.at[s, c, way], self.B) for way in (0, 1)]

        def c1(self):
            s, c = self.slot, self.c
            return [remote(4, s, c, way, c1s.at[s, c, row_halves[way]], c1r.at[s, c, row_halves[way]], self.C) for way in (0, 1)]

        def c2(self):
            s, c = self.slot, self.c
            return [remote(5, s, c, way, c2s.at[s, c, way], c2r.at[s, c, way], self.C) for way in (0, 1)]

        def load_step(self):
            s, c = self.slot, self.c
            return [local(3 + i, s, c, ref.at[self.rows], buf.at[s, c]) for i, (ref, buf) in enumerate(((m, mb), (v, vb), (w, wb)))]

        def store_step(self):
            s, c = self.slot, self.c
            mine = part(wall, {self.A: self.a, self.B: self.b, self.C: self.c3}, self.rows)
            pairs = ((mo.at[s, c], m_out.at[self.rows]), (vo.at[s, c], v_out.at[self.rows]), (wn.at[s, c], mine))
            return [local(6 + i, s, c, src, dst) for i, (src, dst) in enumerate(pairs)]

        def gather(self, which):
            s, c = self.slot, self.c
            if which < 2:
                axis, here, fixed, kind = self.C, self.c3, {self.A: self.a, self.B: self.b}, 6
            elif which < 4:
                axis, here, fixed, kind = self.B, self.b, {self.A: self.a}, 8
            else:
                axis, here, fixed, kind = self.A, self.a, {}, 10
            if which % 2 == 0:
                block = part(wall, fixed | {axis: here}, self.rows)
                src = wn.at[s, c] if which == 0 else block
                return [remote(kind, s, c, way, src, block, axis) for way in (0, 1)]
            out = []
            for way in (0, 1):
                block = fixed | {axis: (here + (3, 1)[way]) % 4}
                rows = self.rows
                if which == 1:
                    rows = self.row_part(row_halves[way])
                elif which == 3:
                    block[self.C] = halves[way]
                else:
                    block[self.rest[0]] = halves[way]
                half = part(wall, block, rows)
                out.append(remote(kind + 1, s, c, way, half, half, axis))
            return out

    def start(copies):
        for copy in copies:
            copy.start()

    def wait(copies):
        for copy in copies:
            copy.wait()

    def loop(n, body, unroll=1):
        lax.fori_loop(0, n, lambda i, _: (body(i), None)[1], None, unroll=unroll)

    def stage0(k):
        start(k.a1())
        start(k.load2())

    def stage1(k):
        wait(k.load2())
        wait(k.a1())
        s, c = k.slot, k.c

        def body(i):
            for way in (0, 1):
                at = (s, c, 2 * way + i // 4, i % 4)
                to = (s, c, way, 2 * way + i // 4, i % 4)
                send2[to] = (send2[to].astype(F32) + recv1[at].astype(F32)).astype(BF)

        loop(8, body)
        start(k.a2())
        start(k.load_own())

    def stage2(k):
        wait(k.load_own())
        wait(k.a2())
        s, c = k.slot, k.c

        def body(i):
            at = (i // 4, i % 4)
            total = own[(s, c) + at].astype(F32) + recv2[(s, c, 0) + at].astype(F32) + recv2[(s, c, 1) + at].astype(F32)
            sa[(s, c) + at] = total

        loop(16, body)
        far = (k.b + 2) % 4

        def pack(i):
            b1s[s, c, i] = sa[(s, c) + k.unit(far, i)].astype(BF)

        loop(4, pack)
        start(k.b1())

    def stage3(k):
        wait(k.b1())
        s, c = k.slot, k.c
        near = ((k.b + 1) % 4, (k.b + 3) % 4)

        def body(i):
            for way in (0, 1):
                b2s[s, c, way, 2 * way + i] = (sa[(s, c) + k.unit(near[way], 2 * way + i)] + b1r[s, c, 2 * way + i].astype(F32)).astype(BF)
                b2s[s, c, way, 2 - 2 * way + i] = sa[(s, c) + k.unit(near[way], 2 - 2 * way + i)].astype(BF)

        loop(2, body)
        start(k.b2())

    def stage4(k):
        wait(k.b2())
        s, c = k.slot, k.c

        def body(i):
            sb[s, c, i] = sa[(s, c) + k.unit(k.b, i)] + b2r[s, c, 0, i].astype(F32) + b2r[s, c, 1, i].astype(F32)

        loop(4, body)
        c1s[s, c] = sb[s, c, (k.c3 + 2) % 4].astype(BF)
        start(k.c1())

    def stage5(k):
        wait(k.c1())
        s, c = k.slot, k.c
        near = ((k.c3 + 1) % 4, (k.c3 + 3) % 4)
        for way in (0, 1):
            add, keep = row_halves[way], row_halves[1 - way]
            c2s[s, c, way, add] = (sb[s, c, near[way], add] + c1r[s, c, add].astype(F32)).astype(BF)
            c2s[s, c, way, keep] = sb[s, c, near[way], keep].astype(BF)
        start(k.c2())
        start(k.load_step())

    def stage6(k):
        wait(k.load_step())
        wait(k.c2())
        s, c = k.slot, k.c
        total = sb[s, c, k.c3] + c2r[s, c, 0].astype(F32) + c2r[s, c, 1].astype(F32)
        grad = total.astype(BF).astype(F32)
        first = 0.9 * mb[s, c] + 0.1 * grad
        second = 0.95 * vb[s, c] + 0.05 * grad * grad
        old = wb[s, c].astype(F32)
        mo[s, c] = first
        vo[s, c] = second
        wn[s, c] = (old - 0.02 * (first * lax.rsqrt(second + 1e-8) + 0.1 * old)).astype(BF)
        start(k.gather(0))
        start(k.store_step())

    def stage7(k):
        wait(k.gather(0))
        start(k.gather(1))

    def stage8(k):
        wait(k.store_step())
        wait(k.gather(1))
        start(k.gather(2))

    def later(n):
        def stage(k):
            wait(k.gather(n - 1))
            start(k.gather(n))
        return stage

    def stage12(k):
        wait(k.gather(5))

    stages = (stage0, stage1, stage2, stage3, stage4, stage5, stage6, stage7, stage8, later(3), later(4), later(5), stage12)

    def iteration(s):
        for number in reversed(range(len(stages))):
            j = s - number

            @pl.when((j >= 0) & (j < n_super))
            def _():
                for c in range(3):
                    stages[number](Chunk(c, j))

    loop(n_super + len(stages) - 1, iteration)


def comm(g, m, v, w, U, n_super, collective_id=0):
    rows = g.shape[3]
    hbm = pl.BlockSpec(memory_space=pl.ANY)
    V, two = pltpu.VMEM, (2, 3)
    scratch = [
        V(two + (4, 4, U, 128), BF), V(two + (2, 4, 4, U, 128), BF), V(two + (2, 4, 4, U, 128), BF), V(two + (4, 4, U, 128), BF),
        V(two + (4, 4, U, 128), F32),
        V(two + (4, U, 128), BF), V(two + (4, U, 128), BF), V(two + (2, 4, U, 128), BF), V(two + (2, 4, U, 128), BF), V(two + (4, U, 128), F32),
        V(two + (U, 128), BF), V(two + (U, 128), BF), V(two + (2, U, 128), BF), V(two + (2, U, 128), BF),
        V(two + (U, 128), F32), V(two + (U, 128), F32), V(two + (U, 128), BF), V(two + (U, 128), F32), V(two + (U, 128), F32), V(two + (U, 128), BF),
        pltpu.SemaphoreType.DMA((12, 2, 3, 2)), pltpu.SemaphoreType.DMA((12, 2, 3, 2)), pltpu.SemaphoreType.DMA((9, 2, 3)),
    ]
    return pl.pallas_call(
        functools.partial(comm_kernel, n_super, U),
        out_shape=(jax.ShapeDtypeStruct(g.shape, BF), jax.ShapeDtypeStruct(m.shape, F32), jax.ShapeDtypeStruct(v.shape, F32)),
        in_specs=[hbm] * 4, out_specs=(hbm,) * 3, scratch_shapes=scratch,
        compiler_params=pltpu.CompilerParams(collective_id=collective_id, has_side_effects=True, vmem_limit_bytes=48 * 2**20),
        name="sum_step_gather",
    )(g, m, v, w)


def dot(a, b, dims):
    return lax.dot_general(a, b, (dims, ((), ())), preferred_element_type=F32)


def scale_of(h):
    wide = h.astype(F32)
    return lax.rsqrt(jnp.mean(wide**2, -1, keepdims=True) + 1e-6)


def hidden(a, w_gate, w_up):
    gate, up = dot(a, w_gate, ((1,), (0,))), dot(a, w_up, ((1,), (0,)))
    return gate, up, (jax.nn.silu(gate) * up).astype(BF)


def of_hidden(d, gate, up):
    d = d.astype(F32)
    s = jax.nn.sigmoid(gate)
    d_gate = d * up * (s * (1 + gate * (1 - s)))
    return d_gate.astype(BF), (d * (gate * s)).astype(BF)


def of_norm(h, scale, d):
    wide, d = h.astype(F32), d.astype(F32)
    along = jnp.mean(wide * d, -1, keepdims=True)
    return (scale * d - wide * (scale * scale * scale) * along).astype(BF)


def down_kernel(p_ref, d_ref, *refs):
    out = refs[-1]
    for ct in range(2):
        @pl.loop(0, 8)
        def _(i):
            rows = pl.ds(pl.multiple_of(i * 512, 512), 512)
            r = jnp.dot(p_ref[rows, :], d_ref[:, ct * 128 : ct * 128 + 128], preferred_element_type=F32)
            out[pl.ds(i * 8, 8), ct * 64 : ct * 64 + 64, :] = r.reshape(8, 64, 128).astype(BF)


def down_gradient(p_t, d, at, g=None):
    tokens = d.shape[0]
    whole = pl.BlockSpec((4096, tokens), lambda i: (0, 0))
    return pl.pallas_call(
        down_kernel,
        grid=(5,),
        out_shape=jax.ShapeDtypeStruct((64, ROWS, 128), BF),
        in_specs=[whole, pl.BlockSpec((tokens, 256), lambda i: (0, i))] + [pl.BlockSpec(memory_space=pl.ANY)] * (g is not None),
        out_specs=pl.BlockSpec((64, 128, 128), lambda i: (0, at // 128 + i, 0)),
        input_output_aliases={} if g is None else {2: 0},
        cost_estimate=pl.CostEstimate(flops=2 * 4096 * 1280 * 1024, bytes_accessed=22 * 10**6, transcendentals=0),
        name="down_gradient",
    )(p_t, d, *([] if g is None else [g]))


def mixed(even, odd):
    row = lax.broadcasted_iota(jnp.int32, even.shape, 1)
    return (jnp.where(row < 4, even, pltpu.roll(odd, 4, 1)), jnp.where(row < 4, pltpu.roll(even, 4, 1), odd))


def gate_up_kernel(a_ref, dg_ref, du_ref, _, out):
    @pl.loop(0, 4)
    def _(i):
        rows = pl.ds(pl.multiple_of(i * 256, 256), 256)
        for at, d in ((0, dg_ref), (32, du_ref)):
            r = jnp.dot(a_ref[rows, :], d[...], preferred_element_type=F32)
            for ct in range(2):
                out[pl.ds(i * 16, 16), at + 16 * ct : at + 16 * ct + 16, :] = r[:, ct * 128 : ct * 128 + 128].reshape(16, 16, 128).astype(BF)
    last = [jnp.dot(a_ref[1024:, :], d[...], preferred_element_type=F32) for d in (dg_ref, du_ref)]
    tiles = [mixed(*(r[:, ct * 128 : ct * 128 + 128].reshape(32, 8, 128) for r in last)) for ct in range(2)]
    for odd in range(2):
        both = jnp.concatenate([tiles[0][odd], tiles[1][odd]], 1).astype(BF)
        for pair in range(32):
            out[2 * pair + odd, 64:80, :] = both[pair]


def gate_up_gradients(a_t, dg, du, at, g):
    tokens = dg.shape[0]
    slab = pl.BlockSpec((tokens, 256), lambda i: (0, i))
    return pl.pallas_call(
        gate_up_kernel,
        grid=(16,),
        out_shape=jax.ShapeDtypeStruct((64, ROWS, 128), BF),
        in_specs=[pl.BlockSpec((1280, tokens), lambda i: (0, 0)), slab, slab, pl.BlockSpec(memory_space=pl.ANY)],
        out_specs=pl.BlockSpec((64, 80, 128), lambda i: (0, at // 80 + i, 0)),
        input_output_aliases={3: 0},
        cost_estimate=pl.CostEstimate(flops=4 * 4096 * 1280 * 1024, bytes_accessed=40 * 10**6, transcendentals=0),
        name="gate_up_gradients",
    )(a_t, dg, du, g)


def unpack_kernel(w_ref, gate, up, down):
    for d in range(4):
        for ct in range(10):
            down[0, 64 * d : 64 * d + 64, ct * 128 : ct * 128 + 128] = w_ref[d, 64 * ct : 64 * ct + 64, :]

    @pl.loop(0, 16)
    def _(slab):
        base = pl.multiple_of(640 + 80 * slab, 16)
        mix = [w_ref[d, pl.ds(base + 64, 16), :].astype(F32) for d in range(4)]
        for ct in range(2):
            tiles = [mixed(*(mix[2 * pair + odd][8 * ct : 8 * ct + 8][None] for odd in range(2))) for pair in range(2)]
            for which, out in enumerate((gate, up)):
                own = [w_ref[d, pl.ds(base + 32 * which + 16 * ct, 16), :].astype(F32) for d in range(4)]
                rows = jnp.concatenate([own[0], tiles[0][which][0], own[1], own[2], tiles[1][which][0], own[3]], 0)
                out[0, :, pl.ds(pl.multiple_of(slab * 256 + ct * 128, 128), 128)] = rows.astype(BF)


def unpack(wall):
    shapes = ((2, 1280, 4096), (2, 1280, 4096), (2, 4096, 1280))
    return pl.pallas_call(
        unpack_kernel,
        grid=(2, 16),
        out_shape=tuple(jax.ShapeDtypeStruct(s, BF) for s in shapes),
        in_specs=[pl.BlockSpec((4, ROWS // 2, 128), lambda l, i: (i, l, 0))],
        out_specs=tuple(pl.BlockSpec((1, s[1] // 16, s[2]), lambda l, i: (1 - l, i, 0)) for s in shapes),
        cost_estimate=pl.CostEstimate(flops=10**6, bytes_accessed=126 * 10**6, transcendentals=0),
        name="unpack",
    )(wall)


def row_order(w_t):
    pairs = w_t.reshape(32, 40, -1)
    own = jnp.concatenate([pairs[:, :16], pairs[:, 24:]], 1)
    return jnp.concatenate([own.reshape(1024, -1), pairs[:, 16:24].reshape(256, -1)], 0)


def to_units(odd, gate, up, down):
    whole, left = [], []
    for t in (gate, up):
        t = jnp.where(odd, jnp.roll(t, -4, 0), t)
        whole.append(t[:16].reshape(16, 16, 2, 128).transpose(1, 2, 0, 3).reshape(16, 32, 128))
        left.append(t[16:].reshape(4, 16, 2, 128).transpose(1, 2, 0, 3))
    slabs = jnp.concatenate(whole + [jnp.concatenate(left, 2).reshape(16, 16, 128)], 1)
    return jnp.concatenate([down.reshape(64, 10, 128).transpose(1, 0, 2).reshape(640, 128), slabs.reshape(1280, 128)], 0)


def from_units(odd, units):
    slabs = units[640:].reshape(16, 80, 128)
    left = slabs[:, 64:].reshape(16, 2, 2, 4, 128)
    out = []
    for i in range(2):
        whole = slabs[:, 32 * i : 32 * i + 32].reshape(16, 2, 16, 128).transpose(2, 0, 1, 3).reshape(16, 4096)
        t = jnp.concatenate([whole, left[:, :, i].transpose(2, 0, 1, 3).reshape(4, 4096)], 0)
        out.append(jnp.where(odd, jnp.roll(t, 4, 0), t))
    return out + [units[:640].reshape(10, 64, 128).transpose(1, 0, 2).reshape(64, 1280)]


def solution(mesh):
    def step(x, dy, *arrays):
        weights, ms, vs = arrays[:3], arrays[3:6], arrays[6:]
        wg, wu, wd = weights
        h0, dy = x[0], dy[0]
        s0 = scale_of(h0)
        a0 = (h0.astype(F32) * s0).astype(BF)
        g0, u0, p0 = hidden(a0, wg[0], wu[0])
        h1 = h0 + dot(p0, wd[0], ((1,), (0,))).astype(BF)
        s1 = scale_of(h1)
        a1 = (h1.astype(F32) * s1).astype(BF)
        g1, u1, p1 = hidden(a1, wg[1], wu[1])
        grads = down_gradient(p1.T, dy, 0)
        dg1, du1 = of_hidden(dot(dy, wd[1], ((1,), (1,))).astype(BF), g1, u1)
        grads = gate_up_gradients(row_order(a1.T), dg1, du1, 640, grads)
        da1 = dot(dg1, wg[1], ((1,), (1,))) + dot(du1, wu[1], ((1,), (1,)))
        dh1 = dy + of_norm(h1, s1, da1)
        grads = down_gradient(p0.T, dh1, 1920, grads)
        dg0, du0 = of_hidden(dot(dh1, wd[0], ((1,), (1,))).astype(BF), g0, u0)
        grads = gate_up_gradients(row_order(a0.T), dg0, du0, 2560, grads)

        me = lax.axis_index("dp")
        odd = me % 2 == 1
        own = [lax.dynamic_slice_in_dim(w, me * (w.shape[1] // 64), w.shape[1] // 64, 1) for w in weights]
        mine = [jnp.concatenate([to_units(odd, *(t[layer] for t in three)) for layer in (1, 0)], 0) for three in (ms, vs, own)]
        wall, *moments = comm(grads.reshape(4, 4, 4, ROWS, 128), *mine, 80, 16)
        new = list(unpack(wall.reshape(64, ROWS, 128)))
        for t in moments:
            layers = [from_units(odd, t[1920 * (1 - layer) :][:1920]) for layer in (0, 1)]
            new += [jnp.stack(pair) for pair in zip(*layers, strict=True)]
        return tuple(new)

    seq, whole, rows = P(("rep", "dp")), P(), P(None, "dp", None)
    return jax.shard_map(
        step,
        mesh=mesh,
        in_specs=(seq, seq) + (whole,) * 3 + (rows,) * 6,
        out_specs=(P("rep"),) * 3 + (P("rep", "dp", None),) * 6,
        check_vma=False,
    )
```

```python
import functools
import jax, jax.numpy as jnp
from jax import lax
from jax.experimental import pallas as pl
from jax.experimental.pallas import tpu as pltpu
from jax.sharding import PartitionSpec as P

AXES = ("x", "y", "z")
STRIDE = {"x": 16, "y": 4, "z": 1}
ORDERS = (("x", "y", "z"), ("y", "z", "x"), ("z", "x", "y"))
BF, F32 = jnp.bfloat16, jnp.float32
D, FF, TOKENS = 1280, 4096, 1024
ROWS = 3840
U, SUPER = 80, 16


def dot(a, b, dims):
    return lax.dot_general(a, b, (dims, ((), ())), preferred_element_type=F32)


class Refs:
    def __init__(self, operands, buffers):
        (self.a_hbm, self.at_hbm, self.dy_hbm, self.h_hbm, self.wg, self.wu, self.wd) = operands
        (self.a, self.at, self.d, self.ws, self.wds, self.p, self.dgu, self.da, self.out, self.sem) = buffers

    def slabs(self, i):
        slot, layer = i % 2, 1 - i // 8
        cols = pl.ds(pl.multiple_of(i % 8 * 512, 512), 512)
        pairs = ((self.wg.at[layer, :, cols], self.ws.at[slot, 0]), (self.wu.at[layer, :, cols], self.ws.at[slot, 1]),
                 (self.wd.at[layer, cols, :], self.wds.at[slot]))
        return [pltpu.make_async_copy(src, dst, self.sem.at[slot, n]) for n, (src, dst) in enumerate(pairs)]

    def states(self, slot):
        return [pltpu.make_async_copy(self.a_hbm.at[slot], self.a, self.sem.at[0, 3]),
                pltpu.make_async_copy(self.at_hbm.at[slot], self.at, self.sem.at[1, 3])]

    def whole(self, src):
        return pltpu.make_async_copy(src, self.d, self.sem.at[0, 4])

    def put(self, g, row, n):
        rows = pl.ds(pl.multiple_of(row, 16), n)
        return [pltpu.make_async_copy(self.out.at[:, :, :, 0:n, :], g.at[:, :, :, rows, :], self.sem.at[1, 4])]


def tasks_begin(r):
    for copy in r.states(0) + r.slabs(0) + [r.whole(r.dy_hbm)]:
        copy.start()
    r.whole(r.dy_hbm).wait()


def tasks(r, g, s):
    slot, at = s // 8, s % 8

    @pl.when(at < 5)
    def _():
        first = (3 * at + 1) // 2

        @pl.when(at == 0)
        def _():
            for copy in r.states(slot):
                copy.wait()

        def one(f, _):
            columns_task(r, g, slot, f, f > first)

        lax.fori_loop(first, (3 * at + 4) // 2, one, None)

    @pl.when((at == 5) & (slot == 0))
    def _():
        for copy in r.states(1):
            copy.start()

    @pl.when((at == 5) | (at == 6))
    def _():
        down_task(r, g, slot, at - 5, 512)

    @pl.when(at == 7)
    def _():
        down_task(r, g, slot, 2, 256)

        @pl.when(slot == 0)
        def _():
            next_layer(r)


def tasks_done(r, g, s):
    slot, at = s // 8, s % 8

    @pl.when(at < 5)
    def _():
        for copy in r.put(g, 1920 * slot + 160 * ((3 * at + 2) // 2), 160):
            copy.wait()

    @pl.when((at == 5) | (at == 6))
    def _():
        for copy in r.put(g, 1920 * slot + 1280 + 256 * (at - 5), 256):
            copy.wait()

    @pl.when(at == 7)
    def _():
        for copy in r.put(g, 1920 * slot + 1792, 128):
            copy.wait()


def columns_task(r, g, slot, f, more):
    i = 8 * slot + f
    b = i % 2
    for copy in r.slabs(i):
        copy.wait()

    @pl.when(i < 15)
    def _():
        for copy in r.slabs(i + 1):
            copy.start()

    cols = pl.ds(pl.multiple_of(f * 512, 512), 512)

    @pl.loop(0, TOKENS // 256)
    def _(t):
        rows = pl.ds(pl.multiple_of(t * 256, 256), 256)
        gate = dot(r.a[rows, :], r.ws[b, 0], ((1,), (0,)))
        up = dot(r.a[rows, :], r.ws[b, 1], ((1,), (0,)))
        dp = dot(r.d[rows, :], r.wds[b], ((1,), (1,))).astype(BF).astype(F32)
        sig = jax.nn.sigmoid(gate)
        silu = gate * sig
        r.p[rows, cols] = (silu * up).astype(BF)
        r.dgu[rows, 0:512] = (dp * up * (sig * (1 + gate * (1 - sig)))).astype(BF)
        r.dgu[rows, 512:1024] = (dp * silu).astype(BF)

    @pl.when(more)
    def _():
        for copy in r.put(g, 1920 * slot + 160 * (f - 1), 160):
            copy.wait()

    @pl.loop(0, 4)
    def _(k):
        rows = pl.ds(pl.multiple_of(k * 320, 64), 320)
        of_gate = dot(r.at[rows, :], r.dgu[:, 0:512], ((1,), (0,)))
        of_up = dot(r.at[rows, :], r.dgu[:, 512:1024], ((1,), (0,)))
        low = lax.broadcasted_iota(jnp.int32, (8, 128), 0) < 4
        for pair in range(8):
            row = 40 * pair
            for half in range(2):
                parts = ([], [])
                for ct in (2 * half, 2 * half + 1):
                    tile = slice(128 * ct, 128 * ct + 128)
                    gm, um = of_gate[row + 16 : row + 24, tile], of_up[row + 16 : row + 24, tile]
                    parts[0].extend((of_gate[row : row + 16, tile], of_up[row : row + 16, tile], jnp.where(low, gm, pltpu.roll(um, 4, 0))))
                    parts[1].extend((of_gate[row + 24 : row + 40, tile], of_up[row + 24 : row + 40, tile], jnp.where(low, pltpu.roll(gm, 4, 0), um)))
                for odd in range(2):
                    r.out[k, pair // 2, pair % 2 * 2 + odd, 80 * half : 80 * half + 80, :] = jnp.concatenate(parts[odd], 0).astype(BF)

    for copy in r.put(g, 1920 * slot + 160 * f, 160):
        copy.start()

    @pl.when(slot == 0)
    def _():
        @pl.loop(0, TOKENS // 256)
        def _(t):
            rows = pl.ds(pl.multiple_of(t * 256, 256), 256)
            more = dot(r.dgu[rows, 0:512], r.ws[b, 0], ((1,), (1,))) + dot(r.dgu[rows, 512:1024], r.ws[b, 1], ((1,), (1,)))

            @pl.when(f == 0)
            def _():
                r.da[rows, :] = more

            @pl.when(f > 0)
            def _():
                r.da[rows, :] += more


def down_task(r, g, slot, t, width):
    cols = pl.ds(pl.multiple_of(t * 512, 512), width)

    @pl.loop(0, 8)
    def _(k):
        of_down = dot(r.p[:, pl.ds(pl.multiple_of(k * 512, 512), 512)], r.d[:, cols], ((0,), (0,)))
        for ct in range(width // 128):
            part = of_down[:, 128 * ct : 128 * ct + 128].reshape(2, 4, 64, 128).astype(BF)
            r.out[k // 2, pl.ds(k % 2 * 2, 2), :, 64 * ct : 64 * ct + 64, :] = part

    for copy in r.put(g, 1920 * slot + 1280 + 256 * t, width // 2):
        copy.start()


def next_layer(r):
    h = pltpu.make_async_copy(r.h_hbm, r.p.at[:, 0:D], r.sem.at[0, 5])
    h.start()
    h.wait()

    @pl.loop(0, TOKENS // 128)
    def _(t):
        rows = pl.ds(pl.multiple_of(t * 128, 128), 128)
        wide = r.p[rows, 0:D].astype(F32)
        d = r.da[rows, :].astype(BF).astype(F32)
        scale = lax.rsqrt(jnp.mean(wide * wide, -1, keepdims=True) + 1e-6)
        along = jnp.mean(wide * d, -1, keepdims=True)
        through = (scale * d - wide * (scale * scale * scale) * along).astype(BF)
        r.d[rows, :] = (r.d[rows, :].astype(F32) + through.astype(F32)).astype(BF)


def comm_kernel(refs, g, m, v, w, wall, m_out, v_out,
                recv1, send2, recv2, own, sa, b1s, b1r, b2s, b2r, sb, c1s, c1r, c2s, c2r,
                mb, vb, wb, mo, vo, wn, ssem, rsem, lsem):
    n_super = SUPER
    me = lax.axis_index("dp")
    pos = {"x": me // 16, "y": (me // 4) % 4, "z": me % 4}
    low = (U // 2 + 15) // 16 * 16
    halves = (pl.ds(0, 2), pl.ds(2, 2))
    row_halves = (pl.ds(0, low), pl.ds(low, U - low))

    def peer(axis, by):
        return {"dp": me + ((pos[axis] + by) % 4 - pos[axis]) * STRIDE[axis]}

    barrier = pltpu.get_barrier_semaphore()
    for axis in AXES:
        for by in (1, 3):
            pl.semaphore_signal(barrier, inc=1, device_id=peer(axis, by), device_id_type=pl.DeviceIdType.MESH)
    pl.semaphore_wait(barrier, 6)

    def part(ref, fixed, rows):
        return ref.at[tuple(fixed.get(axis, slice(None)) for axis in AXES) + (rows, slice(None))]

    def remote(kind, slot, c, way, src, dst, axis):
        return pltpu.make_async_remote_copy(
            src_ref=src, dst_ref=dst, send_sem=ssem.at[kind, slot, c, way], recv_sem=rsem.at[kind, slot, c, way],
            device_id=peer(axis, (1, 3)[way]), device_id_type=pl.DeviceIdType.MESH)

    def local(kind, slot, c, src, dst):
        return pltpu.make_async_copy(src, dst, lsem.at[kind, slot, c])

    class Chunk:
        def __init__(self, c, j):
            self.c, self.slot = c, j % 2
            self.A, self.B, self.C = ORDERS[c]
            self.rest = tuple(axis for axis in AXES if axis != self.A)
            self.ib = self.rest.index(self.B)
            self.rows = pl.ds(pl.multiple_of((3 * j + c) * U, 16), U)
            self.a, self.b, self.c3 = (pos[axis] for axis in ORDERS[c])

        def unit(self, b, i):
            return (b, i) if self.ib == 0 else (i, b)

        def row_part(self, rows):
            return pl.ds(self.rows.start + rows.start, rows.size)

        def a1(self):
            s, c = self.slot, self.c
            return [remote(0, s, c, way, part(g, {self.A: (self.a + 2) % 4, self.rest[0]: halves[way]}, self.rows),
                           recv1.at[s, c, halves[way]], self.A) for way in (0, 1)]

        def load2(self):
            s, c = self.slot, self.c
            return [local(way, s, c, part(g, {self.A: (self.a + (1, 3)[way]) % 4}, self.rows), send2.at[s, c, way]) for way in (0, 1)]

        def load_own(self):
            return [local(2, self.slot, self.c, part(g, {self.A: self.a}, self.rows), own.at[self.slot, self.c])]

        def a2(self):
            s, c = self.slot, self.c
            return [remote(1, s, c, way, send2.at[s, c, way], recv2.at[s, c, way], self.A) for way in (0, 1)]

        def b1(self):
            s, c = self.slot, self.c
            return [remote(2, s, c, way, b1s.at[s, c, halves[way]], b1r.at[s, c, halves[way]], self.B) for way in (0, 1)]

        def b2(self):
            s, c = self.slot, self.c
            return [remote(3, s, c, way, b2s.at[s, c, way], b2r.at[s, c, way], self.B) for way in (0, 1)]

        def c1(self):
            s, c = self.slot, self.c
            return [remote(4, s, c, way, c1s.at[s, c, row_halves[way]], c1r.at[s, c, row_halves[way]], self.C) for way in (0, 1)]

        def c2(self):
            s, c = self.slot, self.c
            return [remote(5, s, c, way, c2s.at[s, c, way], c2r.at[s, c, way], self.C) for way in (0, 1)]

        def load_step(self):
            s, c = self.slot, self.c
            return [local(3 + i, s, c, ref.at[self.rows], buf.at[s, c]) for i, (ref, buf) in enumerate(((m, mb), (v, vb), (w, wb)))]

        def store_step(self):
            s, c = self.slot, self.c
            mine = part(wall, {self.A: self.a, self.B: self.b, self.C: self.c3}, self.rows)
            pairs = ((mo.at[s, c], m_out.at[self.rows]), (vo.at[s, c], v_out.at[self.rows]), (wn.at[s, c], mine))
            return [local(6 + i, s, c, src, dst) for i, (src, dst) in enumerate(pairs)]

        def gather(self, which):
            s, c = self.slot, self.c
            if which < 2:
                axis, here, fixed, kind = self.C, self.c3, {self.A: self.a, self.B: self.b}, 6
            elif which < 4:
                axis, here, fixed, kind = self.B, self.b, {self.A: self.a}, 8
            else:
                axis, here, fixed, kind = self.A, self.a, {}, 10
            if which % 2 == 0:
                block = part(wall, fixed | {axis: here}, self.rows)
                src = wn.at[s, c] if which == 0 else block
                return [remote(kind, s, c, way, src, block, axis) for way in (0, 1)]
            out = []
            for way in (0, 1):
                block = fixed | {axis: (here + (3, 1)[way]) % 4}
                rows = self.rows
                if which == 1:
                    rows = self.row_part(row_halves[way])
                elif which == 3:
                    block[self.C] = halves[way]
                else:
                    block[self.rest[0]] = halves[way]
                half = part(wall, block, rows)
                out.append(remote(kind + 1, s, c, way, half, half, axis))
            return out

    def start(copies):
        for copy in copies:
            copy.start()

    def wait(copies):
        for copy in copies:
            copy.wait()

    def loop(n, body, unroll=1):
        lax.fori_loop(0, n, lambda i, _: (body(i), None)[1], None, unroll=unroll)

    def stage0(k):
        start(k.a1())
        start(k.load2())

    def stage1(k):
        wait(k.load2())
        wait(k.a1())
        s, c = k.slot, k.c

        def body(i):
            for way in (0, 1):
                at = (s, c, 2 * way + i // 4, i % 4)
                to = (s, c, way, 2 * way + i // 4, i % 4)
                send2[to] = (send2[to].astype(F32) + recv1[at].astype(F32)).astype(BF)

        loop(8, body)
        start(k.a2())
        start(k.load_own())

    def stage2(k):
        wait(k.load_own())
        wait(k.a2())
        s, c = k.slot, k.c

        def body(i):
            at = (i // 4, i % 4)
            total = own[(s, c) + at].astype(F32) + recv2[(s, c, 0) + at].astype(F32) + recv2[(s, c, 1) + at].astype(F32)
            sa[(s, c) + at] = total

        loop(16, body)
        far = (k.b + 2) % 4

        def pack(i):
            b1s[s, c, i] = sa[(s, c) + k.unit(far, i)].astype(BF)

        loop(4, pack)
        start(k.b1())

    def stage3(k):
        wait(k.b1())
        s, c = k.slot, k.c
        near = ((k.b + 1) % 4, (k.b + 3) % 4)

        def body(i):
            for way in (0, 1):
                b2s[s, c, way, 2 * way + i] = (sa[(s, c) + k.unit(near[way], 2 * way + i)] + b1r[s, c, 2 * way + i].astype(F32)).astype(BF)
                b2s[s, c, way, 2 - 2 * way + i] = sa[(s, c) + k.unit(near[way], 2 - 2 * way + i)].astype(BF)

        loop(2, body)
        start(k.b2())

    def stage4(k):
        wait(k.b2())
        s, c = k.slot, k.c

        def body(i):
            sb[s, c, i] = sa[(s, c) + k.unit(k.b, i)] + b2r[s, c, 0, i].astype(F32) + b2r[s, c, 1, i].astype(F32)

        loop(4, body)
        c1s[s, c] = sb[s, c, (k.c3 + 2) % 4].astype(BF)
        start(k.c1())

    def stage5(k):
        wait(k.c1())
        s, c = k.slot, k.c
        near = ((k.c3 + 1) % 4, (k.c3 + 3) % 4)
        for way in (0, 1):
            add, keep = row_halves[way], row_halves[1 - way]
            c2s[s, c, way, add] = (sb[s, c, near[way], add] + c1r[s, c, add].astype(F32)).astype(BF)
            c2s[s, c, way, keep] = sb[s, c, near[way], keep].astype(BF)
        start(k.c2())
        start(k.load_step())

    def stage6(k):
        wait(k.load_step())
        wait(k.c2())
        s, c = k.slot, k.c
        total = sb[s, c, k.c3] + c2r[s, c, 0].astype(F32) + c2r[s, c, 1].astype(F32)
        grad = total.astype(BF).astype(F32)
        first = 0.9 * mb[s, c] + 0.1 * grad
        second = 0.95 * vb[s, c] + 0.05 * grad * grad
        old = wb[s, c].astype(F32)
        mo[s, c] = first
        vo[s, c] = second
        wn[s, c] = (old - 0.02 * (first * lax.rsqrt(second + 1e-8) + 0.1 * old)).astype(BF)
        start(k.gather(0))
        start(k.store_step())

    def stage7(k):
        wait(k.gather(0))
        start(k.gather(1))

    def stage8(k):
        wait(k.store_step())
        wait(k.gather(1))
        start(k.gather(2))

    def later(n):
        def stage(k):
            wait(k.gather(n - 1))
            start(k.gather(n))
        return stage

    def stage12(k):
        wait(k.gather(5))

    stages = (stage0, stage1, stage2, stage3, stage4, stage5, stage6, stage7, stage8, later(3), later(4), later(5), stage12)

    def iteration(s):
        @pl.when(s < n_super)
        def _():
            tasks(refs, g, s)

        for number in reversed(range(len(stages))):
            j = s - number

            @pl.when((j >= 0) & (j < n_super))
            def _():
                if number == 0:
                    tasks_done(refs, g, s)
                for c in range(3):
                    stages[number](Chunk(c, j))

    tasks_begin(refs)
    loop(n_super + len(stages) - 1, iteration)


COMM_SCRATCH = 23


def whole_kernel(*refs):
    ins, outs, scratch = refs[:10], refs[10:14], refs[14:]
    m, v, w = ins[7:]
    wall, m_out, v_out, g = outs
    comm_kernel(Refs(ins[:7], scratch[COMM_SCRATCH:]), g, m, v, w, wall, m_out, v_out, *scratch[:COMM_SCRATCH])


def backward_and_step(a, at, dy, h, wg, wu, wd, m, v, w):
    hbm = pl.BlockSpec(memory_space=pl.ANY)
    V, two = pltpu.VMEM, (2, 3)
    comm_scratch = [
        V(two + (4, 4, U, 128), BF), V(two + (2, 4, 4, U, 128), BF), V(two + (2, 4, 4, U, 128), BF), V(two + (4, 4, U, 128), BF),
        V(two + (4, 4, U, 128), F32),
        V(two + (4, U, 128), BF), V(two + (4, U, 128), BF), V(two + (2, 4, U, 128), BF), V(two + (2, 4, U, 128), BF), V(two + (4, U, 128), F32),
        V(two + (U, 128), BF), V(two + (U, 128), BF), V(two + (2, U, 128), BF), V(two + (2, U, 128), BF),
        V(two + (U, 128), F32), V(two + (U, 128), F32), V(two + (U, 128), BF), V(two + (U, 128), F32), V(two + (U, 128), F32), V(two + (U, 128), BF),
        pltpu.SemaphoreType.DMA((12, 2, 3, 2)), pltpu.SemaphoreType.DMA((12, 2, 3, 2)), pltpu.SemaphoreType.DMA((9, 2, 3)),
    ]
    task_scratch = [
        V((TOKENS, D), BF), V((D, TOKENS), BF), V((TOKENS, D), BF), V((2, 2, D, 512), BF), V((2, 512, D), BF),
        V((TOKENS, FF), BF), V((TOKENS, 1024), BF), V((TOKENS, D), F32), V((4, 4, 4, 256, 128), BF), pltpu.SemaphoreType.DMA((2, 6)),
    ]
    units = jax.ShapeDtypeStruct((4, 4, 4, ROWS, 128), BF)
    moment = jax.ShapeDtypeStruct((ROWS, 128), F32)
    return pl.pallas_call(
        whole_kernel,
        out_shape=(units, moment, moment, units),
        in_specs=[hbm] * 10,
        out_specs=(hbm,) * 4,
        scratch_shapes=comm_scratch + task_scratch,
        compiler_params=pltpu.CompilerParams(collective_id=0, has_side_effects=True, vmem_limit_bytes=67043328),
        name="backward_and_step",
    )(a, at, dy, h, wg, wu, wd, m, v, w)[:3]


def unpack_kernel(w_ref, gate, up, down):
    low = lax.broadcasted_iota(jnp.int32, (8, 128), 0) < 4
    for d in range(4):
        for ct in range(10):
            down[0, 64 * d : 64 * d + 64, ct * 128 : ct * 128 + 128] = w_ref[d, 1280 + 64 * ct : 1344 + 64 * ct, :]

    @pl.loop(0, 16)
    def _(slab):
        rows = pl.ds(pl.multiple_of(80 * slab, 16), 80)
        units = [w_ref[d, rows, :].astype(F32) for d in range(4)]
        for ct in range(2):
            own = [u[40 * ct : 40 * ct + 40] for u in units]
            tile = pl.ds(pl.multiple_of(slab * 256 + ct * 128, 128), 128)
            for which, out in enumerate((gate, up)):
                parts = []
                for even, odd in ((own[0], own[1]), (own[2], own[3])):
                    left, right = even[32:40], odd[32:40]
                    if which == 0:
                        right = pltpu.roll(right, 4, 0)
                    else:
                        left = pltpu.roll(left, 4, 0)
                    parts += [even[16 * which : 16 * which + 16], jnp.where(low, left, right), odd[16 * which : 16 * which + 16]]
                out[0, :, tile] = jnp.concatenate(parts, 0).astype(BF)


def unpack(wall):
    shapes = ((2, D, FF), (2, D, FF), (2, FF, D))
    return pl.pallas_call(
        unpack_kernel,
        grid=(2, 16),
        out_shape=tuple(jax.ShapeDtypeStruct(s, BF) for s in shapes),
        in_specs=[pl.BlockSpec((4, ROWS // 2, 128), lambda l, i: (i, l, 0))],
        out_specs=tuple(pl.BlockSpec((1, s[1] // 16, s[2]), lambda l, i: (1 - l, i, 0)) for s in shapes),
        cost_estimate=pl.CostEstimate(flops=10**6, bytes_accessed=126 * 10**6, transcendentals=0),
        name="unpack",
    )(wall)


def to_units(odd, gate, up, down):
    gate, up = (jnp.where(odd, jnp.roll(t, -4, 1), t) for t in (gate, up))
    tiles = jnp.concatenate([gate[:, :16], up[:, :16], gate[:, 16:], up[:, 16:]], 1)
    tiles = tiles.reshape(2, 40, 32, 128).transpose(0, 2, 1, 3).reshape(2, 1280, 128)
    units = jnp.concatenate([tiles, down.reshape(2, 64, 10, 128).transpose(0, 2, 1, 3).reshape(2, 640, 128)], 1)
    return units[::-1].reshape(ROWS, 128)


def from_units(odd, units):
    units = units.reshape(2, 1920, 128)[::-1]
    tiles = units[:, :1280].reshape(2, 32, 40, 128).transpose(0, 2, 1, 3).reshape(2, 40, FF)
    gate = jnp.concatenate([tiles[:, :16], tiles[:, 32:36]], 1)
    up = jnp.concatenate([tiles[:, 16:32], tiles[:, 36:]], 1)
    down = units[:, 1280:].reshape(2, 10, 64, 128).transpose(0, 2, 1, 3).reshape(2, 64, D)
    return [jnp.where(odd, jnp.roll(t, 4, 1), t) for t in (gate, up)] + [down]


def normed(h):
    wide = h.astype(F32)
    return (wide * lax.rsqrt(jnp.mean(wide**2, -1, keepdims=True) + 1e-6)).astype(BF)


def solution(mesh):
    def step(x, dy, *arrays):
        weights, ms, vs = arrays[:3], arrays[3:6], arrays[6:]
        wg, wu, wd = weights
        h0 = x[0]
        a0 = normed(h0)
        gate, up = (dot(a0, w[0], ((1,), (0,))) for w in (wg, wu))
        p0 = (jax.nn.silu(gate) * up).astype(BF)
        h1 = h0 + dot(p0, wd[0], ((1,), (0,))).astype(BF)
        a = jnp.stack([normed(h1), a0])

        me = lax.axis_index("dp")
        odd = me % 2 == 1
        own = [lax.dynamic_slice_in_dim(w, me * (w.shape[1] // 64), w.shape[1] // 64, 1) for w in weights]
        units = [to_units(odd, *three) for three in (ms, vs, own)]
        wall, *moments = backward_and_step(a, a.transpose(0, 2, 1), dy[0], h1, wg, wu, wd, *units)
        return tuple(unpack(wall.reshape(64, ROWS, 128))) + tuple(t for units in moments for t in from_units(odd, units))

    seq, whole, rows = P(("rep", "dp")), P(), P(None, "dp", None)
    return jax.shard_map(
        step,
        mesh=mesh,
        in_specs=(seq, seq) + (whole,) * 3 + (rows,) * 6,
        out_specs=(P("rep"),) * 3 + (P("rep", "dp", None),) * 6,
        check_vma=False,
    )
```

```python
import jax
import jax.numpy as jnp
from jax import lax
from jax.experimental import pallas as pl
from jax.experimental.pallas import tpu as pltpu
from jax.sharding import PartitionSpec as P

AXES = ("x", "y", "z")
STRIDE = {"x": 16, "y": 4, "z": 1}
ORDERS = (("x", "y", "z"), ("y", "z", "x"), ("z", "x", "y"))
BF, F32 = jnp.bfloat16, jnp.float32
D, FF, TOKENS = 1280, 4096, 1024
ROWS = 3840
U, SUPER = 80, 16


def dot(a, b, dims):
    return lax.dot_general(a, b, (dims, ((), ())), preferred_element_type=F32)


def loop(n, body, unroll=1):
    lax.fori_loop(0, n, lambda i, _: (body(i), None)[1], None, unroll=unroll)


def start(copies):
    for copy in copies:
        copy.start()


def wait(copies):
    for copy in copies:
        copy.wait()


class Refs:
    def __init__(self, operands, buffers):
        self.x, self.dy, self.wg, self.wu, self.wd, self.h = operands
        self.a, self.d, self.ws, self.wds, self.p, self.dgu, self.da, self.out, self.sem = buffers
        self.state = self.p.at[:, FF - D :]

    def slabs(self, i):
        slot, layer = i % 2, i // 8 % 2
        cols = pl.ds(pl.multiple_of(i % 8 * 512, 512), 512)
        pairs = ((self.wg.at[layer, :, cols], self.ws.at[slot, 0]), (self.wu.at[layer, :, cols], self.ws.at[slot, 1]),
                 (self.wd.at[layer, cols, :], self.wds.at[slot]))
        return [pltpu.make_async_copy(src, dst, self.sem.at[slot, n]) for n, (src, dst) in enumerate(pairs)]

    def next_slabs(self, i):
        wait(self.slabs(i))

        @pl.when(i < 23)
        def _():
            start(self.slabs(i + 1))

    def copy(self, n, src, dst):
        return [pltpu.make_async_copy(src, dst, self.sem.at[n // 4, 3 + n % 4])]

    def load_x(self):
        return self.copy(0, self.x, self.state)

    def load_dy(self):
        return self.copy(1, self.dy, self.d)

    def keep_h(self):
        return self.copy(2, self.state, self.h)

    def back_h(self):
        return self.copy(3, self.h, self.state)

    def load_a(self):
        return self.copy(4, self.x, self.a)

    def put(self, g, row, n):
        return self.copy(5, self.out.at[:, :, :, 0:n, :], g.at[:, :, :, pl.ds(pl.multiple_of(row, 16), n), :])


def normed(h):
    wide = h.astype(F32)
    return (wide * lax.rsqrt(jnp.mean(wide * wide, -1, keepdims=True) + 1e-6)).astype(BF)


def token_blocks(size, body):
    loop(TOKENS // size, lambda t: body(pl.ds(pl.multiple_of(t * size, size), size)))


def add_to(ref, rows, first, more):
    @pl.when(first)
    def _():
        ref[rows, :] = more

    @pl.when(jnp.logical_not(first))
    def _():
        ref[rows, :] += more


def forward(r):
    start(r.load_x() + r.slabs(0) + r.load_dy())
    wait(r.load_x())

    def norm(rows):
        r.a[rows, :] = normed(r.state[rows, :])

    token_blocks(128, norm)

    def task(f):
        r.next_slabs(f)
        b = f % 2

        def block(rows):
            gate = dot(r.a[rows, :], r.ws[b, 0], ((1,), (0,)))
            up = dot(r.a[rows, :], r.ws[b, 1], ((1,), (0,)))
            p = (gate * jax.nn.sigmoid(gate) * up).astype(BF)
            add_to(r.da, rows, f == 0, dot(p, r.wds[b], ((1,), (0,))))

        token_blocks(256, block)

    loop(8, task)

    def end(rows):
        h = (r.state[rows, :].astype(F32) + r.da[rows, :].astype(BF).astype(F32)).astype(BF)
        r.state[rows, :] = h
        r.a[rows, :] = normed(h)

    token_blocks(128, end)
    start(r.keep_h())
    wait(r.load_dy())


def tasks(r, g, s):
    slot, at = s // 8, s % 8

    @pl.when(at < 5)
    def _():
        first = (3 * at + 1) // 2

        @pl.when(s == 1)
        def _():
            wait(r.keep_h())

        @pl.when(s == 8)
        def _():
            wait(r.load_a())

            def norm(rows):
                r.a[rows, :] = normed(r.a[rows, :])

            token_blocks(128, norm)

        def one(f, _):
            columns_task(r, g, slot, f, f > first)

        lax.fori_loop(first, (3 * at + 4) // 2, one, None)

    @pl.when(s == 5)
    def _():
        start(r.load_a())

    @pl.when((at == 5) | (at == 6))
    def _():
        down_task(r, g, slot, at - 5, 512)

    @pl.when(at == 7)
    def _():
        down_task(r, g, slot, 2, 256)

        @pl.when(slot == 0)
        def _():
            next_layer(r)


def tasks_done(r, g, s):
    slot, at = s // 8, s % 8

    @pl.when(at < 5)
    def _():
        wait(r.put(g, 1920 * slot + 160 * ((3 * at + 2) // 2), 160))

    @pl.when((at == 5) | (at == 6))
    def _():
        wait(r.put(g, 1920 * slot + 1280 + 256 * (at - 5), 256))

    @pl.when(at == 7)
    def _():
        wait(r.put(g, 1920 * slot + 1792, 128))


def columns_task(r, g, slot, f, more):
    i = 8 + 8 * slot + f
    b = i % 2
    r.next_slabs(i)
    cols = pl.ds(pl.multiple_of(f * 512, 512), 512)

    def block(rows):
        gate = dot(r.a[rows, :], r.ws[b, 0], ((1,), (0,)))
        up = dot(r.a[rows, :], r.ws[b, 1], ((1,), (0,)))
        dp = dot(r.d[rows, :], r.wds[b], ((1,), (1,))).astype(BF).astype(F32)
        sig = jax.nn.sigmoid(gate)
        silu = gate * sig
        r.p[rows, cols] = (silu * up).astype(BF)
        r.dgu[rows, 0:512] = (dp * up * (sig * (1 + gate * (1 - sig)))).astype(BF)
        r.dgu[rows, 512:1024] = (dp * silu).astype(BF)

    token_blocks(256, block)

    @pl.when(more)
    def _():
        wait(r.put(g, 1920 * slot + 160 * (f - 1), 160))

    def gradients(k):
        a = r.a[:, pl.ds(pl.multiple_of(k * 640, 640), 640)]
        of_gate = dot(a, r.dgu[:, 0:512], ((0,), (0,)))
        of_up = dot(a, r.dgu[:, 512:1024], ((0,), (0,)))
        low = lax.broadcasted_iota(jnp.int32, (8, 128), 0) < 4
        for pair in range(16):
            row = 40 * pair
            for half in range(2):
                parts = ([], [])
                for ct in (2 * half, 2 * half + 1):
                    tile = slice(128 * ct, 128 * ct + 128)
                    gm, um = of_gate[row + 16 : row + 24, tile], of_up[row + 16 : row + 24, tile]
                    parts[0].extend((of_gate[row : row + 16, tile], of_up[row : row + 16, tile], jnp.where(low, gm, pltpu.roll(um, 4, 0))))
                    parts[1].extend((of_gate[row + 24 : row + 40, tile], of_up[row + 24 : row + 40, tile], jnp.where(low, pltpu.roll(gm, 4, 0), um)))
                for odd in range(2):
                    at = (2 * k + pair // 8, pair // 2 % 4, pair % 2 * 2 + odd)
                    r.out[at + (slice(80 * half, 80 * half + 80),)] = jnp.concatenate(parts[odd], 0).astype(BF)

    loop(2, gradients)
    start(r.put(g, 1920 * slot + 160 * f, 160))

    @pl.when(slot == 0)
    def _():
        def block(rows):
            more = dot(r.dgu[rows, 0:512], r.ws[b, 0], ((1,), (1,))) + dot(r.dgu[rows, 512:1024], r.ws[b, 1], ((1,), (1,)))
            add_to(r.da, rows, f == 0, more)

        token_blocks(256, block)


def down_task(r, g, slot, t, width):
    cols = pl.ds(pl.multiple_of(t * 512, 512), width)

    def block(k):
        of_down = dot(r.p[:, pl.ds(pl.multiple_of(k * 512, 512), 512)], r.d[:, cols], ((0,), (0,)))
        for ct in range(width // 128):
            part = of_down[:, 128 * ct : 128 * ct + 128].reshape(2, 4, 64, 128).astype(BF)
            r.out[k // 2, pl.ds(k % 2 * 2, 2), :, 64 * ct : 64 * ct + 64, :] = part

    loop(8, block)
    start(r.put(g, 1920 * slot + 1280 + 256 * t, width // 2))


def next_layer(r):
    start(r.back_h())
    wait(r.back_h())

    def block(rows):
        wide = r.state[rows, :].astype(F32)
        d = r.da[rows, :].astype(BF).astype(F32)
        scale = lax.rsqrt(jnp.mean(wide * wide, -1, keepdims=True) + 1e-6)
        along = jnp.mean(wide * d, -1, keepdims=True)
        through = (scale * d - wide * (scale * scale * scale) * along).astype(BF)
        r.d[rows, :] = (r.d[rows, :].astype(F32) + through.astype(F32)).astype(BF)

    token_blocks(128, block)


def comm_kernel(r, g, params, moments, wall, moments_out,
                recv1, send2, recv2, own, sa, b1s, b1r, b2s, b2r, sb, c1s, c1r, c2s, c2r,
                gm, gw, gn, dm, dw, dn, wn, ssem, rsem, lsem):
    n_super = SUPER
    me = lax.axis_index("dp")
    pos = {"x": me // 16, "y": (me // 4) % 4, "z": me % 4}
    low = (U // 2 + 15) // 16 * 16
    halves = (pl.ds(0, 2), pl.ds(2, 2))
    row_halves = (pl.ds(0, low), pl.ds(low, U - low))

    def peer(axis, by):
        return {"dp": me + ((pos[axis] + by) % 4 - pos[axis]) * STRIDE[axis]}

    barrier = pltpu.get_barrier_semaphore()
    for axis in AXES:
        for by in (1, 3):
            pl.semaphore_signal(barrier, inc=1, device_id=peer(axis, by), device_id_type=pl.DeviceIdType.MESH)
    forward(r)
    pl.semaphore_wait(barrier, 6)

    def part(ref, fixed, rows):
        return ref.at[tuple(fixed.get(axis, slice(None)) for axis in AXES) + (rows, slice(None))]

    def remote(kind, slot, c, way, src, dst, axis):
        return pltpu.make_async_remote_copy(
            src_ref=src, dst_ref=dst, send_sem=ssem.at[kind, slot, c, way], recv_sem=rsem.at[kind, slot, c, way],
            device_id=peer(axis, (1, 3)[way]), device_id_type=pl.DeviceIdType.MESH)

    def local(kind, slot, c, src, dst):
        return pltpu.make_async_copy(src, dst, lsem.at[kind, slot, c])

    class Chunk:
        def __init__(self, c, j):
            self.c, self.slot = c, j % 2
            self.A, self.B, self.C = ORDERS[c]
            self.rest = tuple(axis for axis in AXES if axis != self.A)
            self.ib = self.rest.index(self.B)
            self.rows = pl.ds(pl.multiple_of((3 * j + c) * U, 16), U)
            self.k, self.layer = (3 * j + c) % 24, 1 - (3 * j + c) // 24
            self.a, self.b, self.c3 = (pos[axis] for axis in ORDERS[c])

        def unit(self, b, i):
            return (b, i) if self.ib == 0 else (i, b)

        def row_part(self, rows):
            return pl.ds(self.rows.start + rows.start, rows.size)

        def a1(self):
            s, c = self.slot, self.c
            return [remote(0, s, c, way, part(g, {self.A: (self.a + 2) % 4, self.rest[0]: halves[way]}, self.rows),
                           recv1.at[s, c, halves[way]], self.A) for way in (0, 1)]

        def load2(self):
            s, c = self.slot, self.c
            return [local(way, s, c, part(g, {self.A: (self.a + (1, 3)[way]) % 4}, self.rows), send2.at[s, c, way]) for way in (0, 1)]

        def load_own(self):
            return [local(2, self.slot, self.c, part(g, {self.A: self.a}, self.rows), own.at[self.slot, self.c])]

        def a2(self):
            s, c = self.slot, self.c
            return [remote(1, s, c, way, send2.at[s, c, way], recv2.at[s, c, way], self.A) for way in (0, 1)]

        def b1(self):
            s, c = self.slot, self.c
            return [remote(2, s, c, way, b1s.at[s, c, halves[way]], b1r.at[s, c, halves[way]], self.B) for way in (0, 1)]

        def b2(self):
            s, c = self.slot, self.c
            return [remote(3, s, c, way, b2s.at[s, c, way], b2r.at[s, c, way], self.B) for way in (0, 1)]

        def c1(self):
            s, c = self.slot, self.c
            return [remote(4, s, c, way, c1s.at[s, c, row_halves[way]], c1r.at[s, c, row_halves[way]], self.C) for way in (0, 1)]

        def c2(self):
            s, c = self.slot, self.c
            return [remote(5, s, c, way, c2s.at[s, c, way], c2r.at[s, c, way], self.C) for way in (0, 1)]

        def of_columns(self, out):
            s, c = self.slot, self.c
            cols = pl.ds(pl.multiple_of(self.k * 256, 256), 256)
            pairs = []
            for i in range(4):
                which = i // 2 * 3 + i % 2
                if out:
                    pairs.append((gn.at[s, c, i], moments_out[which].at[self.layer, :, cols]))
                else:
                    pairs.append((moments[which].at[self.layer, :, cols], gm.at[s, c, i]))
            if not out:
                rows = pl.ds(pl.multiple_of(me // 2 * 40, 8), 40)
                pairs += [(params[i].at[self.layer, rows, cols], gw.at[s, c, i]) for i in range(2)]
            return [local((10 if out else 3) + i, s, c, *pair) for i, pair in enumerate(pairs)]

        def of_down(self, out, q):
            s, c = self.slot, self.c
            tile = 5 * (self.k - 16) // 4
            pairs = []
            for n, (first, rows, at) in enumerate(((16 * q, 64 - 16 * q, 0), (0, 16 + 16 * q, 64 - 16 * q))):
                cols = pl.ds(pl.multiple_of((tile + n) * 128, 128), 128)
                there, here = pl.ds(first, rows), pl.ds(at, rows)
                for i in range(2):
                    if out:
                        pairs.append((dn.at[s, c, i, here], moments_out[3 * i + 2].at[self.layer, there, cols]))
                    else:
                        pairs.append((moments[3 * i + 2].at[self.layer, there, cols], dm.at[s, c, i, here]))
                if not out:
                    mine = pl.ds(pl.multiple_of(me * 64 + first, 16), rows)
                    pairs.append((params[2].at[self.layer, mine, cols], dw.at[s, c, here]))
            return [local((10 if out else 3) + i, s, c, *pair) for i, pair in enumerate(pairs)]

        def step_copies(self, out, act):
            @pl.when(self.k < 16)
            def _():
                act(self.of_columns(out))

            for q in range(4):
                @pl.when((self.k >= 16) & (self.k % 4 == q))
                def _():
                    act(self.of_down(out, q))

        def store_new(self):
            mine = part(wall, {self.A: self.a, self.B: self.b, self.C: self.c3}, self.rows)
            return [local(9, self.slot, self.c, wn.at[self.slot, self.c], mine)]

        def gather(self, which):
            s, c = self.slot, self.c
            if which < 2:
                axis, here, fixed, kind = self.C, self.c3, {self.A: self.a, self.B: self.b}, 6
            elif which < 4:
                axis, here, fixed, kind = self.B, self.b, {self.A: self.a}, 8
            else:
                axis, here, fixed, kind = self.A, self.a, {}, 10
            if which % 2 == 0:
                block = part(wall, fixed | {axis: here}, self.rows)
                src = wn.at[s, c] if which == 0 else block
                return [remote(kind, s, c, way, src, block, axis) for way in (0, 1)]
            out = []
            for way in (0, 1):
                block = fixed | {axis: (here + (3, 1)[way]) % 4}
                rows = self.rows
                if which == 1:
                    rows = self.row_part(row_halves[way])
                elif which == 3:
                    block[self.C] = halves[way]
                else:
                    block[self.rest[0]] = halves[way]
                half = part(wall, block, rows)
                out.append(remote(kind + 1, s, c, way, half, half, axis))
            return out

    def stage0(k):
        start(k.a1())
        start(k.load2())

    def stage1(k):
        wait(k.load2())
        wait(k.a1())
        s, c = k.slot, k.c

        def body(i):
            for way in (0, 1):
                at = (s, c, 2 * way + i // 4, i % 4)
                to = (s, c, way, 2 * way + i // 4, i % 4)
                send2[to] = (send2[to].astype(F32) + recv1[at].astype(F32)).astype(BF)

        loop(8, body)
        start(k.a2())
        start(k.load_own())

    def stage2(k):
        wait(k.load_own())
        wait(k.a2())
        s, c = k.slot, k.c

        def body(i):
            at = (i // 4, i % 4)
            total = own[(s, c) + at].astype(F32) + recv2[(s, c, 0) + at].astype(F32) + recv2[(s, c, 1) + at].astype(F32)
            sa[(s, c) + at] = total

        loop(16, body)
        far = (k.b + 2) % 4

        def pack(i):
            b1s[s, c, i] = sa[(s, c) + k.unit(far, i)].astype(BF)

        loop(4, pack)
        start(k.b1())

    def stage3(k):
        wait(k.b1())
        s, c = k.slot, k.c
        near = ((k.b + 1) % 4, (k.b + 3) % 4)

        def body(i):
            for way in (0, 1):
                b2s[s, c, way, 2 * way + i] = (sa[(s, c) + k.unit(near[way], 2 * way + i)] + b1r[s, c, 2 * way + i].astype(F32)).astype(BF)
                b2s[s, c, way, 2 - 2 * way + i] = sa[(s, c) + k.unit(near[way], 2 - 2 * way + i)].astype(BF)

        loop(2, body)
        start(k.b2())

    def stage4(k):
        wait(k.b2())
        s, c = k.slot, k.c

        def body(i):
            sb[s, c, i] = sa[(s, c) + k.unit(k.b, i)] + b2r[s, c, 0, i].astype(F32) + b2r[s, c, 1, i].astype(F32)

        loop(4, body)
        c1s[s, c] = sb[s, c, (k.c3 + 2) % 4].astype(BF)
        start(k.c1())

    def stage5(k):
        wait(k.c1())
        s, c = k.slot, k.c
        near = ((k.c3 + 1) % 4, (k.c3 + 3) % 4)
        for way in (0, 1):
            add, keep = row_halves[way], row_halves[1 - way]
            c2s[s, c, way, add] = (sb[s, c, near[way], add] + c1r[s, c, add].astype(F32)).astype(BF)
            c2s[s, c, way, keep] = sb[s, c, near[way], keep].astype(BF)
        start(k.c2())
        k.step_copies(False, start)

    def adamw(old, first, second, grad):
        first = 0.9 * first + 0.1 * grad
        second = 0.95 * second + 0.05 * grad * grad
        return old - 0.02 * (first * lax.rsqrt(second + 1e-8) + 0.1 * old), first, second

    def step_columns(k, grad):
        s, c = k.slot, k.c
        low = lax.broadcasted_iota(jnp.int32, (8, 128), 0) < 4
        odd = me % 2 == 1
        unit = []
        for ct in range(2):
            tile = slice(128 * ct, 128 * ct + 128)
            mix = grad[40 * ct + 32 : 40 * ct + 40]
            turned = pltpu.roll(mix, 4, 0)
            whole, left = [], []
            for i in range(2):
                rest = jnp.where(odd, (turned, mix)[i], (mix, turned)[i])
                rows = jnp.concatenate([grad[40 * ct + 16 * i : 40 * ct + 16 * i + 16], rest], 0)
                rows = jnp.where(odd, pltpu.roll(rows, 4, 0), rows)
                pair = gw[s, c, i, :, tile].astype(F32)
                old = jnp.where(odd, pltpu.roll(pair[16:40], 20, 0), pair[0:24])
                new, first, second = adamw(old, gm[s, c, i, :, tile], gm[s, c, 2 + i, :, tile], rows)
                gn[s, c, i, :, tile] = first
                gn[s, c, 2 + i, :, tile] = second
                new = jnp.where(odd, pltpu.roll(new, 20, 0), new)
                whole.append(new[:16])
                turn = pltpu.roll(new[16:], 4, 0)
                left.append(jnp.where(odd, (turn, new[16:])[i], (new[16:], turn)[i]))
            unit += whole + [jnp.where(low, *left)]
        wn[s, c] = jnp.concatenate(unit, 0).astype(BF)

    def stage6(k):
        k.step_copies(False, wait)
        wait(k.c2())
        s, c = k.slot, k.c
        total = sb[s, c, k.c3] + c2r[s, c, 0].astype(F32) + c2r[s, c, 1].astype(F32)
        grad = total.astype(BF).astype(F32)

        @pl.when(k.k < 16)
        def _():
            step_columns(k, grad)

        @pl.when(k.k >= 16)
        def _():
            new, dn[s, c, 0], dn[s, c, 1] = adamw(dw[s, c].astype(F32), dm[s, c, 0], dm[s, c, 1], grad)
            wn[s, c] = new.astype(BF)

        start(k.gather(0))
        start(k.store_new())
        k.step_copies(True, start)

    def stage7(k):
        wait(k.gather(0))
        start(k.gather(1))

    def stage8(k):
        wait(k.store_new())
        k.step_copies(True, wait)
        wait(k.gather(1))
        start(k.gather(2))

    def later(n):
        def stage(k):
            wait(k.gather(n - 1))
            start(k.gather(n))
        return stage

    def stage12(k):
        wait(k.gather(5))

    stages = (stage0, stage1, stage2, stage3, stage4, stage5, stage6, stage7, stage8, later(3), later(4), later(5), stage12)

    def iteration(s):
        @pl.when(s < n_super)
        def _():
            tasks(r, g, s)

        for number in reversed(range(len(stages))):
            j = s - number

            @pl.when((j >= 0) & (j < n_super))
            def _():
                if number == 0:
                    tasks_done(r, g, s)
                for c in range(3):
                    stages[number](Chunk(c, j))

    loop(n_super + len(stages) - 1, iteration)


def whole_kernel(*refs):
    (x, dy), params, moments = refs[:2], refs[2:5], refs[5:11]
    wall, moments_out, g, h = refs[11], refs[12:18], refs[18], refs[19]
    scratch, n = refs[20:], COMM_SCRATCH
    comm_kernel(Refs((x, dy, *params, h), scratch[n:]), g, params, moments, wall, moments_out, *scratch[:n])


COMM_SCRATCH = 24


def whole_step(x, dy, params, moments):
    hbm = pl.BlockSpec(memory_space=pl.ANY)
    V, two = pltpu.VMEM, (2, 3)
    comm_scratch = [
        V(two + (4, 4, U, 128), BF), V(two + (2, 4, 4, U, 128), BF), V(two + (2, 4, 4, U, 128), BF), V(two + (4, 4, U, 128), BF),
        V(two + (4, 4, U, 128), F32),
        V(two + (4, U, 128), BF), V(two + (4, U, 128), BF), V(two + (2, 4, U, 128), BF), V(two + (2, 4, U, 128), BF), V(two + (4, U, 128), F32),
        V(two + (U, 128), BF), V(two + (U, 128), BF), V(two + (2, U, 128), BF), V(two + (2, U, 128), BF),
        V(two + (4, 24, 256), F32), V(two + (2, 40, 256), BF), V(two + (4, 24, 256), F32),
        V(two + (2, U, 128), F32), V(two + (U, 128), BF), V(two + (2, U, 128), F32), V(two + (U, 128), BF),
        pltpu.SemaphoreType.DMA((12, 2, 3, 2)), pltpu.SemaphoreType.DMA((12, 2, 3, 2)), pltpu.SemaphoreType.DMA((14, 2, 3)),
    ]
    assert len(comm_scratch) == COMM_SCRATCH
    task_scratch = [
        V((TOKENS, D), BF), V((TOKENS, D), BF), V((2, 2, D, 512), BF), V((2, 512, D), BF),
        V((TOKENS, FF), BF), V((TOKENS, 1024), BF), V((TOKENS, D), F32), V((4, 4, 4, 256, 128), BF), pltpu.SemaphoreType.DMA((2, 7)),
    ]
    units = jax.ShapeDtypeStruct((4, 4, 4, ROWS, 128), BF)
    outs = pl.pallas_call(
        whole_kernel,
        out_shape=(units, *(jax.ShapeDtypeStruct(t.shape, F32) for t in moments), units, jax.ShapeDtypeStruct(x.shape, BF)),
        in_specs=[hbm] * 11,
        out_specs=(hbm,) * 9,
        scratch_shapes=comm_scratch + task_scratch,
        compiler_params=pltpu.CompilerParams(collective_id=0, has_side_effects=True, vmem_limit_bytes=67043328),
        name="whole_step",
    )(x, dy, *params, *moments)
    return outs[0], outs[1:7]


UNPACK = 8


def unpack_kernel(w_ref, gate, up, down):
    low = lax.broadcasted_iota(jnp.int32, (8, 128), 0) < 4

    def of_device(d):
        for ct in range(10):
            down[0, pl.ds(pl.multiple_of(64 * d, 64), 64), ct * 128 : ct * 128 + 128] = w_ref[d, 1280 + 64 * ct : 1344 + 64 * ct, :]

    loop(UNPACK, of_device)

    def slab(n):
        rows = pl.ds(pl.multiple_of(80 * n, 16), 80)
        units = [w_ref[d, rows, :].astype(F32) for d in range(UNPACK)]
        for ct in range(2):
            own = [u[40 * ct : 40 * ct + 40] for u in units]
            tile = pl.ds(pl.multiple_of(n * 256 + ct * 128, 128), 128)
            for which, out in enumerate((gate, up)):
                parts = []
                for even, odd in zip(own[::2], own[1::2], strict=True):
                    left, right = even[32:40], odd[32:40]
                    if which == 0:
                        right = pltpu.roll(right, 4, 0)
                    else:
                        left = pltpu.roll(left, 4, 0)
                    parts += [even[16 * which : 16 * which + 16], jnp.where(low, left, right), odd[16 * which : 16 * which + 16]]
                out[0, :, tile] = jnp.concatenate(parts, 0).astype(BF)

    loop(16, slab)


def unpack(wall):
    shapes = ((2, D, FF), (2, D, FF), (2, FF, D))
    blocks = 64 // UNPACK
    return pl.pallas_call(
        unpack_kernel,
        grid=(2, blocks),
        out_shape=tuple(jax.ShapeDtypeStruct(s, BF) for s in shapes),
        in_specs=[pl.BlockSpec((UNPACK, ROWS // 2, 128), lambda l, i: (i, l, 0))],
        out_specs=tuple(pl.BlockSpec((1, s[1] // blocks, s[2]), lambda l, i: (1 - l, i, 0)) for s in shapes),
        cost_estimate=pl.CostEstimate(flops=10**6, bytes_accessed=126 * 10**6, transcendentals=0),
        name="unpack",
    )(wall)


def solution(mesh):
    def step(x, dy, *arrays):
        moments = [jnp.pad(t, ((0, 0), (0, -t.shape[1] % 8), (0, 0))) for t in arrays[3:]]
        wall, new = whole_step(x[0], dy[0], arrays[:3], moments)
        return (*unpack(wall.reshape(64, ROWS, 128)), *(t[:, : old.shape[1]] for t, old in zip(new, arrays[3:], strict=True)))

    seq, whole, rows = P(("rep", "dp")), P(), P(None, "dp", None)
    return jax.shard_map(
        step,
        mesh=mesh,
        in_specs=(seq, seq) + (whole,) * 3 + (rows,) * 6,
        out_specs=(P("rep"),) * 3 + (P("rep", "dp", None),) * 6,
        check_vma=False,
    )
```

```python
import functools

import jax
import jax.numpy as jnp
from jax import lax
from jax.experimental import pallas as pl
from jax.experimental.pallas import tpu as pltpu
from jax.sharding import PartitionSpec as P

AXES = ("x", "y", "z")
STRIDE = {"x": 16, "y": 4, "z": 1}
ORDERS = (("x", "y", "z"), ("y", "z", "x"), ("z", "x", "y"))
BF, F32 = jnp.bfloat16, jnp.float32
D, FF, TOKENS = 1280, 4096, 1024
ROWS = 3840
U, SUPER = 80, 16


def dot(a, b, dims):
    return lax.dot_general(a, b, (dims, ((), ())), preferred_element_type=F32)


def loop(n, body, unroll=1):
    lax.fori_loop(0, n, lambda i, _: (body(i), None)[1], None, unroll=unroll)


def start(copies):
    for copy in copies:
        copy.start()


def wait(copies):
    for copy in copies:
        copy.wait()


class Refs:
    def __init__(self, operands, buffers):
        self.x, self.dy, self.wg, self.wu, self.wd, self.h, self.kept = operands
        self.a, self.d, self.ws, self.wds, self.p, self.dgu, self.da, self.out, self.sem = buffers
        self.state = self.p.at[:, FF - D :]

    def slabs(self, i):
        slot, layer = i % 2, (i // 8 + 1) // 2 % 2
        pairs = [(self.wd.at[layer, pl.ds(pl.multiple_of(i % 8 * 512, 512), 512), :], self.wds.at[slot])]
        for n in range(4):
            cols = pl.ds(pl.multiple_of(i % 8 * 512 + n // 2 * 256, 256), 256)
            pairs.append(((self.wg, self.wu)[n % 2].at[layer, :, cols], self.ws.at[slot, :, 256 * n : 256 * n + 256]))
        return [pltpu.make_async_copy(src, dst, self.sem.at[slot, n]) for n, (src, dst) in enumerate(pairs)]

    def next_slabs(self, i):
        wait(self.slabs(i))

        @pl.when(i < 31)
        def _():
            start(self.slabs(i + 1))

    def copy(self, n, src, dst):
        return [pltpu.make_async_copy(src, dst, self.sem.at[n // 6, 5 + n % 6])]

    def load_x(self):
        return self.copy(0, self.x, self.state)

    def load_dy(self):
        return self.copy(1, self.dy, self.d)

    def keep_h(self):
        return self.copy(2, self.state, self.h)

    def back_h(self):
        return self.copy(3, self.h, self.state)

    def load_a(self):
        return self.copy(4, self.x, self.a)

    def keep(self, f):
        return self.copy(5 + f % 2, self.dgu.at[f % 2], self.kept.at[f])

    def back(self, f):
        return self.copy(7 + f % 2, self.kept.at[f], self.dgu.at[f % 2])

    def put(self, g, row, n, at=0, sem=0):
        return self.copy(9 + sem, self.out.at[:, :, :, pl.ds(pl.multiple_of(at, 16), n), :], g.at[:, :, :, pl.ds(pl.multiple_of(row, 16), n), :])


def normed(h):
    wide = h.astype(F32)
    return (wide * lax.rsqrt(jnp.mean(wide * wide, -1, keepdims=True) + 1e-6)).astype(BF)


def token_blocks(size, body):
    loop(TOKENS // size, lambda t: body(pl.ds(pl.multiple_of(t * size, size), size)))


def add_to(ref, rows, first, more):
    @pl.when(first)
    def _():
        ref[rows, :] = more

    @pl.when(jnp.logical_not(first))
    def _():
        ref[rows, :] += more


def gate_and_up(r, rows, b, half):
    both = dot(r.a[rows, :], r.ws[b, :, 512 * half : 512 * half + 512], ((1,), (0,)))
    return both[:, :256], both[:, 256:]


def forward(r):
    start(r.load_x() + r.slabs(0) + r.load_dy())
    wait(r.load_x())

    def norm(rows):
        r.a[rows, :] = normed(r.state[rows, :])

    token_blocks(128, norm)

    def task(f):
        r.next_slabs(f)
        b = f % 2

        def block(rows):
            p = []
            for half in range(2):
                gate, up = gate_and_up(r, rows, b, half)
                p.append((gate * jax.nn.sigmoid(gate) * up).astype(BF))
            add_to(r.da, rows, f == 0, dot(jnp.concatenate(p, 1), r.wds[b], ((1,), (0,))))

        token_blocks(256, block)

    loop(8, task)

    def end(rows):
        h = (r.state[rows, :].astype(F32) + r.da[rows, :].astype(BF).astype(F32)).astype(BF)
        r.state[rows, :] = h
        r.a[rows, :] = normed(h)

    token_blocks(128, end)
    start(r.keep_h())
    wait(r.load_dy())


def tasks(r, g, s):
    slot, at = s // 8, s % 8

    @pl.when(s == 1)
    def _():
        wait(r.keep_h())

    @pl.when(s == 8)
    def _():
        wait(r.load_a())

        def norm(rows):
            r.a[rows, :] = normed(r.a[rows, :])

        token_blocks(128, norm)

    def one(n, _):
        @pl.when(n % 2 == 0)
        def _():
            hidden_task(r, slot, n // 2)

        columns_task(r, g, slot, n, n % 3)

    lax.fori_loop(jnp.minimum(3 * at, 16), jnp.minimum(3 * at + 3, 16), one, None)

    @pl.when(at == 5)
    def _():
        @pl.when(slot == 0)
        def _():
            start(r.load_a())
            wait(r.keep(7))
            start(r.back(0))
            start(r.back(1))

        wait(r.put(g, 1920 * slot + 1200, 80))

    @pl.when((at == 5) | (at == 6))
    def _():
        down_task(r, g, slot, at - 5, 512)

    @pl.when(at == 7)
    def _():
        down_task(r, g, slot, 2, 256)

    @pl.when((at >= 5) & (slot == 0))
    def _():
        lax.fori_loop(3 * (at - 5), jnp.minimum(3 * (at - 4), 8), lambda f, _: da_task(r, f), None)

        @pl.when(at == 7)
        def _():
            next_layer(r)


def tasks_done(r, g, s):
    slot, at = s // 8, s % 8

    @pl.when(at < 5)
    def _():
        for n in range(3):
            wait(r.put(g, 1920 * slot + 80 * (3 * at + n), 80, 80 * n, n))

    @pl.when((at == 5) | (at == 6))
    def _():
        wait(r.put(g, 1920 * slot + 1280 + 256 * (at - 5), 256))

    @pl.when(at == 7)
    def _():
        wait(r.put(g, 1920 * slot + 1792, 128))


def hidden_task(r, slot, f):
    i = 8 + 16 * slot + f
    b = i % 2
    r.next_slabs(i)

    @pl.when((slot == 0) & (f > 0))
    def _():
        wait(r.keep(f - 1))

    def block(rows):
        dp = dot(r.d[rows, :], r.wds[b], ((1,), (1,))).astype(BF).astype(F32)
        for half in range(2):
            gate, up = gate_and_up(r, rows, b, half)
            sig = jax.nn.sigmoid(gate)
            silu = gate * sig
            d = dp[:, 256 * half : 256 * half + 256]
            r.p[rows, pl.ds(pl.multiple_of(f * 512 + 256 * half, 256), 256)] = (silu * up).astype(BF)
            r.dgu[b, rows, 512 * half : 512 * half + 256] = (d * up * (sig * (1 + gate * (1 - sig)))).astype(BF)
            r.dgu[b, rows, 512 * half + 256 : 512 * half + 512] = (d * silu).astype(BF)

    token_blocks(256, block)

    @pl.when(slot == 0)
    def _():
        start(r.keep(f))


def columns_task(r, g, slot, n, region):
    b = n // 2 % 2
    cols = pl.ds(pl.multiple_of(n % 2 * 512, 512), 512)

    def gradients(k):
        of_both = dot(r.a[:, pl.ds(pl.multiple_of(k * 640, 640), 640)], r.dgu[b, :, cols], ((0,), (0,)))
        low = lax.broadcasted_iota(jnp.int32, (8, 128), 0) < 4
        for pair in range(16):
            row = 40 * pair
            parts = ([], [])
            for ct in range(2):
                gate, up = (of_both[row : row + 40, at + 128 * ct : at + 128 * ct + 128] for at in (0, 256))
                gm, um = gate[16:24], up[16:24]
                parts[0].extend((gate[:16], up[:16], jnp.where(low, gm, pltpu.roll(um, 4, 0))))
                parts[1].extend((gate[24:], up[24:], jnp.where(low, pltpu.roll(gm, 4, 0), um)))
            for odd in range(2):
                at = (2 * k + pair // 8, pair // 2 % 4, pair % 2 * 2 + odd)
                r.out[at + (pl.ds(pl.multiple_of(80 * region, 16), 80),)] = jnp.concatenate(parts[odd], 0).astype(BF)

    loop(2, gradients)
    for m in range(3):
        @pl.when(region == m)
        def _():
            start(r.put(g, 1920 * slot + 80 * n, 80, 80 * m, m))


def da_task(r, f):
    i = 16 + f
    r.next_slabs(i)
    wait(r.back(f))
    b = i % 2

    def block(rows):
        add_to(r.da, rows, f == 0, dot(r.dgu[b, rows, :], r.ws[b], ((1,), (1,))))

    token_blocks(256, block)

    @pl.when(f < 6)
    def _():
        start(r.back(f + 2))


def down_task(r, g, slot, t, width):
    cols = pl.ds(pl.multiple_of(t * 512, 512), width)

    def block(k):
        of_down = dot(r.p[:, pl.ds(pl.multiple_of(k * 512, 512), 512)], r.d[:, cols], ((0,), (0,)))
        for ct in range(width // 128):
            part = of_down[:, 128 * ct : 128 * ct + 128].reshape(2, 4, 64, 128).astype(BF)
            r.out[k // 2, pl.ds(k % 2 * 2, 2), :, 64 * ct : 64 * ct + 64, :] = part

    loop(8, block)
    start(r.put(g, 1920 * slot + 1280 + 256 * t, width // 2))


def next_layer(r):
    start(r.back_h())
    wait(r.back_h())

    def block(rows):
        wide = r.state[rows, :].astype(F32)
        d = r.da[rows, :].astype(BF).astype(F32)
        scale = lax.rsqrt(jnp.mean(wide * wide, -1, keepdims=True) + 1e-6)
        along = jnp.mean(wide * d, -1, keepdims=True)
        through = (scale * d - wide * (scale * scale * scale) * along).astype(BF)
        r.d[rows, :] = (r.d[rows, :].astype(F32) + through.astype(F32)).astype(BF)

    token_blocks(128, block)


def comm_kernel(r, g, params, moments, wall, moments_out,
                recv1, send2, recv2, own, sa, b1s, b1r, b2s, b2r, sb, c1s, c1r, c2s, c2r,
                gm, gw, gn, rows24, dm, dw, dn, wn, ssem, rsem, lsem):
    n_super = SUPER
    me = lax.axis_index("dp")
    pos = {"x": me // 16, "y": (me // 4) % 4, "z": me % 4}
    low = (U // 2 + 15) // 16 * 16
    halves = (pl.ds(0, 2), pl.ds(2, 2))
    row_halves = (pl.ds(0, low), pl.ds(low, U - low))

    def peer(axis, by):
        return {"dp": me + ((pos[axis] + by) % 4 - pos[axis]) * STRIDE[axis]}

    barrier = pltpu.get_barrier_semaphore()
    for axis in AXES:
        for by in (1, 3):
            pl.semaphore_signal(barrier, inc=1, device_id=peer(axis, by), device_id_type=pl.DeviceIdType.MESH)
    forward(r)
    pl.semaphore_wait(barrier, 6)

    def part(ref, fixed, rows):
        return ref.at[tuple(fixed.get(axis, slice(None)) for axis in AXES) + (rows, slice(None))]

    def remote(kind, slot, c, way, src, dst, axis):
        return pltpu.make_async_remote_copy(
            src_ref=src, dst_ref=dst, send_sem=ssem.at[kind, slot, c, way], recv_sem=rsem.at[kind, slot, c, way],
            device_id=peer(axis, (1, 3)[way]), device_id_type=pl.DeviceIdType.MESH)

    def local(kind, slot, c, src, dst):
        return pltpu.make_async_copy(src, dst, lsem.at[kind, slot, c])

    class Chunk:
        def __init__(self, c, j):
            self.c, self.slot = c, j % 2
            self.A, self.B, self.C = ORDERS[c]
            self.rest = tuple(axis for axis in AXES if axis != self.A)
            self.ib = self.rest.index(self.B)
            self.rows = pl.ds(pl.multiple_of((3 * j + c) * U, 16), U)
            self.k, self.layer = (3 * j + c) % 24, 1 - (3 * j + c) // 24
            self.a, self.b, self.c3 = (pos[axis] for axis in ORDERS[c])

        def unit(self, b, i):
            return (b, i) if self.ib == 0 else (i, b)

        def row_part(self, rows):
            return pl.ds(self.rows.start + rows.start, rows.size)

        def a1(self):
            s, c = self.slot, self.c
            return [remote(0, s, c, way, part(g, {self.A: (self.a + 2) % 4, self.rest[0]: halves[way]}, self.rows),
                           recv1.at[s, c, halves[way]], self.A) for way in (0, 1)]

        def load2(self):
            s, c = self.slot, self.c
            return [local(way, s, c, part(g, {self.A: (self.a + (1, 3)[way]) % 4}, self.rows), send2.at[s, c, way]) for way in (0, 1)]

        def load_own(self):
            return [local(2, self.slot, self.c, part(g, {self.A: self.a}, self.rows), own.at[self.slot, self.c])]

        def a2(self):
            s, c = self.slot, self.c
            return [remote(1, s, c, way, send2.at[s, c, way], recv2.at[s, c, way], self.A) for way in (0, 1)]

        def b1(self):
            s, c = self.slot, self.c
            return [remote(2, s, c, way, b1s.at[s, c, halves[way]], b1r.at[s, c, halves[way]], self.B) for way in (0, 1)]

        def b2(self):
            s, c = self.slot, self.c
            return [remote(3, s, c, way, b2s.at[s, c, way], b2r.at[s, c, way], self.B) for way in (0, 1)]

        def c1(self):
            s, c = self.slot, self.c
            return [remote(4, s, c, way, c1s.at[s, c, row_halves[way]], c1r.at[s, c, row_halves[way]], self.C) for way in (0, 1)]

        def c2(self):
            s, c = self.slot, self.c
            return [remote(5, s, c, way, c2s.at[s, c, way], c2r.at[s, c, way], self.C) for way in (0, 1)]

        def of_columns(self, out):
            s, c = self.slot, self.c
            cols = pl.ds(pl.multiple_of(self.k * 256, 256), 256)
            pairs = []
            for i in range(4):
                which = i // 2 * 3 + i % 2
                if out:
                    pairs.append((gn.at[s, c, i], moments_out[which].at[self.layer, :, cols]))
                else:
                    pairs.append((moments[which].at[self.layer, :, cols], gm.at[s, c, i]))
            if not out:
                rows = pl.ds(pl.multiple_of(me // 2 * 40, 8), 40)
                pairs += [(params[i].at[self.layer, rows, cols], gw.at[s, c, i]) for i in range(2)]
            return [local((10 if out else 3) + i, s, c, *pair) for i, pair in enumerate(pairs)]

        def of_down(self, out, q):
            s, c = self.slot, self.c
            tile = 5 * (self.k - 16) // 4
            pairs = []
            for n, (first, rows, at) in enumerate(((16 * q, 64 - 16 * q, 0), (0, 16 + 16 * q, 64 - 16 * q))):
                cols = pl.ds(pl.multiple_of((tile + n) * 128, 128), 128)
                there, here = pl.ds(first, rows), pl.ds(at, rows)
                for i in range(2):
                    if out:
                        pairs.append((dn.at[s, c, i, here], moments_out[3 * i + 2].at[self.layer, there, cols]))
                    else:
                        pairs.append((moments[3 * i + 2].at[self.layer, there, cols], dm.at[s, c, i, here]))
                if not out:
                    mine = pl.ds(pl.multiple_of(me * 64 + first, 16), rows)
                    pairs.append((params[2].at[self.layer, mine, cols], dw.at[s, c, here]))
            return [local((10 if out else 3) + i, s, c, *pair) for i, pair in enumerate(pairs)]

        def step_copies(self, out, act):
            @pl.when(self.k < 16)
            def _():
                act(self.of_columns(out))

            for q in range(4):
                @pl.when((self.k >= 16) & (self.k % 4 == q))
                def _():
                    act(self.of_down(out, q))

        def store_new(self):
            mine = part(wall, {self.A: self.a, self.B: self.b, self.C: self.c3}, self.rows)
            return [local(9, self.slot, self.c, wn.at[self.slot, self.c], mine)]

        def gather(self, which):
            s, c = self.slot, self.c
            if which < 2:
                axis, here, fixed, kind = self.C, self.c3, {self.A: self.a, self.B: self.b}, 6
            elif which < 4:
                axis, here, fixed, kind = self.B, self.b, {self.A: self.a}, 8
            else:
                axis, here, fixed, kind = self.A, self.a, {}, 10
            if which % 2 == 0:
                block = part(wall, fixed | {axis: here}, self.rows)
                src = wn.at[s, c] if which == 0 else block
                return [remote(kind, s, c, way, src, block, axis) for way in (0, 1)]
            out = []
            for way in (0, 1):
                block = fixed | {axis: (here + (3, 1)[way]) % 4}
                rows = self.rows
                if which == 1:
                    rows = self.row_part(row_halves[way])
                elif which == 3:
                    block[self.C] = halves[way]
                else:
                    block[self.rest[0]] = halves[way]
                half = part(wall, block, rows)
                out.append(remote(kind + 1, s, c, way, half, half, axis))
            return out

    def stage0(k):
        start(k.a1())
        start(k.load2())

    def stage1(k):
        wait(k.load2())
        wait(k.a1())
        s, c = k.slot, k.c

        def body(i):
            for way in (0, 1):
                at = (s, c, 2 * way + i // 4, i % 4)
                to = (s, c, way, 2 * way + i // 4, i % 4)
                send2[to] = (send2[to].astype(F32) + recv1[at].astype(F32)).astype(BF)

        loop(8, body)
        start(k.a2())
        start(k.load_own())

    def stage2(k):
        wait(k.load_own())
        wait(k.a2())
        s, c = k.slot, k.c

        def body(i):
            at = (i // 4, i % 4)
            total = own[(s, c) + at].astype(F32) + recv2[(s, c, 0) + at].astype(F32) + recv2[(s, c, 1) + at].astype(F32)
            sa[(s, c) + at] = total

        loop(16, body)
        far = (k.b + 2) % 4

        def pack(i):
            b1s[s, c, i] = sa[(s, c) + k.unit(far, i)].astype(BF)

        loop(4, pack)
        start(k.b1())

    def stage3(k):
        wait(k.b1())
        s, c = k.slot, k.c
        near = ((k.b + 1) % 4, (k.b + 3) % 4)

        def body(i):
            for way in (0, 1):
                b2s[s, c, way, 2 * way + i] = (sa[(s, c) + k.unit(near[way], 2 * way + i)] + b1r[s, c, 2 * way + i].astype(F32)).astype(BF)
                b2s[s, c, way, 2 - 2 * way + i] = sa[(s, c) + k.unit(near[way], 2 - 2 * way + i)].astype(BF)

        loop(2, body)
        start(k.b2())

    def stage4(k):
        wait(k.b2())
        s, c = k.slot, k.c

        def body(i):
            sb[s, c, i] = sa[(s, c) + k.unit(k.b, i)] + b2r[s, c, 0, i].astype(F32) + b2r[s, c, 1, i].astype(F32)

        loop(4, body)
        c1s[s, c] = sb[s, c, (k.c3 + 2) % 4].astype(BF)
        start(k.c1())

    def stage5(k):
        wait(k.c1())
        s, c = k.slot, k.c
        near = ((k.c3 + 1) % 4, (k.c3 + 3) % 4)
        for way in (0, 1):
            add, keep = row_halves[way], row_halves[1 - way]
            c2s[s, c, way, add] = (sb[s, c, near[way], add] + c1r[s, c, add].astype(F32)).astype(BF)
            c2s[s, c, way, keep] = sb[s, c, near[way], keep].astype(BF)
        start(k.c2())
        k.step_copies(False, start)

    def adamw(old, first, second, grad):
        first = 0.9 * first + 0.1 * grad
        second = 0.95 * second + 0.05 * grad * grad
        return old - 0.02 * (first * lax.rsqrt(second + 1e-8) + 0.1 * old), first, second

    def step_columns(k, grad):
        s, c = k.slot, k.c
        low = lax.broadcasted_iota(jnp.int32, (8, 128), 0) < 4
        odd = me % 2 == 1
        unit = []
        for ct in range(2):
            tile = slice(128 * ct, 128 * ct + 128)
            mix = grad[40 * ct + 32 : 40 * ct + 40]
            turned = pltpu.roll(mix, 4, 0)
            whole, left = [], []
            for i in range(2):
                rest = jnp.where(odd, (turned, mix)[i], (mix, turned)[i])
                rows = jnp.concatenate([grad[40 * ct + 16 * i : 40 * ct + 16 * i + 16], rest], 0)
                rows = jnp.where(odd, pltpu.roll(rows, 4, 0), rows)
                pair = gw[s, c, i, :, tile].astype(F32)
                old = jnp.where(odd, pltpu.roll(pair[16:40], 20, 0), pair[0:24])
                new, first, second = adamw(old[:20], gm[s, c, i, :, tile], gm[s, c, 2 + i, :, tile], rows[:20])
                gn[s, c, i, :, tile] = first
                gn[s, c, 2 + i, :, tile] = second
                rows24[ct, i, 0:20] = new
                new = rows24[ct, i]
                new = jnp.where(odd, pltpu.roll(new, 20, 0), new)
                whole.append(new[:16])
                turn = pltpu.roll(new[16:], 4, 0)
                left.append(jnp.where(odd, (turn, new[16:])[i], (new[16:], turn)[i]))
            unit += whole + [jnp.where(low, *left)]
        wn[s, c] = jnp.concatenate(unit, 0).astype(BF)

    def stage6(k):
        k.step_copies(False, wait)
        wait(k.c2())
        s, c = k.slot, k.c
        total = sb[s, c, k.c3] + c2r[s, c, 0].astype(F32) + c2r[s, c, 1].astype(F32)
        grad = total.astype(BF).astype(F32)

        @pl.when(k.k < 16)
        def _():
            step_columns(k, grad)

        @pl.when(k.k >= 16)
        def _():
            new, dn[s, c, 0], dn[s, c, 1] = adamw(dw[s, c].astype(F32), dm[s, c, 0], dm[s, c, 1], grad)
            wn[s, c] = new.astype(BF)

        start(k.gather(0))
        start(k.store_new())
        k.step_copies(True, start)

    def stage7(k):
        wait(k.gather(0))
        start(k.gather(1))

    def stage8(k):
        wait(k.store_new())
        k.step_copies(True, wait)
        wait(k.gather(1))
        start(k.gather(2))

    def later(n):
        def stage(k):
            wait(k.gather(n - 1))
            start(k.gather(n))
        return stage

    def stage12(k):
        wait(k.gather(5))

    stages = (stage0, stage1, stage2, stage3, stage4, stage5, stage6, stage7, stage8, later(3), later(4), later(5), stage12)

    def iteration(s):
        @pl.when(s < n_super)
        def _():
            tasks(r, g, s)

        for number in reversed(range(len(stages))):
            j = s - number

            @pl.when((j >= 0) & (j < n_super))
            def _():
                if number == 0:
                    tasks_done(r, g, s)
                for c in range(3):
                    stages[number](Chunk(c, j))

    loop(n_super + len(stages) - 1, iteration)


def whole_kernel(*refs):
    (x, dy), params, moments = refs[:2], refs[2:5], refs[5:11]
    wall, moments_out, g, kept = refs[11], refs[12:18], refs[18], refs[19:21]
    scratch, n = refs[21:], COMM_SCRATCH
    comm_kernel(Refs((x, dy, *params, *kept), scratch[n:]), g, params, moments, wall, moments_out, *scratch[:n])


COMM_SCRATCH = 25


def whole_step(x, dy, params, moments):
    hbm = pl.BlockSpec(memory_space=pl.ANY)
    V, two = pltpu.VMEM, (2, 3)
    comm_scratch = [
        V(two + (4, 4, U, 128), BF), V(two + (2, 4, 4, U, 128), BF), V(two + (2, 4, 4, U, 128), BF), V(two + (4, 4, U, 128), BF),
        V(two + (4, 4, U, 128), F32),
        V(two + (4, U, 128), BF), V(two + (4, U, 128), BF), V(two + (2, 4, U, 128), BF), V(two + (2, 4, U, 128), BF), V(two + (4, U, 128), F32),
        V(two + (U, 128), BF), V(two + (U, 128), BF), V(two + (2, U, 128), BF), V(two + (2, U, 128), BF),
        V(two + (4, 20, 256), F32), V(two + (2, 40, 256), BF), V(two + (4, 20, 256), F32), V((2, 2, 24, 128), F32),
        V(two + (2, U, 128), F32), V(two + (U, 128), BF), V(two + (2, U, 128), F32), V(two + (U, 128), BF),
        pltpu.SemaphoreType.DMA((12, 2, 3, 2)), pltpu.SemaphoreType.DMA((12, 2, 3, 2)), pltpu.SemaphoreType.DMA((14, 2, 3)),
    ]
    assert len(comm_scratch) == COMM_SCRATCH
    task_scratch = [
        V((TOKENS, D), BF), V((TOKENS, D), BF), V((2, D, 1024), BF), V((2, 512, D), BF),
        V((TOKENS, FF), BF), V((2, TOKENS, 1024), BF), V((TOKENS, D), F32), V((4, 4, 4, 256, 128), BF), pltpu.SemaphoreType.DMA((2, 11)),
    ]
    units = jax.ShapeDtypeStruct((4, 4, 4, ROWS, 128), BF)
    outs = pl.pallas_call(
        whole_kernel,
        out_shape=(units, *(jax.ShapeDtypeStruct(t.shape, F32) for t in moments), units, jax.ShapeDtypeStruct(x.shape, BF), jax.ShapeDtypeStruct((8, TOKENS, 1024), BF)),
        in_specs=[hbm] * 11,
        out_specs=(hbm,) * 10,
        scratch_shapes=comm_scratch + task_scratch,
        compiler_params=pltpu.CompilerParams(collective_id=0, has_side_effects=True, vmem_limit_bytes=67043328),
        name="whole_step",
    )(x, dy, *params, *moments)
    return outs[0], outs[1:7]


UNPACK = 8


def unpack_kernel(first, second, third, gate, up, down):
    low = lax.broadcasted_iota(jnp.int32, (8, 128), 0) < 4

    def of_device(d):
        for ct in range(10):
            down[0, pl.ds(pl.multiple_of(64 * d, 64), 64), ct * 128 : ct * 128 + 128] = third[d, 64 * ct : 64 * ct + 64, :]

    loop(UNPACK, of_device)

    def slab(n):
        rows = pl.ds(pl.multiple_of(80 * n, 16), 80)
        for at, ref in ((0, first), (2048, second)):
            units = [ref[d, rows, :].astype(F32) for d in range(UNPACK)]
            for ct in range(2):
                own = [u[40 * ct : 40 * ct + 40] for u in units]
                tile = pl.ds(pl.multiple_of(n * 256 + at + ct * 128, 128), 128)
                for which, out in enumerate((gate, up)):
                    parts = []
                    for even, odd in zip(own[::2], own[1::2], strict=True):
                        left, right = even[32:40], odd[32:40]
                        if which == 0:
                            right = pltpu.roll(right, 4, 0)
                        else:
                            left = pltpu.roll(left, 4, 0)
                        parts += [even[16 * which : 16 * which + 16], jnp.where(low, left, right), odd[16 * which : 16 * which + 16]]
                    out[0, :, tile] = jnp.concatenate(parts, 0).astype(BF)

    loop(8, slab)


def unpack(wall):
    shapes = ((2, D, FF), (2, D, FF), (2, FF, D))
    blocks = 64 // UNPACK
    return pl.pallas_call(
        unpack_kernel,
        grid=(2, blocks),
        out_shape=tuple(jax.ShapeDtypeStruct(s, BF) for s in shapes),
        in_specs=[pl.BlockSpec((UNPACK, 640, 128), functools.partial(lambda third, l, i: (i, 3 * l + third, 0), third)) for third in range(3)],
        out_specs=tuple(pl.BlockSpec((1, s[1] // blocks, s[2]), lambda l, i: (1 - l, i, 0)) for s in shapes),
        cost_estimate=pl.CostEstimate(flops=10**6, bytes_accessed=126 * 10**6, transcendentals=0),
        name="unpack",
    )(wall, wall, wall)


def solution(mesh):
    def step(x, dy, *arrays):
        wall, moments = whole_step(x[0], dy[0], arrays[:3], arrays[3:])
        return (*unpack(wall.reshape(64, ROWS, 128)), *moments)

    seq, whole, rows = P(("rep", "dp")), P(), P(None, "dp", None)
    return jax.shard_map(
        step,
        mesh=mesh,
        in_specs=(seq, seq) + (whole,) * 3 + (rows,) * 6,
        out_specs=(P("rep"),) * 3 + (P("rep", "dp", None),) * 6,
        check_vma=False,
    )
```

```python
import functools

import jax
import jax.numpy as jnp
from jax import lax
from jax.experimental import pallas as pl
from jax.experimental.pallas import tpu as pltpu
from jax.sharding import PartitionSpec as P

AXES = ("x", "y", "z")
STRIDE = {"x": 16, "y": 4, "z": 1}
ORDERS = (("x", "y", "z"), ("y", "z", "x"), ("z", "x", "y"))
BF, F32 = jnp.bfloat16, jnp.float32
D, FF, TOKENS = 1280, 4096, 1024
ROWS = 3840
U, SUPER = 80, 16

MIDDLE = "DAADAEAAAAA"
CUTS = (2, 3, 4, 4, 5, 8, 12, 14, 18, 21, 24, 25, 27, 28, 29, 33, 35, 39, 42, 46, 49, 53, 56, 60, 61, 62, 63)
LAYER = 24 + len(MIDDLE) + 1
ITEMS = LAYER + 27


def entries():
    rows = {"W": 80, "D": 256, "E": 128}
    items = "PWW" * 8 + MIDDLE + "X" + "PWW" * 8 + "DDE"
    made, steps, step = 0, [], 0
    while len(steps) < SUPER:
        first, last = ((0, *CUTS)[step], CUTS[step]) if step < len(CUTS) else (ITEMS, ITEMS)
        made += sum(rows.get(item, 0) for item in items[first:last])
        if made >= 3 * U * (len(steps) + 1):
            steps.append(step)
        step += 1
    return tuple(steps)


ENTRIES = entries()


def lookup(step, values):
    out = values[0]
    for i in range(1, len(values)):
        if values[i] != values[i - 1]:
            out = out + jnp.where(step >= i, values[i] - values[i - 1], 0)
    return out


def entered(step):
    return sum(jnp.where(step > entry, 1, 0) for entry in ENTRIES)


def dot(a, b, dims):
    return lax.dot_general(a, b, (dims, ((), ())), preferred_element_type=F32)


def loop(n, body, unroll=1):
    lax.fori_loop(0, n, lambda i, _: (body(i), None)[1], None, unroll=unroll)


def start(copies):
    for copy in copies:
        copy.start()


def wait(copies):
    for copy in copies:
        copy.wait()


class Refs:
    def __init__(self, operands, buffers):
        self.x, self.dy, self.wg, self.wu, self.wd, self.h, self.kept = operands
        self.a, self.d, self.ws, self.wds, self.p, self.dgu, self.da, self.out, self.sem = buffers
        self.state = self.p.at[:, FF - D :]

    def slabs(self, i):
        slot, layer = i % 2, (i // 8 + 1) // 2 % 2
        pairs = [(self.wd.at[layer, pl.ds(pl.multiple_of(i % 8 * 512, 512), 512), :], self.wds.at[slot])]
        for n in range(4):
            cols = pl.ds(pl.multiple_of(i % 8 * 512 + n // 2 * 256, 256), 256)
            pairs.append(((self.wg, self.wu)[n % 2].at[layer, :, cols], self.ws.at[slot, :, 256 * n : 256 * n + 256]))
        return [pltpu.make_async_copy(src, dst, self.sem.at[slot, n]) for n, (src, dst) in enumerate(pairs)]

    def next_slabs(self, i):
        wait(self.slabs(i))

        @pl.when(i < 31)
        def _():
            start(self.slabs(i + 1))

    def copy(self, n, src, dst):
        return [pltpu.make_async_copy(src, dst, self.sem.at[n // 6, 5 + n % 6])]

    def load_x(self):
        return self.copy(0, self.x, self.state)

    def load_dy(self):
        return self.copy(1, self.dy, self.d)

    def keep_h(self):
        return self.copy(2, self.state, self.h)

    def back_h(self):
        return self.copy(3, self.h, self.state)

    def load_a(self):
        return self.copy(4, self.x, self.a)

    def keep(self, f):
        return self.copy(5 + f % 2, self.dgu.at[f % 2], self.kept.at[f])

    def back(self, f):
        return self.copy(7 + f % 2, self.kept.at[f], self.dgu.at[f % 2])

    def put(self, g, row, n, at=0, sem=0):
        return self.copy(9 + sem, self.out.at[:, :, :, pl.ds(pl.multiple_of(at, 16), n), :], g.at[:, :, :, pl.ds(pl.multiple_of(row, 16), n), :])


def normed(h):
    wide = h.astype(F32)
    return (wide * lax.rsqrt(jnp.mean(wide * wide, -1, keepdims=True) + 1e-6)).astype(BF)


def token_blocks(size, body, unrolled=False):
    if unrolled:
        for t in range(TOKENS // size):
            body(pl.ds(t * size, size))
    else:
        loop(TOKENS // size, lambda t: body(pl.ds(pl.multiple_of(t * size, size), size)))


def add_to(ref, rows, first, more):
    @pl.when(first)
    def _():
        ref[rows, :] = more

    @pl.when(jnp.logical_not(first))
    def _():
        ref[rows, :] += more


def gate_and_up(r, rows, b, half):
    both = dot(r.a[rows, :], r.ws[b, :, 512 * half : 512 * half + 512], ((1,), (0,)))
    return both[:, :256], both[:, 256:]


def forward(r):
    start(r.load_x() + r.slabs(0) + r.load_dy())
    wait(r.load_x())

    def norm(rows):
        r.a[rows, :] = normed(r.state[rows, :])

    token_blocks(128, norm)

    def task(f):
        r.next_slabs(f)
        b = f % 2

        def block(rows):
            p = []
            for half in range(2):
                gate, up = gate_and_up(r, rows, b, half)
                p.append((gate * jax.nn.sigmoid(gate) * up).astype(BF))
            add_to(r.da, rows, f == 0, dot(jnp.concatenate(p, 1), r.wds[b], ((1,), (0,))))

        token_blocks(512, block, True)

    with jax.named_scope("forward"):
        loop(8, task)

    def end(rows):
        h = (r.state[rows, :].astype(F32) + r.da[rows, :].astype(BF).astype(F32)).astype(BF)
        r.state[rows, :] = h
        r.a[rows, :] = normed(h)

    token_blocks(128, end)
    start(r.keep_h())
    wait(r.load_dy())


def do_item(r, g, i):
    slot = jnp.where(i >= LAYER, 1, 0)
    at = i - LAYER * slot

    @pl.when(at < 24)
    def _():
        f, part = at // 3, at % 3

        @pl.when(part == 0)
        def _():
            @pl.when(i == 3)
            def _():
                wait(r.keep_h())

            with jax.named_scope("hidden"):
                hidden_task(r, slot, f)

        @pl.when(part > 0)
        def _():
            with jax.named_scope("columns"):
                columns_task(r, g, slot, 2 * f + part - 1)

    @pl.when(i == 24)
    def _():
        start(r.load_a())
        wait(r.keep(7))
        start(r.back(0))
        start(r.back(1))

    downs = [at for at, kind in enumerate(MIDDLE) if kind != "A"]
    t = jnp.where(slot == 1, at - 24, sum(jnp.where(at > 24 + d, 1, 0) for d in downs[:2]))
    down = (slot == 1) & (at >= 24)
    for d in downs:
        down = down | ((slot == 0) & (at == 24 + d))

    @pl.when(down & (t < 2))
    def _():
        with jax.named_scope("down512"):
            down_task(r, g, slot, t, 512)

    @pl.when(down & (t == 2))
    def _():
        with jax.named_scope("down256"):
            down_task(r, g, slot, t, 256)

    @pl.when((i >= 24) & (i < LAYER - 1) & jnp.logical_not(down))
    def _():
        with jax.named_scope("da"):
            da_task(r, at - 24 - sum(jnp.where(at > 24 + d, 1, 0) for d in downs))

    @pl.when(i == LAYER - 1)
    def _():
        with jax.named_scope("next"):
            next_layer(r)


def item_done(r, g, i):
    slot = jnp.where(i >= LAYER, 1, 0)
    at = i - LAYER * slot
    n = at // 3 * 2 + at % 3 - 1

    for m in range(3):
        @pl.when((at < 24) & (at % 3 > 0) & (n % 3 == m))
        def _():
            wait(r.put(g, 1920 * slot + 80 * n, 80, 80 * m, m))

    downs = [at for at, kind in enumerate(MIDDLE) if kind != "A"]
    for t in range(3):
        @pl.when(((slot == 0) & (at == 24 + downs[t])) | ((slot == 1) & (at == 24 + t)))
        def _():
            wait(r.put(g, 1920 * slot + 1280 + 256 * t, (256, 256, 128)[t]))


def hidden_task(r, slot, f):
    i = 8 + 16 * slot + f
    b = i % 2
    r.next_slabs(i)

    @pl.when((slot == 0) & (f > 0))
    def _():
        wait(r.keep(f - 1))

    def block(rows):
        dp = dot(r.d[rows, :], r.wds[b], ((1,), (1,))).astype(BF).astype(F32)
        for half in range(2):
            gate, up = gate_and_up(r, rows, b, half)
            sig = jax.nn.sigmoid(gate)
            silu = gate * sig
            d = dp[:, 256 * half : 256 * half + 256]
            r.p[rows, pl.ds(pl.multiple_of(f * 512 + 256 * half, 256), 256)] = (silu * up).astype(BF)
            r.dgu[b, rows, 512 * half : 512 * half + 256] = (d * up * (sig * (1 + gate * (1 - sig)))).astype(BF)
            r.dgu[b, rows, 512 * half + 256 : 512 * half + 512] = (d * silu).astype(BF)

    token_blocks(512, block, True)

    @pl.when(slot == 0)
    def _():
        start(r.keep(f))


def columns_task(r, g, slot, n):
    b, region = n // 2 % 2, n % 3
    cols = pl.ds(pl.multiple_of(n % 2 * 512, 512), 512)

    def gradients(k):
        of_both = dot(r.a[:, k * 640 : k * 640 + 640], r.dgu[b, :, cols], ((0,), (0,)))
        low = lax.broadcasted_iota(jnp.int32, (8, 128), 0) < 4
        for pair in range(16):
            row = 40 * pair
            parts = ([], [])
            for ct in range(2):
                gate, up = (of_both[row : row + 40, at + 128 * ct : at + 128 * ct + 128] for at in (0, 256))
                gm, um = gate[16:24], up[16:24]
                parts[0].extend((gate[:16], up[:16], jnp.where(low, gm, pltpu.roll(um, 4, 0))))
                parts[1].extend((gate[24:], up[24:], jnp.where(low, pltpu.roll(gm, 4, 0), um)))
            for odd in range(2):
                at = (2 * k + pair // 8, pair // 2 % 4, pair % 2 * 2 + odd)
                r.out[at + (pl.ds(pl.multiple_of(80 * region, 16), 80),)] = jnp.concatenate(parts[odd], 0).astype(BF)

    for k in range(2):
        gradients(k)
    for m in range(3):
        @pl.when(region == m)
        def _():
            start(r.put(g, 1920 * slot + 80 * n, 80, 80 * m, m))


def da_task(r, f):
    i = 16 + f
    r.next_slabs(i)
    wait(r.back(f))
    b = i % 2

    def block(rows):
        add_to(r.da, rows, f == 0, dot(r.dgu[b, rows, :], r.ws[b], ((1,), (1,))))

    token_blocks(512, block, True)

    @pl.when(f < 6)
    def _():
        start(r.back(f + 2))


def down_task(r, g, slot, t, width):
    cols = pl.ds(pl.multiple_of(t * 512, 512), width)

    def block(k):
        of_down = dot(r.p[:, pl.ds(pl.multiple_of(k * 512, 512), 512)], r.d[:, cols], ((0,), (0,)))
        for ct in range(width // 128):
            part = of_down[:, 128 * ct : 128 * ct + 128].reshape(2, 4, 64, 128).astype(BF)
            r.out[k // 2, pl.ds(k % 2 * 2, 2), :, 64 * ct : 64 * ct + 64, :] = part

    loop(8, block)
    start(r.put(g, 1920 * slot + 1280 + 256 * t, width // 2))


def next_layer(r):
    start(r.back_h())
    wait(r.back_h())

    def block(rows):
        wide = r.state[rows, :].astype(F32)
        d = r.da[rows, :].astype(BF).astype(F32)
        scale = lax.rsqrt(jnp.mean(wide * wide, -1, keepdims=True) + 1e-6)
        along = jnp.mean(wide * d, -1, keepdims=True)
        through = (scale * d - wide * (scale * scale * scale) * along).astype(BF)
        r.d[rows, :] = (r.d[rows, :].astype(F32) + through.astype(F32)).astype(BF)

    token_blocks(128, block)
    wait(r.load_a())

    def norm(rows):
        r.a[rows, :] = normed(r.a[rows, :])

    token_blocks(128, norm)


def comm_kernel(r, g, params, moments, wall, moments_out,
                recv1, send2, recv2, own, sa, b1s, b1r, b2s, b2r, sb, c1s, c1r, c2s, c2r,
                gm, gw, gn, rows24, dm, dw, dn, wn, ssem, rsem, lsem):
    me = lax.axis_index("dp")
    pos = {"x": me // 16, "y": (me // 4) % 4, "z": me % 4}
    low = (U // 2 + 15) // 16 * 16
    halves = (pl.ds(0, 2), pl.ds(2, 2))
    row_halves = (pl.ds(0, low), pl.ds(low, U - low))

    def peer(axis, by):
        return {"dp": me + ((pos[axis] + by) % 4 - pos[axis]) * STRIDE[axis]}

    barrier = pltpu.get_barrier_semaphore()
    for axis in AXES:
        for by in (1, 3):
            pl.semaphore_signal(barrier, inc=1, device_id=peer(axis, by), device_id_type=pl.DeviceIdType.MESH)
    forward(r)
    pl.semaphore_wait(barrier, 6)

    def part(ref, fixed, rows):
        return ref.at[tuple(fixed.get(axis, slice(None)) for axis in AXES) + (rows, slice(None))]

    def remote(kind, slot, c, way, src, dst, axis):
        return pltpu.make_async_remote_copy(
            src_ref=src, dst_ref=dst, send_sem=ssem.at[kind, slot, c, way], recv_sem=rsem.at[kind, slot, c, way],
            device_id=peer(axis, (1, 3)[way]), device_id_type=pl.DeviceIdType.MESH)

    def local(kind, slot, c, src, dst):
        return pltpu.make_async_copy(src, dst, lsem.at[kind, slot, c])

    class Chunk:
        def __init__(self, c, j):
            self.c, self.slot = c, j % 2
            self.A, self.B, self.C = ORDERS[c]
            self.rest = tuple(axis for axis in AXES if axis != self.A)
            self.ib = self.rest.index(self.B)
            self.rows = pl.ds(pl.multiple_of((3 * j + c) * U, 16), U)
            self.k, self.layer = (3 * j + c) % 24, 1 - (3 * j + c) // 24
            self.a, self.b, self.c3 = (pos[axis] for axis in ORDERS[c])

        def unit(self, b, i):
            return (b, i) if self.ib == 0 else (i, b)

        def row_part(self, rows):
            return pl.ds(self.rows.start + rows.start, rows.size)

        def a1(self):
            s, c = self.slot, self.c
            return [remote(0, s, c, way, part(g, {self.A: (self.a + 2) % 4, self.rest[0]: halves[way]}, self.rows),
                           recv1.at[s, c, halves[way]], self.A) for way in (0, 1)]

        def load2(self):
            s, c = self.slot, self.c
            return [local(way, s, c, part(g, {self.A: (self.a + (1, 3)[way]) % 4}, self.rows), send2.at[s, c, way]) for way in (0, 1)]

        def load_own(self):
            return [local(2, self.slot, self.c, part(g, {self.A: self.a}, self.rows), own.at[self.slot, self.c])]

        def a2(self):
            s, c = self.slot, self.c
            return [remote(1, s, c, way, send2.at[s, c, way], recv2.at[s, c, way], self.A) for way in (0, 1)]

        def b1(self):
            s, c = self.slot, self.c
            return [remote(2, s, c, way, b1s.at[s, c, halves[way]], b1r.at[s, c, halves[way]], self.B) for way in (0, 1)]

        def b2(self):
            s, c = self.slot, self.c
            return [remote(3, s, c, way, b2s.at[s, c, way], b2r.at[s, c, way], self.B) for way in (0, 1)]

        def c1(self):
            s, c = self.slot, self.c
            return [remote(4, s, c, way, c1s.at[s, c, row_halves[way]], c1r.at[s, c, row_halves[way]], self.C) for way in (0, 1)]

        def c2(self):
            s, c = self.slot, self.c
            return [remote(5, s, c, way, c2s.at[s, c, way], c2r.at[s, c, way], self.C) for way in (0, 1)]

        def of_columns(self, out):
            s, c = self.slot, self.c
            cols = pl.ds(pl.multiple_of(self.k * 256, 256), 256)
            pairs = []
            for i in range(4):
                which = i // 2 * 3 + i % 2
                if out:
                    pairs.append((gn.at[s, c, i], moments_out[which].at[self.layer, :, cols]))
                else:
                    pairs.append((moments[which].at[self.layer, :, cols], gm.at[s, c, i]))
            if not out:
                rows = pl.ds(pl.multiple_of(me // 2 * 40, 8), 40)
                pairs += [(params[i].at[self.layer, rows, cols], gw.at[s, c, i]) for i in range(2)]
            return [local((10 if out else 3) + i, s, c, *pair) for i, pair in enumerate(pairs)]

        def of_down(self, out, q):
            s, c = self.slot, self.c
            tile = 5 * (self.k - 16) // 4
            pairs = []
            for n, (first, rows, at) in enumerate(((16 * q, 64 - 16 * q, 0), (0, 16 + 16 * q, 64 - 16 * q))):
                cols = pl.ds(pl.multiple_of((tile + n) * 128, 128), 128)
                there, here = pl.ds(first, rows), pl.ds(at, rows)
                for i in range(2):
                    if out:
                        pairs.append((dn.at[s, c, i, here], moments_out[3 * i + 2].at[self.layer, there, cols]))
                    else:
                        pairs.append((moments[3 * i + 2].at[self.layer, there, cols], dm.at[s, c, i, here]))
                if not out:
                    mine = pl.ds(pl.multiple_of(me * 64 + first, 16), rows)
                    pairs.append((params[2].at[self.layer, mine, cols], dw.at[s, c, here]))
            return [local((10 if out else 3) + i, s, c, *pair) for i, pair in enumerate(pairs)]

        def step_copies(self, out, act):
            @pl.when(self.k < 16)
            def _():
                act(self.of_columns(out))

            for q in range(4):
                @pl.when((self.k >= 16) & (self.k % 4 == q))
                def _():
                    act(self.of_down(out, q))

        def store_new(self):
            mine = part(wall, {self.A: self.a, self.B: self.b, self.C: self.c3}, self.rows)
            return [local(9, self.slot, self.c, wn.at[self.slot, self.c], mine)]

        def gather(self, which):
            s, c = self.slot, self.c
            if which < 2:
                axis, here, fixed, kind = self.C, self.c3, {self.A: self.a, self.B: self.b}, 6
            elif which < 4:
                axis, here, fixed, kind = self.B, self.b, {self.A: self.a}, 8
            else:
                axis, here, fixed, kind = self.A, self.a, {}, 10
            if which % 2 == 0:
                block = part(wall, fixed | {axis: here}, self.rows)
                src = wn.at[s, c] if which == 0 else block
                return [remote(kind, s, c, way, src, block, axis) for way in (0, 1)]
            out = []
            for way in (0, 1):
                block = fixed | {axis: (here + (3, 1)[way]) % 4}
                rows = self.rows
                if which == 1:
                    rows = self.row_part(row_halves[way])
                elif which == 3:
                    block[self.C] = halves[way]
                else:
                    block[self.rest[0]] = halves[way]
                half = part(wall, block, rows)
                out.append(remote(kind + 1, s, c, way, half, half, axis))
            return out

    def stage0(k):
        start(k.a1())
        start(k.load2())

    def stage1(k):
        wait(k.load2())
        wait(k.a1())
        s, c = k.slot, k.c

        def body(i):
            for way in (0, 1):
                at = (s, c, 2 * way + i // 4, i % 4)
                to = (s, c, way, 2 * way + i // 4, i % 4)
                send2[to] = (send2[to].astype(F32) + recv1[at].astype(F32)).astype(BF)

        loop(8, body)
        start(k.a2())
        start(k.load_own())

    def stage2(k):
        wait(k.load_own())
        wait(k.a2())
        s, c = k.slot, k.c

        def body(i):
            at = (i // 4, i % 4)
            total = own[(s, c) + at].astype(F32) + recv2[(s, c, 0) + at].astype(F32) + recv2[(s, c, 1) + at].astype(F32)
            sa[(s, c) + at] = total

        loop(16, body)
        far = (k.b + 2) % 4

        def pack(i):
            b1s[s, c, i] = sa[(s, c) + k.unit(far, i)].astype(BF)

        loop(4, pack)
        start(k.b1())

    def stage3(k):
        wait(k.b1())
        s, c = k.slot, k.c
        near = ((k.b + 1) % 4, (k.b + 3) % 4)

        def body(i):
            for way in (0, 1):
                b2s[s, c, way, 2 * way + i] = (sa[(s, c) + k.unit(near[way], 2 * way + i)] + b1r[s, c, 2 * way + i].astype(F32)).astype(BF)
                b2s[s, c, way, 2 - 2 * way + i] = sa[(s, c) + k.unit(near[way], 2 - 2 * way + i)].astype(BF)

        loop(2, body)
        start(k.b2())

    def stage4(k):
        wait(k.b2())
        s, c = k.slot, k.c

        def body(i):
            sb[s, c, i] = sa[(s, c) + k.unit(k.b, i)] + b2r[s, c, 0, i].astype(F32) + b2r[s, c, 1, i].astype(F32)

        loop(4, body)
        c1s[s, c] = sb[s, c, (k.c3 + 2) % 4].astype(BF)
        start(k.c1())

    def stage5(k):
        wait(k.c1())
        s, c = k.slot, k.c
        near = ((k.c3 + 1) % 4, (k.c3 + 3) % 4)
        for way in (0, 1):
            add, keep = row_halves[way], row_halves[1 - way]
            c2s[s, c, way, add] = (sb[s, c, near[way], add] + c1r[s, c, add].astype(F32)).astype(BF)
            c2s[s, c, way, keep] = sb[s, c, near[way], keep].astype(BF)
        start(k.c2())
        k.step_copies(False, start)

    def adamw(old, first, second, grad):
        first = 0.9 * first + 0.1 * grad
        second = 0.95 * second + 0.05 * grad * grad
        return old - 0.02 * (first * lax.rsqrt(second + 1e-8) + 0.1 * old), first, second

    def step_columns(k, grad):
        s, c = k.slot, k.c
        low = lax.broadcasted_iota(jnp.int32, (8, 128), 0) < 4
        odd = me % 2 == 1
        unit = []
        for ct in range(2):
            tile = slice(128 * ct, 128 * ct + 128)
            mix = grad[40 * ct + 32 : 40 * ct + 40]
            turned = pltpu.roll(mix, 4, 0)
            whole, left = [], []
            for i in range(2):
                rest = jnp.where(odd, (turned, mix)[i], (mix, turned)[i])
                rows = jnp.concatenate([grad[40 * ct + 16 * i : 40 * ct + 16 * i + 16], rest], 0)
                rows = jnp.where(odd, pltpu.roll(rows, 4, 0), rows)
                pair = gw[s, c, i, :, tile].astype(F32)
                old = jnp.where(odd, pltpu.roll(pair[16:40], 20, 0), pair[0:24])
                new, first, second = adamw(old[:20], gm[s, c, i, :, tile], gm[s, c, 2 + i, :, tile], rows[:20])
                gn[s, c, i, :, tile] = first
                gn[s, c, 2 + i, :, tile] = second
                rows24[ct, i, 0:20] = new
                new = rows24[ct, i]
                new = jnp.where(odd, pltpu.roll(new, 20, 0), new)
                whole.append(new[:16])
                turn = pltpu.roll(new[16:], 4, 0)
                left.append(jnp.where(odd, (turn, new[16:])[i], (new[16:], turn)[i]))
            unit += whole + [jnp.where(low, *left)]
        wn[s, c] = jnp.concatenate(unit, 0).astype(BF)

    def stage6(k):
        k.step_copies(False, wait)
        wait(k.c2())
        s, c = k.slot, k.c
        total = sb[s, c, k.c3] + c2r[s, c, 0].astype(F32) + c2r[s, c, 1].astype(F32)
        grad = total.astype(BF).astype(F32)

        @pl.when(k.k < 16)
        def _():
            step_columns(k, grad)

        @pl.when(k.k >= 16)
        def _():
            new, dn[s, c, 0], dn[s, c, 1] = adamw(dw[s, c].astype(F32), dm[s, c, 0], dm[s, c, 1], grad)
            wn[s, c] = new.astype(BF)

        start(k.gather(0))
        start(k.store_new())
        k.step_copies(True, start)

    def stage7(k):
        wait(k.gather(0))
        start(k.gather(1))

    def stage8(k):
        wait(k.store_new())
        k.step_copies(True, wait)
        wait(k.gather(1))
        start(k.gather(2))

    def later(n):
        def stage(k):
            wait(k.gather(n - 1))
            start(k.gather(n))
        return stage

    def stage12(k):
        wait(k.gather(5))

    stages = (stage0, stage1, stage2, stage3, stage4, stage5, stage6, stage7, stage8, later(3), later(4), later(5), stage12)

    def step(now):
        first, last = lookup(now, (0, *CUTS)), lookup(now, CUTS)
        lax.fori_loop(first, last, lambda i, _: do_item(r, g, i), None)
        before = [entered(now + 1 - k) for k in range(len(stages) + 1)]
        for number in reversed(range(len(stages))):
            if number == 0:
                lax.fori_loop(first, last, lambda i, _: item_done(r, g, i), None)

            @pl.when(before[number] > before[number + 1])
            def _():
                with jax.named_scope(f"stage{number}"):
                    for c in range(3):
                        stages[number](Chunk(c, before[number + 1]))

    loop(ENTRIES[-1] + len(stages), step)


def whole_kernel(*refs):
    (x, dy), params, moments = refs[:2], refs[2:5], refs[5:11]
    wall, moments_out, g, kept = refs[11], refs[12:18], refs[18], refs[19:21]
    scratch, n = refs[21:], COMM_SCRATCH
    comm_kernel(Refs((x, dy, *params, *kept), scratch[n:]), g, params, moments, wall, moments_out, *scratch[:n])


COMM_SCRATCH = 25


def whole_step(x, dy, params, moments):
    hbm = pl.BlockSpec(memory_space=pl.ANY)
    V, two = pltpu.VMEM, (2, 3)
    comm_scratch = [
        V(two + (4, 4, U, 128), BF), V(two + (2, 4, 4, U, 128), BF), V(two + (2, 4, 4, U, 128), BF), V(two + (4, 4, U, 128), BF),
        V(two + (4, 4, U, 128), F32),
        V(two + (4, U, 128), BF), V(two + (4, U, 128), BF), V(two + (2, 4, U, 128), BF), V(two + (2, 4, U, 128), BF), V(two + (4, U, 128), F32),
        V(two + (U, 128), BF), V(two + (U, 128), BF), V(two + (2, U, 128), BF), V(two + (2, U, 128), BF),
        V(two + (4, 20, 256), F32), V(two + (2, 40, 256), BF), V(two + (4, 20, 256), F32), V((2, 2, 24, 128), F32),
        V(two + (2, U, 128), F32), V(two + (U, 128), BF), V(two + (2, U, 128), F32), V(two + (U, 128), BF),
        pltpu.SemaphoreType.DMA((12, 2, 3, 2)), pltpu.SemaphoreType.DMA((12, 2, 3, 2)), pltpu.SemaphoreType.DMA((14, 2, 3)),
    ]
    assert len(comm_scratch) == COMM_SCRATCH
    task_scratch = [
        V((TOKENS, D), BF), V((TOKENS, D), BF), V((2, D, 1024), BF), V((2, 512, D), BF),
        V((TOKENS, FF), BF), V((2, TOKENS, 1024), BF), V((TOKENS, D), F32), V((4, 4, 4, 256, 128), BF), pltpu.SemaphoreType.DMA((2, 11)),
    ]
    units = jax.ShapeDtypeStruct((4, 4, 4, ROWS, 128), BF)
    outs = pl.pallas_call(
        whole_kernel,
        out_shape=(units, *(jax.ShapeDtypeStruct(t.shape, F32) for t in moments), units, jax.ShapeDtypeStruct(x.shape, BF), jax.ShapeDtypeStruct((8, TOKENS, 1024), BF)),
        in_specs=[hbm] * 11,
        out_specs=(hbm,) * 10,
        scratch_shapes=comm_scratch + task_scratch,
        compiler_params=pltpu.CompilerParams(collective_id=0, has_side_effects=True, vmem_limit_bytes=67043328),
        name="whole_step",
    )(x, dy, *params, *moments)
    return outs[0], outs[1:7]


UNPACK = 8


def unpack_kernel(first, second, third, gate, up, down):
    low = lax.broadcasted_iota(jnp.int32, (8, 128), 0) < 4

    def of_device(d):
        for ct in range(10):
            down[0, pl.ds(pl.multiple_of(64 * d, 64), 64), ct * 128 : ct * 128 + 128] = third[d, 64 * ct : 64 * ct + 64, :]

    loop(UNPACK, of_device)

    def slab(n):
        rows = pl.ds(pl.multiple_of(80 * n, 16), 80)
        for at, ref in ((0, first), (2048, second)):
            units = [ref[d, rows, :].astype(F32) for d in range(UNPACK)]
            for ct in range(2):
                own = [u[40 * ct : 40 * ct + 40] for u in units]
                tile = pl.ds(pl.multiple_of(n * 256 + at + ct * 128, 128), 128)
                for which, out in enumerate((gate, up)):
                    parts = []
                    for even, odd in zip(own[::2], own[1::2], strict=True):
                        left, right = even[32:40], odd[32:40]
                        if which == 0:
                            right = pltpu.roll(right, 4, 0)
                        else:
                            left = pltpu.roll(left, 4, 0)
                        parts += [even[16 * which : 16 * which + 16], jnp.where(low, left, right), odd[16 * which : 16 * which + 16]]
                    out[0, :, tile] = jnp.concatenate(parts, 0).astype(BF)

    loop(8, slab)


def unpack(wall):
    shapes = ((2, D, FF), (2, D, FF), (2, FF, D))
    blocks = 64 // UNPACK
    return pl.pallas_call(
        unpack_kernel,
        grid=(2, blocks),
        out_shape=tuple(jax.ShapeDtypeStruct(s, BF) for s in shapes),
        in_specs=[pl.BlockSpec((UNPACK, 640, 128), functools.partial(lambda third, l, i: (i, 3 * l + third, 0), third)) for third in range(3)],
        out_specs=tuple(pl.BlockSpec((1, s[1] // blocks, s[2]), lambda l, i: (1 - l, i, 0)) for s in shapes),
        cost_estimate=pl.CostEstimate(flops=10**6, bytes_accessed=126 * 10**6, transcendentals=0),
        name="unpack",
    )(wall, wall, wall)


def solution(mesh):
    def step(x, dy, *arrays):
        wall, moments = whole_step(x[0], dy[0], arrays[:3], arrays[3:])
        return (*unpack(wall.reshape(64, ROWS, 128)), *moments)

    seq, whole, rows = P(("rep", "dp")), P(), P(None, "dp", None)
    return jax.shard_map(
        step,
        mesh=mesh,
        in_specs=(seq, seq) + (whole,) * 3 + (rows,) * 6,
        out_specs=(P("rep"),) * 3 + (P("rep", "dp", None),) * 6,
        check_vma=False,
    )
```

```python
import functools

import jax
import jax.numpy as jnp
from jax import lax
from jax.experimental import pallas as pl
from jax.experimental.pallas import tpu as pltpu
from jax.sharding import PartitionSpec as P

AXES = ("x", "y", "z")
STRIDE = {"x": 16, "y": 4, "z": 1}
ORDERS = (("x", "y", "z"), ("y", "z", "x"), ("z", "x", "y"))
BF, F32 = jnp.bfloat16, jnp.float32
D, FF, TOKENS = 1280, 4096, 1024
ROWS = 3840
U, SUPER = 80, 16

MIDDLE = "DADAAAAEAAA"
CUTS = (1, 4, 5, 8, 12, 14, 18, 21, 23, 24, 25, 26, 27, 29, 32, 34, 38, 42, 45, 49, 53, 57, 60, 61, 62, 63)
LAYER = 24 + len(MIDDLE) + 1
ITEMS = LAYER + 27


def entries():
    rows = {"W": 80, "D": 256, "E": 128}
    items = "PWW" * 8 + MIDDLE + "X" + "PWW" * 8 + "DDE"
    made, steps, step = 0, [], 0
    while len(steps) < SUPER:
        first, last = ((0, *CUTS)[step], CUTS[step]) if step < len(CUTS) else (ITEMS, ITEMS)
        made += sum(rows.get(item, 0) for item in items[first:last])
        if made >= 3 * U * (len(steps) + 1):
            steps.append(step)
        step += 1
    return tuple(steps)


ENTRIES = entries()


def lookup(step, values):
    out = values[0]
    for i in range(1, len(values)):
        if values[i] != values[i - 1]:
            out = out + jnp.where(step >= i, values[i] - values[i - 1], 0)
    return out


def entered(step):
    return sum(jnp.where(step > entry, 1, 0) for entry in ENTRIES)


def dot(a, b, dims):
    return lax.dot_general(a, b, (dims, ((), ())), preferred_element_type=F32)


def loop(n, body, unroll=1):
    lax.fori_loop(0, n, lambda i, _: (body(i), None)[1], None, unroll=unroll)


def start(copies):
    for copy in copies:
        copy.start()


def wait(copies):
    for copy in copies:
        copy.wait()


class Refs:
    def __init__(self, operands, buffers):
        self.x, self.dy, self.wg, self.wu, self.wd, self.h, self.kept = operands
        self.a, self.d, self.ws, self.wds, self.p, self.dgu, self.da, self.out, self.sem = buffers
        self.state = self.p.at[:, FF - D :]

    def slabs(self, i):
        slot, layer = i % 2, (i // 8 + 1) // 2 % 2
        pairs = [(self.wd.at[layer, pl.ds(pl.multiple_of(i % 8 * 512, 512), 512), :], self.wds.at[slot])]
        for n in range(4):
            cols = pl.ds(pl.multiple_of(i % 8 * 512 + n // 2 * 256, 256), 256)
            pairs.append(((self.wg, self.wu)[n % 2].at[layer, :, cols], self.ws.at[slot, :, 256 * n : 256 * n + 256]))
        return [pltpu.make_async_copy(src, dst, self.sem.at[slot, n]) for n, (src, dst) in enumerate(pairs)]

    def next_slabs(self, i):
        wait(self.slabs(i))

        @pl.when(i < 31)
        def _():
            start(self.slabs(i + 1))

    def copy(self, n, src, dst):
        return [pltpu.make_async_copy(src, dst, self.sem.at[n // 6, 5 + n % 6])]

    def load_x(self):
        return self.copy(0, self.x, self.state)

    def load_dy(self):
        return self.copy(1, self.dy, self.d)

    def keep_h(self):
        return self.copy(2, self.state, self.h)

    def back_h(self):
        return self.copy(3, self.h, self.state)

    def load_a(self):
        return self.copy(4, self.x, self.a)

    def keep(self, f):
        return self.copy(5 + f % 2, self.dgu.at[f % 2], self.kept.at[f])

    def back(self, f):
        return self.copy(7 + f % 2, self.kept.at[f], self.dgu.at[f % 2])

    def put(self, g, row, n, at=0, sem=0):
        return self.copy(9 + sem, self.out.at[:, :, :, pl.ds(pl.multiple_of(at, 16), n), :], g.at[:, :, :, pl.ds(pl.multiple_of(row, 16), n), :])


def normed(h):
    wide = h.astype(F32)
    return (wide * lax.rsqrt(jnp.mean(wide * wide, -1, keepdims=True) + 1e-6)).astype(BF)


def token_blocks(size, body, unrolled=False):
    if unrolled:
        for t in range(TOKENS // size):
            body(pl.ds(t * size, size))
    else:
        loop(TOKENS // size, lambda t: body(pl.ds(pl.multiple_of(t * size, size), size)))


def add_to(ref, rows, cols, first, more):
    ref[rows, cols] = jnp.where(first, more, ref[rows, cols] + more)


PARTS = (slice(0, 1024), slice(1024, D))


def gate_and_up(r, rows, b, half):
    both = dot(r.a[rows, :], r.ws[b, :, 512 * half : 512 * half + 512], ((1,), (0,)))
    return both[:, :256], both[:, 256:]


def forward(r):
    start(r.load_x() + r.slabs(0) + r.load_dy())
    wait(r.load_x())

    def norm(rows):
        r.a[rows, :] = normed(r.state[rows, :])

    token_blocks(128, norm)

    def task(f):
        r.next_slabs(f)
        b = f % 2

        def block(rows):
            p = []
            for half in range(2):
                gate, up = gate_and_up(r, rows, b, half)
                p.append((gate * jax.nn.sigmoid(gate) * up).astype(BF))
            p = jnp.concatenate(p, 1)
            for cols in PARTS:
                add_to(r.da, rows, cols, f == 0, dot(p, r.wds[b, :, cols], ((1,), (0,))))

        token_blocks(512, block, True)

    with jax.named_scope("forward"):
        loop(8, task)

    def end(rows):
        h = (r.state[rows, :].astype(F32) + r.da[rows, :].astype(BF).astype(F32)).astype(BF)
        r.state[rows, :] = h
        r.a[rows, :] = normed(h)

    token_blocks(128, end)
    start(r.keep_h())
    wait(r.load_dy())


def do_item(r, g, i):
    slot = jnp.where(i >= LAYER, 1, 0)
    at = i - LAYER * slot

    @pl.when(at < 24)
    def _():
        f, part = at // 3, at % 3

        @pl.when(part == 0)
        def _():
            @pl.when(i == 3)
            def _():
                wait(r.keep_h())

            with jax.named_scope("hidden"):
                hidden_task(r, slot, f)

        @pl.when(part > 0)
        def _():
            with jax.named_scope("columns"):
                columns_task(r, g, slot, 2 * f + part - 1)

    @pl.when(i == 24)
    def _():
        start(r.load_a())
        wait(r.keep(7))
        start(r.back(0))
        start(r.back(1))

    downs = [at for at, kind in enumerate(MIDDLE) if kind != "A"]
    t = jnp.where(slot == 1, at - 24, sum(jnp.where(at > 24 + d, 1, 0) for d in downs[:2]))
    down = (slot == 1) & (at >= 24)
    for d in downs:
        down = down | ((slot == 0) & (at == 24 + d))

    @pl.when(down & (t < 2))
    def _():
        with jax.named_scope("down512"):
            down_task(r, g, slot, t, 512)

    @pl.when(down & (t == 2))
    def _():
        with jax.named_scope("down256"):
            down_task(r, g, slot, t, 256)

    @pl.when((i >= 24) & (i < LAYER - 1) & jnp.logical_not(down))
    def _():
        with jax.named_scope("da"):
            da_task(r, at - 24 - sum(jnp.where(at > 24 + d, 1, 0) for d in downs))

    @pl.when(i == LAYER - 1)
    def _():
        with jax.named_scope("next"):
            next_layer(r)


def item_done(r, g, i):
    slot = jnp.where(i >= LAYER, 1, 0)
    at = i - LAYER * slot
    n = at // 3 * 2 + at % 3 - 1

    for m in range(3):
        @pl.when((at < 24) & (at % 3 > 0) & (n % 3 == m))
        def _():
            wait(r.put(g, 1920 * slot + 80 * n, 80, 80 * m, m))

    downs = [at for at, kind in enumerate(MIDDLE) if kind != "A"]
    for t in range(3):
        @pl.when(((slot == 0) & (at == 24 + downs[t])) | ((slot == 1) & (at == 24 + t)))
        def _():
            wait(r.put(g, 1920 * slot + 1280 + 256 * t, (256, 256, 128)[t]))


def hidden_task(r, slot, f):
    i = 8 + 16 * slot + f
    b = i % 2
    r.next_slabs(i)

    @pl.when((slot == 0) & (f > 0))
    def _():
        wait(r.keep(f - 1))

    def block(rows):
        dp = dot(r.d[rows, :], r.wds[b], ((1,), (1,))).astype(BF).astype(F32)
        for half in range(2):
            gate, up = gate_and_up(r, rows, b, half)
            sig = jax.nn.sigmoid(gate)
            silu = gate * sig
            d = dp[:, 256 * half : 256 * half + 256]
            r.p[rows, pl.ds(pl.multiple_of(f * 512 + 256 * half, 256), 256)] = (silu * up).astype(BF)
            r.dgu[b, rows, 512 * half : 512 * half + 256] = (d * up * (sig * (1 + gate * (1 - sig)))).astype(BF)
            r.dgu[b, rows, 512 * half + 256 : 512 * half + 512] = (d * silu).astype(BF)

    token_blocks(512, block, True)

    @pl.when(slot == 0)
    def _():
        start(r.keep(f))


def columns_task(r, g, slot, n):
    b, region = n // 2 % 2, n % 3
    cols = pl.ds(pl.multiple_of(n % 2 * 512, 512), 512)

    def gradients(k):
        of_both = dot(r.a[:, k * 640 : k * 640 + 640], r.dgu[b, :, cols], ((0,), (0,)))
        low = lax.broadcasted_iota(jnp.int32, (8, 128), 0) < 4
        for pair in range(16):
            row = 40 * pair
            parts = ([], [])
            for ct in range(2):
                gate, up = (of_both[row : row + 40, at + 128 * ct : at + 128 * ct + 128] for at in (0, 256))
                gm, um = gate[16:24], up[16:24]
                parts[0].extend((gate[:16], up[:16], jnp.where(low, gm, pltpu.roll(um, 4, 0))))
                parts[1].extend((gate[24:], up[24:], jnp.where(low, pltpu.roll(gm, 4, 0), um)))
            for odd in range(2):
                at = (2 * k + pair // 8, pair // 2 % 4, pair % 2 * 2 + odd)
                r.out[at + (pl.ds(pl.multiple_of(80 * region, 16), 80),)] = jnp.concatenate(parts[odd], 0).astype(BF)

    for k in range(2):
        gradients(k)
    for m in range(3):
        @pl.when(region == m)
        def _():
            start(r.put(g, 1920 * slot + 80 * n, 80, 80 * m, m))


def da_task(r, f):
    i = 16 + f
    r.next_slabs(i)
    wait(r.back(f))
    b = i % 2

    def block(rows):
        for cols in PARTS:
            add_to(r.da, rows, cols, f == 0, dot(r.dgu[b, rows, :], r.ws[b, cols, :], ((1,), (1,))))

    token_blocks(512, block, True)

    @pl.when(f < 6)
    def _():
        start(r.back(f + 2))


def down_task(r, g, slot, t, width):
    cols = pl.ds(pl.multiple_of(t * 512, 512), width)

    for k in range(4):
        of_down = dot(r.p[:, 1024 * k : 1024 * k + 1024], r.d[:, cols], ((0,), (0,)))
        for ct in range(width // 128):
            part = of_down[:, 128 * ct : 128 * ct + 128].reshape(4, 4, 64, 128).astype(BF)
            r.out[k, :, :, 64 * ct : 64 * ct + 64, :] = part

    start(r.put(g, 1920 * slot + 1280 + 256 * t, width // 2))


def next_layer(r):
    start(r.back_h())
    wait(r.back_h())

    def block(rows):
        wide = r.state[rows, :].astype(F32)
        d = r.da[rows, :].astype(BF).astype(F32)
        scale = lax.rsqrt(jnp.mean(wide * wide, -1, keepdims=True) + 1e-6)
        along = jnp.mean(wide * d, -1, keepdims=True)
        through = (scale * d - wide * (scale * scale * scale) * along).astype(BF)
        r.d[rows, :] = (r.d[rows, :].astype(F32) + through.astype(F32)).astype(BF)

    token_blocks(128, block)
    wait(r.load_a())

    def norm(rows):
        r.a[rows, :] = normed(r.a[rows, :])

    token_blocks(128, norm)


def comm_kernel(r, g, params, moments, wall, moments_out,
                recv1, send2, recv2, own, sa, b1s, b1r, b2s, b2r, sb, c1s, c1r, c2s, c2r,
                gm, gw, gn, rows24, dm, dw, dn, wn, ssem, rsem, lsem):
    me = lax.axis_index("dp")
    pos = {"x": me // 16, "y": (me // 4) % 4, "z": me % 4}
    low = (U // 2 + 15) // 16 * 16
    halves = (pl.ds(0, 2), pl.ds(2, 2))
    row_halves = (pl.ds(0, low), pl.ds(low, U - low))

    def peer(axis, by):
        return {"dp": me + ((pos[axis] + by) % 4 - pos[axis]) * STRIDE[axis]}

    barrier = pltpu.get_barrier_semaphore()
    for axis in AXES:
        for by in (1, 3):
            pl.semaphore_signal(barrier, inc=1, device_id=peer(axis, by), device_id_type=pl.DeviceIdType.MESH)
    forward(r)
    pl.semaphore_wait(barrier, 6)

    def part(ref, fixed, rows):
        return ref.at[tuple(fixed.get(axis, slice(None)) for axis in AXES) + (rows, slice(None))]

    def remote(kind, slot, c, way, src, dst, axis):
        return pltpu.make_async_remote_copy(
            src_ref=src, dst_ref=dst, send_sem=ssem.at[kind, slot, c, way], recv_sem=rsem.at[kind, slot, c, way],
            device_id=peer(axis, (1, 3)[way]), device_id_type=pl.DeviceIdType.MESH)

    def local(kind, slot, c, src, dst):
        return pltpu.make_async_copy(src, dst, lsem.at[kind, slot, c])

    class Chunk:
        def __init__(self, c, j):
            self.c, self.slot = c, j % 2
            self.A, self.B, self.C = ORDERS[c]
            self.rest = tuple(axis for axis in AXES if axis != self.A)
            self.ib = self.rest.index(self.B)
            self.rows = pl.ds(pl.multiple_of((3 * j + c) * U, 16), U)
            self.k, self.layer = (3 * j + c) % 24, 1 - (3 * j + c) // 24
            self.a, self.b, self.c3 = (pos[axis] for axis in ORDERS[c])

        def unit(self, b, i):
            return (b, i) if self.ib == 0 else (i, b)

        def row_part(self, rows):
            return pl.ds(self.rows.start + rows.start, rows.size)

        def a1(self):
            s, c = self.slot, self.c
            return [remote(0, s, c, way, part(g, {self.A: (self.a + 2) % 4, self.rest[0]: halves[way]}, self.rows),
                           recv1.at[s, c, halves[way]], self.A) for way in (0, 1)]

        def load2(self):
            s, c = self.slot, self.c
            return [local(way, s, c, part(g, {self.A: (self.a + (1, 3)[way]) % 4}, self.rows), send2.at[s, c, way]) for way in (0, 1)]

        def load_own(self):
            return [local(2, self.slot, self.c, part(g, {self.A: self.a}, self.rows), own.at[self.slot, self.c])]

        def a2(self):
            s, c = self.slot, self.c
            return [remote(1, s, c, way, send2.at[s, c, way], recv2.at[s, c, way], self.A) for way in (0, 1)]

        def b1(self):
            s, c = self.slot, self.c
            return [remote(2, s, c, way, b1s.at[s, c, halves[way]], b1r.at[s, c, halves[way]], self.B) for way in (0, 1)]

        def b2(self):
            s, c = self.slot, self.c
            return [remote(3, s, c, way, b2s.at[s, c, way], b2r.at[s, c, way], self.B) for way in (0, 1)]

        def c1(self):
            s, c = self.slot, self.c
            return [remote(4, s, c, way, c1s.at[s, c, row_halves[way]], c1r.at[s, c, row_halves[way]], self.C) for way in (0, 1)]

        def c2(self):
            s, c = self.slot, self.c
            return [remote(5, s, c, way, c2s.at[s, c, way], c2r.at[s, c, way], self.C) for way in (0, 1)]

        def of_columns(self, out):
            s, c = self.slot, self.c
            cols = pl.ds(pl.multiple_of(self.k * 256, 256), 256)
            pairs = []
            for i in range(4):
                which = i // 2 * 3 + i % 2
                if out:
                    pairs.append((gn.at[s, c, i], moments_out[which].at[self.layer, :, cols]))
                else:
                    pairs.append((moments[which].at[:, :, cols], gm.at[s, c, i]))
            if not out:
                rows = pl.ds(pl.multiple_of(me // 2 * 40, 8), 40)
                pairs += [(params[i].at[self.layer, rows, cols], gw.at[s, c, i]) for i in range(2)]
            return [local((10 if out else 3) + i, s, c, *pair) for i, pair in enumerate(pairs)]

        def of_down(self, out, q):
            s, c = self.slot, self.c
            tile = 5 * (self.k - 16) // 4
            pairs = []
            for n, (first, rows, at) in enumerate(((16 * q, 64 - 16 * q, 0), (0, 16 + 16 * q, 64 - 16 * q))):
                cols = pl.ds(pl.multiple_of((tile + n) * 128, 128), 128)
                there, here = pl.ds(first, rows), pl.ds(at, rows)
                for i in range(2):
                    if out:
                        pairs.append((dn.at[s, c, i, here], moments_out[3 * i + 2].at[self.layer, there, cols]))
                    else:
                        pairs.append((moments[3 * i + 2].at[self.layer, there, cols], dm.at[s, c, i, here]))
                if not out:
                    mine = pl.ds(pl.multiple_of(me * 64 + first, 16), rows)
                    pairs.append((params[2].at[self.layer, mine, cols], dw.at[s, c, here]))
            return [local((10 if out else 3) + i, s, c, *pair) for i, pair in enumerate(pairs)]

        def step_copies(self, out, act):
            @pl.when(self.k < 16)
            def _():
                act(self.of_columns(out))

            for q in range(4):
                @pl.when((self.k >= 16) & (self.k % 4 == q))
                def _():
                    act(self.of_down(out, q))

        def store_new(self):
            mine = part(wall, {self.A: self.a, self.B: self.b, self.C: self.c3}, self.rows)
            return [local(9, self.slot, self.c, wn.at[self.slot, self.c], mine)]

        def gather(self, which):
            s, c = self.slot, self.c
            if which < 2:
                axis, here, fixed, kind = self.C, self.c3, {self.A: self.a, self.B: self.b}, 6
            elif which < 4:
                axis, here, fixed, kind = self.B, self.b, {self.A: self.a}, 8
            else:
                axis, here, fixed, kind = self.A, self.a, {}, 10
            if which % 2 == 0:
                block = part(wall, fixed | {axis: here}, self.rows)
                src = wn.at[s, c] if which == 0 else block
                return [remote(kind, s, c, way, src, block, axis) for way in (0, 1)]
            out = []
            for way in (0, 1):
                block = fixed | {axis: (here + (3, 1)[way]) % 4}
                rows = self.rows
                if which == 1:
                    rows = self.row_part(row_halves[way])
                elif which == 3:
                    block[self.C] = halves[way]
                else:
                    block[self.rest[0]] = halves[way]
                half = part(wall, block, rows)
                out.append(remote(kind + 1, s, c, way, half, half, axis))
            return out

    def stage0(k):
        start(k.a1())
        start(k.load2())

    def stage1(k):
        wait(k.load2())
        wait(k.a1())
        s, c = k.slot, k.c

        def body(i):
            for way in (0, 1):
                at = (s, c, 2 * way + i // 4, i % 4)
                to = (s, c, way, 2 * way + i // 4, i % 4)
                send2[to] = (send2[to].astype(F32) + recv1[at].astype(F32)).astype(BF)

        loop(8, body)
        start(k.a2())
        start(k.load_own())

    def stage2(k):
        wait(k.load_own())
        wait(k.a2())
        s, c = k.slot, k.c

        def body(i):
            at = (i // 4, i % 4)
            total = own[(s, c) + at].astype(F32) + recv2[(s, c, 0) + at].astype(F32) + recv2[(s, c, 1) + at].astype(F32)
            sa[(s, c) + at] = total

        loop(16, body)
        far = (k.b + 2) % 4

        def pack(i):
            b1s[s, c, i] = sa[(s, c) + k.unit(far, i)].astype(BF)

        loop(4, pack)
        start(k.b1())

    def stage3(k):
        wait(k.b1())
        s, c = k.slot, k.c
        near = ((k.b + 1) % 4, (k.b + 3) % 4)

        def body(i):
            for way in (0, 1):
                b2s[s, c, way, 2 * way + i] = (sa[(s, c) + k.unit(near[way], 2 * way + i)] + b1r[s, c, 2 * way + i].astype(F32)).astype(BF)
                b2s[s, c, way, 2 - 2 * way + i] = sa[(s, c) + k.unit(near[way], 2 - 2 * way + i)].astype(BF)

        loop(2, body)
        start(k.b2())

    def stage4(k):
        wait(k.b2())
        s, c = k.slot, k.c

        def body(i):
            sb[s, c, i] = sa[(s, c) + k.unit(k.b, i)] + b2r[s, c, 0, i].astype(F32) + b2r[s, c, 1, i].astype(F32)

        loop(4, body)
        c1s[s, c] = sb[s, c, (k.c3 + 2) % 4].astype(BF)
        start(k.c1())

    def stage5(k):
        wait(k.c1())
        s, c = k.slot, k.c
        near = ((k.c3 + 1) % 4, (k.c3 + 3) % 4)
        for way in (0, 1):
            add, keep = row_halves[way], row_halves[1 - way]
            c2s[s, c, way, add] = (sb[s, c, near[way], add] + c1r[s, c, add].astype(F32)).astype(BF)
            c2s[s, c, way, keep] = sb[s, c, near[way], keep].astype(BF)
        start(k.c2())
        k.step_copies(False, start)

    def adamw(old, first, second, grad):
        first = 0.9 * first + 0.1 * grad
        second = 0.95 * second + 0.05 * grad * grad
        return old - 0.02 * (first * lax.rsqrt(second + 1e-8) + 0.1 * old), first, second

    def step_columns(k, grad):
        s, c = k.slot, k.c
        low = lax.broadcasted_iota(jnp.int32, (8, 128), 0) < 4
        odd = me % 2 == 1
        unit = []
        for ct in range(2):
            tile = slice(128 * ct, 128 * ct + 128)
            mix = grad[40 * ct + 32 : 40 * ct + 40]
            turned = pltpu.roll(mix, 4, 0)
            whole, left = [], []
            for i in range(2):
                rest = jnp.where(odd, (turned, mix)[i], (mix, turned)[i])
                rows = jnp.concatenate([grad[40 * ct + 16 * i : 40 * ct + 16 * i + 16], rest], 0)
                rows = jnp.where(odd, pltpu.roll(rows, 4, 0), rows)
                pair = gw[s, c, i, :, tile].astype(F32)
                old = jnp.where(odd, pltpu.roll(pair[16:40], 20, 0), pair[0:24])
                first, second = (jnp.where(k.layer == 1, gm[s, c, n, :, 1, tile], gm[s, c, n, :, 0, tile]) for n in (i, 2 + i))
                new, first, second = adamw(old[:20], first, second, rows[:20])
                gn[s, c, i, :, tile] = first
                gn[s, c, 2 + i, :, tile] = second
                rows24[ct, i, 0:20] = new
                new = rows24[ct, i]
                new = jnp.where(odd, pltpu.roll(new, 20, 0), new)
                whole.append(new[:16])
                turn = pltpu.roll(new[16:], 4, 0)
                left.append(jnp.where(odd, (turn, new[16:])[i], (new[16:], turn)[i]))
            unit += whole + [jnp.where(low, *left)]
        wn[s, c] = jnp.concatenate(unit, 0).astype(BF)

    def stage6(k):
        k.step_copies(False, wait)
        wait(k.c2())
        s, c = k.slot, k.c
        total = sb[s, c, k.c3] + c2r[s, c, 0].astype(F32) + c2r[s, c, 1].astype(F32)
        grad = total.astype(BF).astype(F32)

        @pl.when(k.k < 16)
        def _():
            step_columns(k, grad)

        @pl.when(k.k >= 16)
        def _():
            new, dn[s, c, 0], dn[s, c, 1] = adamw(dw[s, c].astype(F32), dm[s, c, 0], dm[s, c, 1], grad)
            wn[s, c] = new.astype(BF)

        start(k.gather(0))
        start(k.store_new())
        k.step_copies(True, start)

    def stage7(k):
        wait(k.gather(0))
        start(k.gather(1))

    def stage8(k):
        wait(k.store_new())
        k.step_copies(True, wait)
        wait(k.gather(1))
        start(k.gather(2))

    def later(n):
        def stage(k):
            wait(k.gather(n - 1))
            start(k.gather(n))
        return stage

    def stage12(k):
        wait(k.gather(5))

    stages = (stage0, stage1, stage2, stage3, stage4, stage5, stage6, stage7, stage8, later(3), later(4), later(5), stage12)

    def step(now):
        first, last = lookup(now, (0, *CUTS)), lookup(now, CUTS)
        lax.fori_loop(first, last, lambda i, _: do_item(r, g, i), None)
        before = [entered(now + 1 - k) for k in range(len(stages) + 1)]
        for number in reversed(range(len(stages))):
            if number == 0:
                lax.fori_loop(first, last, lambda i, _: item_done(r, g, i), None)

            @pl.when(before[number] > before[number + 1])
            def _():
                with jax.named_scope(f"stage{number}"):
                    for c in range(3):
                        stages[number](Chunk(c, before[number + 1]))

    loop(ENTRIES[-1] + len(stages), step)


def whole_kernel(*refs):
    (x, dy), params, moments = refs[:2], refs[2:5], refs[5:11]
    wall, moments_out, g, kept = refs[11], refs[12:18], refs[18], refs[19:21]
    scratch, n = refs[21:], COMM_SCRATCH
    comm_kernel(Refs((x, dy, *params, *kept), scratch[n:]), g, params, moments, wall, moments_out, *scratch[:n])


COMM_SCRATCH = 25


def whole_step(x, dy, params, moments):
    hbm = pl.BlockSpec(memory_space=pl.ANY)
    V, two = pltpu.VMEM, (2, 3)
    comm_scratch = [
        V(two + (4, 4, U, 128), BF), V(two + (2, 4, 4, U, 128), BF), V(two + (2, 4, 4, U, 128), BF), V(two + (4, 4, U, 128), BF),
        V(two + (4, 4, U, 128), F32),
        V(two + (4, U, 128), BF), V(two + (4, U, 128), BF), V(two + (2, 4, U, 128), BF), V(two + (2, 4, U, 128), BF), V(two + (4, U, 128), F32),
        V(two + (U, 128), BF), V(two + (U, 128), BF), V(two + (2, U, 128), BF), V(two + (2, U, 128), BF),
        V(two + (4, 20, 2, 256), F32), V(two + (2, 40, 256), BF), V(two + (4, 20, 256), F32), V((2, 2, 24, 128), F32),
        V(two + (2, U, 128), F32), V(two + (U, 128), BF), V(two + (2, U, 128), F32), V(two + (U, 128), BF),
        pltpu.SemaphoreType.DMA((12, 2, 3, 2)), pltpu.SemaphoreType.DMA((12, 2, 3, 2)), pltpu.SemaphoreType.DMA((14, 2, 3)),
    ]
    assert len(comm_scratch) == COMM_SCRATCH
    task_scratch = [
        V((TOKENS, D), BF), V((TOKENS, D), BF), V((2, D, 1024), BF), V((2, 512, D), BF),
        V((TOKENS, FF), BF), V((2, TOKENS, 1024), BF), V((TOKENS, D), F32), V((4, 4, 4, 256, 128), BF), pltpu.SemaphoreType.DMA((2, 11)),
    ]
    units = jax.ShapeDtypeStruct((4, 4, 4, ROWS, 128), BF)
    outs = pl.pallas_call(
        whole_kernel,
        out_shape=(units, *(jax.ShapeDtypeStruct((2, t.size // (2 * t.shape[-1]), t.shape[-1]), F32) for t in moments), units, jax.ShapeDtypeStruct(x.shape, BF), jax.ShapeDtypeStruct((8, TOKENS, 1024), BF)),
        in_specs=[hbm] * 11,
        out_specs=(hbm,) * 10,
        scratch_shapes=comm_scratch + task_scratch,
        compiler_params=pltpu.CompilerParams(collective_id=0, has_side_effects=True, vmem_limit_bytes=67043328),
        name="whole_step",
    )(x, dy, *params, *moments)
    return outs[0].reshape(64, ROWS, 128), outs[1:7]


UNPACK = 8


def unpack_kernel(first, second, third, *refs):
    ins, (gate, up, down), outs = refs[:6], refs[6:9], refs[9:]
    low = lax.broadcasted_iota(jnp.int32, (8, 128), 0) < 4

    def of_device(d):
        for ct in range(10):
            down[0, pl.ds(pl.multiple_of(64 * d, 64), 64), ct * 128 : ct * 128 + 128] = third[d, 64 * ct : 64 * ct + 64, :]

    loop(UNPACK, of_device)

    def slab(n):
        rows = pl.ds(pl.multiple_of(80 * n, 16), 80)
        for at, ref in ((0, first), (2048, second)):
            units = [ref[d, rows, :].astype(F32) for d in range(UNPACK)]
            for ct in range(2):
                own = [u[40 * ct : 40 * ct + 40] for u in units]
                tile = pl.ds(pl.multiple_of(n * 256 + at + ct * 128, 128), 128)
                for which, out in enumerate((gate, up)):
                    parts = []
                    for even, odd in zip(own[::2], own[1::2], strict=True):
                        left, right = even[32:40], odd[32:40]
                        if which == 0:
                            right = pltpu.roll(right, 4, 0)
                        else:
                            left = pltpu.roll(left, 4, 0)
                        parts += [even[16 * which : 16 * which + 16], jnp.where(low, left, right), odd[16 * which : 16 * which + 16]]
                    out[0, :, tile] = jnp.concatenate(parts, 0).astype(BF)

    loop(8, slab)
    for n, (t, new) in enumerate(zip(ins, outs, strict=True)):
        if n % 3 == 2:
            new[...] = t[...]
        else:
            for layer in range(2):
                new[:, layer, :] = t[layer]


def unpack(wall, moments):
    shapes = ((2, D, FF), (2, D, FF), (2, FF, D))
    blocks = 64 // UNPACK
    steps = 2 * blocks
    ins = [pl.BlockSpec((UNPACK, 640, 128), functools.partial(lambda third, l, i: (i, 3 * l + third, 0), third)) for third in range(3)]
    outs = [pl.BlockSpec((1, s[1] // blocks, s[2]), lambda l, i: (1 - l, i, 0)) for s in shapes]
    new = []
    for n, t in enumerate(moments):
        if n % 3 == 2:
            spec = pl.BlockSpec((1, t.shape[1] // blocks, t.shape[2]), lambda l, i: (l, i, 0))
            ins.append(spec)
            outs.append(spec)
            new.append(t.shape)
        else:
            cols = t.shape[2] // steps
            ins.append(pl.BlockSpec((2, t.shape[1], cols), lambda l, i: (0, 0, blocks * l + i)))
            outs.append(pl.BlockSpec((t.shape[1], 2, cols), lambda l, i: (0, 0, blocks * l + i)))
            new.append((t.shape[1], 2, t.shape[2]))
    return pl.pallas_call(
        unpack_kernel,
        grid=(2, blocks),
        out_shape=[jax.ShapeDtypeStruct(s, BF) for s in shapes] + [jax.ShapeDtypeStruct(s, F32) for s in new],
        in_specs=ins,
        out_specs=outs,
        cost_estimate=pl.CostEstimate(flops=10**6, bytes_accessed=142 * 10**6, transcendentals=0),
        name="unpack",
    )(wall, wall, wall, *moments)


def solution(mesh):
    def step(x, dy, *arrays):
        turned = [t if n % 3 == 2 else t.transpose(1, 0, 2) for n, t in enumerate(arrays[3:])]
        out = unpack(*whole_step(x[0], dy[0], arrays[:3], turned))
        return (*out[:3], *(t if n % 3 == 2 else t.transpose(1, 0, 2) for n, t in enumerate(out[3:])))

    seq, whole, rows = P(("rep", "dp")), P(), P(None, "dp", None)
    return jax.shard_map(
        step,
        mesh=mesh,
        in_specs=(seq, seq) + (whole,) * 3 + (rows,) * 6,
        out_specs=(P("rep"),) * 3 + (P("rep", "dp", None),) * 6,
        check_vma=False,
    )
```

```python
import jax
import jax.numpy as jnp
from jax import lax
from jax.experimental import pallas as pl
from jax.experimental.pallas import tpu as pltpu
from jax.sharding import PartitionSpec as P

AXES = ("x", "y", "z")
STRIDE = {"x": 16, "y": 4, "z": 1}
ORDERS = (("x", "y", "z"), ("y", "z", "x"), ("z", "x", "y"))
BF, F32 = jnp.bfloat16, jnp.float32
D, FF, TOKENS = 1280, 4096, 1024
ROWS = 3840
U, SUPER = 80, 16

MIDDLE = "DADAAEAAAAA"
CUTS = (5, 9, 14, 18, 21, 24, 25, 27, 28, 31, 32, 36, 39, 42, 44, 46, 49, 53, 56, 60, 61, 62, 63)
LAYER = 24 + len(MIDDLE) + 1
ITEMS = LAYER + 27


def entries():
    rows = {"W": 80, "D": 256, "E": 128}
    items = "PWW" * 8 + MIDDLE + "X" + "PWW" * 8 + "DDE"
    made, steps, step = 0, [], 0
    while len(steps) < SUPER:
        first, last = ((0, *CUTS)[step], CUTS[step]) if step < len(CUTS) else (ITEMS, ITEMS)
        made += sum(rows.get(item, 0) for item in items[first:last])
        if made >= 3 * U * (len(steps) + 1):
            steps.append(step)
        step += 1
    return tuple(steps)


ENTRIES = entries()


def lookup(step, values):
    out = values[0]
    for i in range(1, len(values)):
        if values[i] != values[i - 1]:
            out = out + jnp.where(step >= i, values[i] - values[i - 1], 0)
    return out


def entered(step):
    return sum(jnp.where(step > entry, 1, 0) for entry in ENTRIES)


def dot(a, b, dims):
    return lax.dot_general(a, b, (dims, ((), ())), preferred_element_type=F32)


def loop(n, body, unroll=1):
    lax.fori_loop(0, n, lambda i, _: (body(i), None)[1], None, unroll=unroll)


def start(copies):
    for copy in copies:
        copy.start()


def wait(copies):
    for copy in copies:
        copy.wait()


class Refs:
    def __init__(self, operands, buffers):
        self.x, self.dy, self.wg, self.wu, self.wd, self.h, self.kept = operands
        self.a, self.d, self.ws, self.wds, self.p, self.dgu, self.da, self.out, self.sem = buffers
        self.state = self.p.at[:, FF - D :]

    def slabs(self, i):
        slot, layer = i % 2, (i // 8 + 1) // 2 % 2
        pairs = [(self.wd.at[layer, pl.ds(pl.multiple_of(i % 8 * 512, 512), 512), :], self.wds.at[slot])]
        for n in range(4):
            cols = pl.ds(pl.multiple_of(i % 8 * 512 + n // 2 * 256, 256), 256)
            pairs.append(((self.wg, self.wu)[n % 2].at[layer, :, cols], self.ws.at[slot, :, 256 * n : 256 * n + 256]))
        return [pltpu.make_async_copy(src, dst, self.sem.at[slot, n]) for n, (src, dst) in enumerate(pairs)]

    def next_slabs(self, i):
        wait(self.slabs(i))

        @pl.when(i < 31)
        def _():
            start(self.slabs(i + 1))

    def copy(self, n, src, dst):
        return [pltpu.make_async_copy(src, dst, self.sem.at[n // 6, 5 + n % 6])]

    def load_x(self, part):
        rows = pl.ds(part * TOKENS // 4, TOKENS // 4)
        return [pltpu.make_async_copy(self.x.at[rows, :], self.p.at[rows, FF - D :], self.sem.at[part // 2, 11 + part % 2])]

    def load_dy(self):
        return self.copy(1, self.dy, self.d)

    def keep_h(self):
        return self.copy(2, self.state, self.h)

    def back_h(self):
        return self.copy(3, self.h, self.state)

    def load_a(self):
        return self.copy(4, self.x, self.a)

    def keep(self, f):
        return self.copy(5 + f % 2, self.dgu.at[f % 2], self.kept.at[f])

    def back(self, f):
        return self.copy(7 + f % 2, self.kept.at[f], self.dgu.at[f % 2])

    def put(self, g, row, n, at=0, sem=0):
        return self.copy(9 + sem, self.out.at[:, :, :, pl.ds(pl.multiple_of(at, 16), n), :], g.at[:, :, :, pl.ds(pl.multiple_of(row, 16), n), :])


def normed(h):
    wide = h.astype(F32)
    return (wide * lax.rsqrt(jnp.mean(wide * wide, -1, keepdims=True) + 1e-6)).astype(BF)


def token_blocks(size, body, unrolled=False):
    if unrolled:
        for t in range(TOKENS // size):
            body(pl.ds(t * size, size))
    else:
        loop(TOKENS // size, lambda t: body(pl.ds(pl.multiple_of(t * size, size), size)))


def add_to(ref, rows, cols, first, more):
    ref[rows, cols] = jnp.where(first, more, ref[rows, cols] + more)


PARTS = (slice(0, 1024), slice(1024, D))


def gate_and_up(r, rows, b, half):
    both = dot(r.a[rows, :], r.ws[b, :, 512 * half : 512 * half + 512], ((1,), (0,)))
    return both[:, :256], both[:, 256:]


def forward(r):
    for part in range(4):
        start(r.load_x(part))
    start(r.slabs(0) + r.load_dy())
    for part in range(4):
        wait(r.load_x(part))

        def norm(n):
            rows = pl.ds(pl.multiple_of(part * TOKENS // 4 + n * 128, 128), 128)
            r.a[rows, :] = normed(r.state[rows, :])

        loop(TOKENS // 512, norm)

    def task(f):
        r.next_slabs(f)
        b = f % 2

        def block(rows):
            p = []
            for half in range(2):
                gate, up = gate_and_up(r, rows, b, half)
                p.append((gate * jax.nn.sigmoid(gate) * up).astype(BF))
            p = jnp.concatenate(p, 1)
            for cols in PARTS:
                add_to(r.da, rows, cols, f == 0, dot(p, r.wds[b, :, cols], ((1,), (0,))))

        token_blocks(512, block, True)

    with jax.named_scope("forward"):
        loop(8, task)

    def end(rows):
        h = (r.state[rows, :].astype(F32) + r.da[rows, :].astype(BF).astype(F32)).astype(BF)
        r.state[rows, :] = h
        r.a[rows, :] = normed(h)

    token_blocks(128, end)
    start(r.keep_h())
    wait(r.load_dy())


def do_item(r, g, i):
    slot = jnp.where(i >= LAYER, 1, 0)
    at = i - LAYER * slot

    @pl.when(at < 24)
    def _():
        f, part = at // 3, at % 3

        @pl.when(part == 0)
        def _():
            @pl.when(i == 3)
            def _():
                wait(r.keep_h())

            with jax.named_scope("hidden"):
                hidden_task(r, slot, f)

        @pl.when(part > 0)
        def _():
            with jax.named_scope("columns"):
                columns_task(r, g, slot, 2 * f + part - 1)

    @pl.when(i == 24)
    def _():
        start(r.load_a())
        wait(r.keep(7))
        start(r.back(0))
        start(r.back(1))

    downs = [at for at, kind in enumerate(MIDDLE) if kind != "A"]
    t = jnp.where(slot == 1, at - 24, sum(jnp.where(at > 24 + d, 1, 0) for d in downs[:2]))
    down = (slot == 1) & (at >= 24)
    for d in downs:
        down = down | ((slot == 0) & (at == 24 + d))

    @pl.when(down & (t < 2))
    def _():
        with jax.named_scope("down512"):
            down_task(r, g, slot, t, 512)

    @pl.when(down & (t == 2))
    def _():
        with jax.named_scope("down256"):
            down_task(r, g, slot, t, 256)

    @pl.when((i >= 24) & (i < LAYER - 1) & jnp.logical_not(down))
    def _():
        with jax.named_scope("da"):
            da_task(r, at - 24 - sum(jnp.where(at > 24 + d, 1, 0) for d in downs))

    @pl.when(i == LAYER - 1)
    def _():
        with jax.named_scope("next"):
            next_layer(r)


def item_done(r, g, i):
    slot = jnp.where(i >= LAYER, 1, 0)
    at = i - LAYER * slot
    n = at // 3 * 2 + at % 3 - 1

    for m in range(3):
        @pl.when((at < 24) & (at % 3 > 0) & (n % 3 == m))
        def _():
            wait(r.put(g, 1920 * slot + 80 * n, 80, 80 * m, m))

    downs = [at for at, kind in enumerate(MIDDLE) if kind != "A"]
    for t in range(3):
        @pl.when(((slot == 0) & (at == 24 + downs[t])) | ((slot == 1) & (at == 24 + t)))
        def _():
            wait(r.put(g, 1920 * slot + 1280 + 256 * t, (256, 256, 128)[t]))


def hidden_task(r, slot, f):
    i = 8 + 16 * slot + f
    b = i % 2
    r.next_slabs(i)

    @pl.when((slot == 0) & (f > 0))
    def _():
        wait(r.keep(f - 1))

    def block(rows):
        dp = dot(r.d[rows, :], r.wds[b], ((1,), (1,))).astype(BF).astype(F32)
        for half in range(2):
            gate, up = gate_and_up(r, rows, b, half)
            sig = jax.nn.sigmoid(gate)
            silu = gate * sig
            d = dp[:, 256 * half : 256 * half + 256]
            r.p[rows, pl.ds(pl.multiple_of(f * 512 + 256 * half, 256), 256)] = (silu * up).astype(BF)
            r.dgu[b, rows, 512 * half : 512 * half + 256] = (d * up * (sig * (1 + (gate - silu)))).astype(BF)
            r.dgu[b, rows, 512 * half + 256 : 512 * half + 512] = (d * silu).astype(BF)

    token_blocks(512, block, True)

    @pl.when(slot == 0)
    def _():
        start(r.keep(f))


def columns_task(r, g, slot, n):
    b, region = n // 2 % 2, n % 3
    cols = pl.ds(pl.multiple_of(n % 2 * 512, 512), 512)

    def gradients(k):
        of_both = dot(r.a[:, k * 640 : k * 640 + 640], r.dgu[b, :, cols], ((0,), (0,)))
        low = lax.broadcasted_iota(jnp.int32, (8, 128), 0) < 4
        for pair in range(16):
            row = 40 * pair
            parts = ([], [])
            for ct in range(2):
                gate, up = (of_both[row : row + 40, at + 128 * ct : at + 128 * ct + 128] for at in (0, 256))
                gm, um = gate[16:24], up[16:24]
                parts[0].extend((gate[:16], up[:16], jnp.where(low, gm, pltpu.roll(um, 4, 0))))
                parts[1].extend((gate[24:], up[24:], jnp.where(low, pltpu.roll(gm, 4, 0), um)))
            for odd in range(2):
                at = (2 * k + pair // 8, pair // 2 % 4, pair % 2 * 2 + odd)
                r.out[at + (pl.ds(pl.multiple_of(80 * region, 16), 80),)] = jnp.concatenate(parts[odd], 0).astype(BF)

    for k in range(2):
        gradients(k)
    for m in range(3):
        @pl.when(region == m)
        def _():
            start(r.put(g, 1920 * slot + 80 * n, 80, 80 * m, m))


def da_task(r, f):
    i = 16 + f
    r.next_slabs(i)
    wait(r.back(f))
    b = i % 2

    def block(rows):
        for cols in PARTS:
            add_to(r.da, rows, cols, f == 0, dot(r.dgu[b, rows, :], r.ws[b, cols, :], ((1,), (1,))))

    token_blocks(512, block, True)

    @pl.when(f < 6)
    def _():
        start(r.back(f + 2))


def down_task(r, g, slot, t, width):
    cols = pl.ds(pl.multiple_of(t * 512, 512), width)

    for k in range(4):
        of_down = dot(r.p[:, 1024 * k : 1024 * k + 1024], r.d[:, cols], ((0,), (0,)))
        for ct in range(width // 128):
            part = of_down[:, 128 * ct : 128 * ct + 128].reshape(4, 4, 64, 128).astype(BF)
            r.out[k, :, :, 64 * ct : 64 * ct + 64, :] = part

    start(r.put(g, 1920 * slot + 1280 + 256 * t, width // 2))


def next_layer(r):
    start(r.back_h())
    wait(r.back_h())

    def block(rows):
        wide = r.state[rows, :].astype(F32)
        d = r.da[rows, :].astype(BF).astype(F32)
        scale = lax.rsqrt(jnp.mean(wide * wide, -1, keepdims=True) + 1e-6)
        along = jnp.mean(wide * d, -1, keepdims=True)
        through = (scale * d - wide * (scale * scale * scale) * along).astype(BF)
        r.d[rows, :] = (r.d[rows, :].astype(F32) + through.astype(F32)).astype(BF)

    token_blocks(128, block)
    wait(r.load_a())

    def norm(rows):
        r.a[rows, :] = normed(r.a[rows, :])

    token_blocks(128, norm)


def comm_kernel(r, g, params, moments, wall, moments_out,
                recv1, send2, recv2, own, sa, b1s, b1r, b2s, b2r, sb, c1s, c1r, c2s, c2r,
                gm, gw, gn, rows24, dm, dw, dn, wn, ssem, rsem, lsem):
    me = lax.axis_index("dp")
    pos = {"x": me // 16, "y": (me // 4) % 4, "z": me % 4}
    low = (U // 2 + 15) // 16 * 16
    halves = (pl.ds(0, 2), pl.ds(2, 2))
    row_halves = (pl.ds(0, low), pl.ds(low, U - low))

    def peer(axis, by):
        return {"dp": me + ((pos[axis] + by) % 4 - pos[axis]) * STRIDE[axis]}

    barrier = pltpu.get_barrier_semaphore()
    for axis in AXES:
        for by in (1, 3):
            pl.semaphore_signal(barrier, inc=1, device_id=peer(axis, by), device_id_type=pl.DeviceIdType.MESH)
    forward(r)
    pl.semaphore_wait(barrier, 6)

    def part(ref, fixed, rows):
        return ref.at[tuple(fixed.get(axis, slice(None)) for axis in AXES) + (rows, slice(None))]

    def remote(kind, slot, c, way, src, dst, axis):
        return pltpu.make_async_remote_copy(
            src_ref=src, dst_ref=dst, send_sem=ssem.at[kind, slot, c, way], recv_sem=rsem.at[kind, slot, c, way],
            device_id=peer(axis, (1, 3)[way]), device_id_type=pl.DeviceIdType.MESH)

    def local(kind, slot, c, src, dst):
        return pltpu.make_async_copy(src, dst, lsem.at[kind, slot, c])

    class Chunk:
        def __init__(self, c, j):
            self.c, self.slot = c, j % 2
            self.A, self.B, self.C = ORDERS[c]
            self.rest = tuple(axis for axis in AXES if axis != self.A)
            self.ib = self.rest.index(self.B)
            self.rows = pl.ds(pl.multiple_of((3 * j + c) * U, 16), U)
            self.k, self.layer = (3 * j + c) % 24, 1 - (3 * j + c) // 24
            self.a, self.b, self.c3 = (pos[axis] for axis in ORDERS[c])

        def unit(self, b, i):
            return (b, i) if self.ib == 0 else (i, b)

        def row_part(self, rows):
            return pl.ds(self.rows.start + rows.start, rows.size)

        def a1(self):
            s, c = self.slot, self.c
            return [remote(0, s, c, way, part(g, {self.A: (self.a + 2) % 4, self.rest[0]: halves[way]}, self.rows),
                           recv1.at[s, c, halves[way]], self.A) for way in (0, 1)]

        def load2(self):
            s, c = self.slot, self.c
            return [local(way, s, c, part(g, {self.A: (self.a + (1, 3)[way]) % 4}, self.rows), send2.at[s, c, way]) for way in (0, 1)]

        def load_own(self):
            return [local(2, self.slot, self.c, part(g, {self.A: self.a}, self.rows), own.at[self.slot, self.c])]

        def a2(self):
            s, c = self.slot, self.c
            return [remote(1, s, c, way, send2.at[s, c, way], recv2.at[s, c, way], self.A) for way in (0, 1)]

        def b1(self):
            s, c = self.slot, self.c
            return [remote(2, s, c, way, b1s.at[s, c, halves[way]], b1r.at[s, c, halves[way]], self.B) for way in (0, 1)]

        def b2(self):
            s, c = self.slot, self.c
            return [remote(3, s, c, way, b2s.at[s, c, way], b2r.at[s, c, way], self.B) for way in (0, 1)]

        def c1(self):
            s, c = self.slot, self.c
            return [remote(4, s, c, way, c1s.at[s, c, row_halves[way]], c1r.at[s, c, row_halves[way]], self.C) for way in (0, 1)]

        def c2(self):
            s, c = self.slot, self.c
            return [remote(5, s, c, way, c2s.at[s, c, way], c2r.at[s, c, way], self.C) for way in (0, 1)]

        def of_columns(self, out):
            s, c = self.slot, self.c
            cols = pl.ds(pl.multiple_of(self.k * 256, 256), 256)
            pairs = []
            for i in range(4):
                which = i // 2 * 3 + i % 2
                if out:
                    pairs.append((gn.at[s, c, i], moments_out[which].at[self.layer, :, cols]))
                else:
                    pairs.append((moments[which].at[:, :, cols], gm.at[s, c, i]))
            if not out:
                rows = pl.ds(pl.multiple_of(me // 2 * 40, 8), 40)
                pairs += [(params[i].at[self.layer, rows, cols], gw.at[s, c, i]) for i in range(2)]
            return [local((10 if out else 3) + i, s, c, *pair) for i, pair in enumerate(pairs)]

        def of_down(self, out, q):
            s, c = self.slot, self.c
            tile = 5 * (self.k - 16) // 4
            pairs = []
            for n, (first, rows, at) in enumerate(((16 * q, 64 - 16 * q, 0), (0, 16 + 16 * q, 64 - 16 * q))):
                cols = pl.ds(pl.multiple_of((tile + n) * 128, 128), 128)
                there, here = pl.ds(first, rows), pl.ds(at, rows)
                for i in range(2):
                    if out:
                        pairs.append((dn.at[s, c, i, here], moments_out[3 * i + 2].at[self.layer, there, cols]))
                    else:
                        pairs.append((moments[3 * i + 2].at[self.layer, there, cols], dm.at[s, c, i, here]))
                if not out:
                    mine = pl.ds(pl.multiple_of(me * 64 + first, 16), rows)
                    pairs.append((params[2].at[self.layer, mine, cols], dw.at[s, c, here]))
            return [local((10 if out else 3) + i, s, c, *pair) for i, pair in enumerate(pairs)]

        def step_copies(self, out, act):
            @pl.when(self.k < 16)
            def _():
                act(self.of_columns(out))

            for q in range(4):
                @pl.when((self.k >= 16) & (self.k % 4 == q))
                def _():
                    act(self.of_down(out, q))

        def store_new(self):
            mine = part(wall, {self.A: self.a, self.B: self.b, self.C: self.c3}, self.rows)
            return [local(9, self.slot, self.c, wn.at[self.slot, self.c], mine)]

        def gather(self, which):
            s, c = self.slot, self.c
            if which < 2:
                axis, here, fixed, kind = self.C, self.c3, {self.A: self.a, self.B: self.b}, 6
            elif which < 4:
                axis, here, fixed, kind = self.B, self.b, {self.A: self.a}, 8
            else:
                axis, here, fixed, kind = self.A, self.a, {}, 10
            if which % 2 == 0:
                block = part(wall, fixed | {axis: here}, self.rows)
                src = wn.at[s, c] if which == 0 else block
                return [remote(kind, s, c, way, src, block, axis) for way in (0, 1)]
            out = []
            for way in (0, 1):
                block = fixed | {axis: (here + (3, 1)[way]) % 4}
                rows = self.rows
                if which == 1:
                    rows = self.row_part(row_halves[way])
                elif which == 3:
                    block[self.C] = halves[way]
                else:
                    block[self.rest[0]] = halves[way]
                half = part(wall, block, rows)
                out.append(remote(kind + 1, s, c, way, half, half, axis))
            return out

    def stage0(k):
        start(k.a1())
        start(k.load2())

    def stage1(k):
        wait(k.load2())
        wait(k.a1())
        s, c = k.slot, k.c

        def body(i):
            for way in (0, 1):
                at = (s, c, 2 * way + i // 4, i % 4)
                to = (s, c, way, 2 * way + i // 4, i % 4)
                send2[to] = (send2[to].astype(F32) + recv1[at].astype(F32)).astype(BF)

        loop(8, body)
        start(k.a2())
        start(k.load_own())

    def stage2(k):
        wait(k.load_own())
        wait(k.a2())
        s, c = k.slot, k.c

        def body(i):
            at = (i // 4, i % 4)
            total = own[(s, c) + at].astype(F32) + recv2[(s, c, 0) + at].astype(F32) + recv2[(s, c, 1) + at].astype(F32)
            sa[(s, c) + at] = total

        loop(16, body)
        far = (k.b + 2) % 4

        def pack(i):
            b1s[s, c, i] = sa[(s, c) + k.unit(far, i)].astype(BF)

        loop(4, pack)
        start(k.b1())

    def stage3(k):
        wait(k.b1())
        s, c = k.slot, k.c
        near = ((k.b + 1) % 4, (k.b + 3) % 4)

        def body(i):
            for way in (0, 1):
                b2s[s, c, way, 2 * way + i] = (sa[(s, c) + k.unit(near[way], 2 * way + i)] + b1r[s, c, 2 * way + i].astype(F32)).astype(BF)
                b2s[s, c, way, 2 - 2 * way + i] = sa[(s, c) + k.unit(near[way], 2 - 2 * way + i)].astype(BF)

        loop(2, body)
        start(k.b2())

    def stage4(k):
        wait(k.b2())
        s, c = k.slot, k.c

        def body(i):
            sb[s, c, i] = sa[(s, c) + k.unit(k.b, i)] + b2r[s, c, 0, i].astype(F32) + b2r[s, c, 1, i].astype(F32)

        loop(4, body)
        c1s[s, c] = sb[s, c, (k.c3 + 2) % 4].astype(BF)
        start(k.c1())

    def stage5(k):
        wait(k.c1())
        s, c = k.slot, k.c
        near = ((k.c3 + 1) % 4, (k.c3 + 3) % 4)
        for way in (0, 1):
            add, keep = row_halves[way], row_halves[1 - way]
            c2s[s, c, way, add] = (sb[s, c, near[way], add] + c1r[s, c, add].astype(F32)).astype(BF)
            c2s[s, c, way, keep] = sb[s, c, near[way], keep].astype(BF)
        start(k.c2())
        k.step_copies(False, start)

    def adamw(old, first, second, grad):
        first = 0.9 * first + 0.1 * grad
        second = 0.95 * second + 0.05 * grad * grad
        return old - 0.02 * (first * lax.rsqrt(second + 1e-8) + 0.1 * old), first, second

    def step_columns(k, grad):
        s, c = k.slot, k.c
        low = lax.broadcasted_iota(jnp.int32, (8, 128), 0) < 4
        odd = me % 2 == 1
        unit = []
        for ct in range(2):
            tile = slice(128 * ct, 128 * ct + 128)
            mix = grad[40 * ct + 32 : 40 * ct + 40]
            turned = pltpu.roll(mix, 4, 0)
            whole, left = [], []
            for i in range(2):
                rest = jnp.where(odd, (turned, mix)[i], (mix, turned)[i])
                rows = jnp.concatenate([grad[40 * ct + 16 * i : 40 * ct + 16 * i + 16], rest], 0)
                rows = jnp.where(odd, pltpu.roll(rows, 4, 0), rows)
                pair = gw[s, c, i, :, tile].astype(F32)
                old = jnp.where(odd, pltpu.roll(pair[16:40], 20, 0), pair[0:24])
                first, second = (jnp.where(k.layer == 1, gm[s, c, n, :, 1, tile], gm[s, c, n, :, 0, tile]) for n in (i, 2 + i))
                new, first, second = adamw(old[:20], first, second, rows[:20])
                gn[s, c, i, :, tile] = first
                gn[s, c, 2 + i, :, tile] = second
                rows24[ct, i, 0:20] = new
                new = rows24[ct, i]
                new = jnp.where(odd, pltpu.roll(new, 20, 0), new)
                whole.append(new[:16])
                turn = pltpu.roll(new[16:], 4, 0)
                left.append(jnp.where(odd, (turn, new[16:])[i], (new[16:], turn)[i]))
            unit += whole + [jnp.where(low, *left)]
        wn[s, c] = jnp.concatenate(unit, 0).astype(BF)

    def stage6(k):
        k.step_copies(False, wait)
        wait(k.c2())
        s, c = k.slot, k.c
        total = sb[s, c, k.c3] + c2r[s, c, 0].astype(F32) + c2r[s, c, 1].astype(F32)
        grad = total.astype(BF).astype(F32)

        @pl.when(k.k < 16)
        def _():
            step_columns(k, grad)

        @pl.when(k.k >= 16)
        def _():
            new, dn[s, c, 0], dn[s, c, 1] = adamw(dw[s, c].astype(F32), dm[s, c, 0], dm[s, c, 1], grad)
            wn[s, c] = new.astype(BF)

        start(k.gather(0))
        start(k.store_new())
        k.step_copies(True, start)

    def stage7(k):
        wait(k.gather(0))
        start(k.gather(1))

    def stage8(k):
        wait(k.store_new())
        k.step_copies(True, wait)
        wait(k.gather(1))
        start(k.gather(2))

    def later(n):
        def stage(k):
            wait(k.gather(n - 1))
            start(k.gather(n))
        return stage

    def stage12(k):
        wait(k.gather(5))

    stages = (stage0, stage1, stage2, stage3, stage4, stage5, stage6, stage7, stage8, later(3), later(4), later(5), stage12)

    def step(now):
        first, last = lookup(now, (0, *CUTS)), lookup(now, CUTS)
        lax.fori_loop(first, last, lambda i, _: do_item(r, g, i), None)
        before = [entered(now + 1 - k) for k in range(len(stages) + 1)]
        for number in reversed(range(len(stages))):
            if number == 0:
                lax.fori_loop(first, last, lambda i, _: item_done(r, g, i), None)

            @pl.when(before[number] > before[number + 1])
            def _():
                with jax.named_scope(f"stage{number}"):
                    for c in range(3):
                        stages[number](Chunk(c, before[number + 1]))

    loop(ENTRIES[-1] + len(stages), step)


def whole_kernel(*refs):
    (x, dy), params, moments = refs[:2], refs[2:5], refs[5:11]
    wall, moments_out, g, kept = refs[11], refs[12:18], refs[18], refs[19:21]
    scratch, n = refs[21:], COMM_SCRATCH
    comm_kernel(Refs((x, dy, *params, *kept), scratch[n:]), g, params, moments, wall, moments_out, *scratch[:n])


COMM_SCRATCH = 25


def whole_step(x, dy, params, moments):
    hbm = pl.BlockSpec(memory_space=pl.ANY)
    V, two = pltpu.VMEM, (2, 3)
    comm_scratch = [
        V(two + (4, 4, U, 128), BF), V(two + (2, 4, 4, U, 128), BF), V(two + (2, 4, 4, U, 128), BF), V(two + (4, 4, U, 128), BF),
        V(two + (4, 4, U, 128), F32),
        V(two + (4, U, 128), BF), V(two + (4, U, 128), BF), V(two + (2, 4, U, 128), BF), V(two + (2, 4, U, 128), BF), V(two + (4, U, 128), F32),
        V(two + (U, 128), BF), V(two + (U, 128), BF), V(two + (2, U, 128), BF), V(two + (2, U, 128), BF),
        V(two + (4, 20, 2, 256), F32), V(two + (2, 40, 256), BF), V(two + (4, 20, 256), F32), V((2, 2, 24, 128), F32),
        V(two + (2, U, 128), F32), V(two + (U, 128), BF), V(two + (2, U, 128), F32), V(two + (U, 128), BF),
        pltpu.SemaphoreType.DMA((12, 2, 3, 2)), pltpu.SemaphoreType.DMA((12, 2, 3, 2)), pltpu.SemaphoreType.DMA((14, 2, 3)),
    ]
    assert len(comm_scratch) == COMM_SCRATCH
    task_scratch = [
        V((TOKENS, D), BF), V((TOKENS, D), BF), V((2, D, 1024), BF), V((2, 512, D), BF),
        V((TOKENS, FF), BF), V((2, TOKENS, 1024), BF), V((TOKENS, D), F32), V((4, 4, 4, 256, 128), BF), pltpu.SemaphoreType.DMA((2, 13)),
    ]
    units = jax.ShapeDtypeStruct((4, 4, 4, ROWS, 128), BF)
    outs = pl.pallas_call(
        whole_kernel,
        out_shape=(units, *(jax.ShapeDtypeStruct((2, t.size // (2 * t.shape[-1]), t.shape[-1]), F32) for t in moments), units, jax.ShapeDtypeStruct(x.shape, BF), jax.ShapeDtypeStruct((8, TOKENS, 1024), BF)),
        in_specs=[hbm] * 11,
        out_specs=(hbm,) * 10,
        scratch_shapes=comm_scratch + task_scratch,
        compiler_params=pltpu.CompilerParams(collective_id=0, has_side_effects=True, vmem_limit_bytes=67043328),
        name="whole_step",
    )(x, dy, *params, *moments)
    return outs[0].reshape(64, ROWS, 128), outs[1:7]


UNPACK, SLOTS = 4, 4


def unpack_kernel(wall, *refs):
    ins, (gate, up, down), outs = refs[:6], refs[6:9], refs[9:15]
    buf, gate_buf, up_buf, down_buf, turn, turned, plain, sem, moment_sem = refs[15:]
    low = lax.broadcasted_iota(jnp.int32, (8, 128), 0) < 4
    blocks = 64 // UNPACK

    def load(i):
        rows = pl.ds(pl.multiple_of(i // blocks * (ROWS // 2), 128), ROWS // 2)
        return [pltpu.make_async_copy(wall.at[pl.ds(i % blocks * UNPACK, UNPACK), rows, :], buf.at[i % SLOTS], sem.at[0, i % SLOTS])]

    def store(i):
        copies = []
        for n, (src, dst) in enumerate(((gate_buf, gate), (up_buf, up), (down_buf, down))):
            rows = src.shape[1]
            there = dst.at[1 - i // blocks, pl.ds(pl.multiple_of(i % blocks * rows, 16), rows), :]
            copies.append(pltpu.make_async_copy(src.at[i % SLOTS], there, sem.at[1 + n, i % SLOTS]))
        return copies

    def moments(out):
        copies = []
        for n in range(6):
            if n % 3 == 2:
                pair = (plain.at[n // 3], outs[n]) if out else (ins[n], plain.at[n // 3])
            else:
                pair = (turned.at[n // 3 * 2 + n % 3], outs[n]) if out else (ins[n], turn.at[n // 3 * 2 + n % 3])
            copies.append(pltpu.make_async_copy(*pair, moment_sem.at[n]))
        return copies

    for i in range(SLOTS - 1):
        start(load(i))
    start(moments(False))

    def block(i):
        slot = i % SLOTS
        wait(load(i))

        @pl.when(i + SLOTS - 1 < 2 * blocks)
        def _():
            start(load(i + SLOTS - 1))

        @pl.when(i >= SLOTS)
        def _():
            wait(store(i - SLOTS))

        for d in range(UNPACK):
            for ct in range(10):
                down_buf[slot, 64 * d : 64 * d + 64, ct * 128 : ct * 128 + 128] = buf[slot, d, 1280 + 64 * ct : 1344 + 64 * ct, :]

        def slab(n):
            rows = pl.ds(pl.multiple_of(80 * n, 16), 80)
            units = [buf[slot, d, rows, :].astype(F32) for d in range(UNPACK)]
            for ct in range(2):
                own = [u[40 * ct : 40 * ct + 40] for u in units]
                tile = pl.ds(pl.multiple_of(n * 256 + ct * 128, 128), 128)
                for which, out in enumerate((gate_buf, up_buf)):
                    parts = []
                    for even, odd in zip(own[::2], own[1::2], strict=True):
                        left, right = even[32:40], odd[32:40]
                        if which == 0:
                            right = pltpu.roll(right, 4, 0)
                        else:
                            left = pltpu.roll(left, 4, 0)
                        parts += [even[16 * which : 16 * which + 16], jnp.where(low, left, right), odd[16 * which : 16 * which + 16]]
                    out[slot, :, tile] = jnp.concatenate(parts, 0).astype(BF)

        loop(16, slab)
        start(store(i))

        @pl.when(i == blocks)
        def _():
            wait(moments(False))
            for n in range(4):
                for layer in range(2):
                    turned[n, :, layer, :] = turn[n, layer]
            start(moments(True))

    loop(2 * blocks, block)
    for i in range(2 * blocks - SLOTS, 2 * blocks):
        wait(store(i))
    wait(moments(True))


def unpack(wall, moments):
    shapes = ((2, D, FF), (2, D, FF), (2, FF, D))
    new = [t.shape if n % 3 == 2 else (t.shape[1], 2, t.shape[2]) for n, t in enumerate(moments)]
    hbm, V = pl.BlockSpec(memory_space=pl.ANY), pltpu.VMEM
    rows = [s[1] // 64 * UNPACK for s in shapes]
    return pl.pallas_call(
        unpack_kernel,
        out_shape=[jax.ShapeDtypeStruct(s, BF) for s in shapes] + [jax.ShapeDtypeStruct(s, F32) for s in new],
        in_specs=[hbm] * 7,
        out_specs=[hbm] * 9,
        scratch_shapes=[
            V((SLOTS, UNPACK, ROWS // 2, 128), BF), *(V((SLOTS, n, s[2]), BF) for n, s in zip(rows, shapes, strict=True)),
            V((4, *moments[0].shape), F32), V((4, *new[0]), F32), V((2, *moments[2].shape), F32),
            pltpu.SemaphoreType.DMA((4, SLOTS)), pltpu.SemaphoreType.DMA((6,)),
        ],
        compiler_params=pltpu.CompilerParams(vmem_limit_bytes=67043328),
        cost_estimate=pl.CostEstimate(flops=10**6, bytes_accessed=142 * 10**6, transcendentals=0),
        name="unpack",
    )(wall, *moments)


def solution(mesh):
    def step(x, dy, *arrays):
        turned = [t if n % 3 == 2 else t.transpose(1, 0, 2) for n, t in enumerate(arrays[3:])]
        out = unpack(*whole_step(x[0], dy[0], arrays[:3], turned))
        return (*out[:3], *(t if n % 3 == 2 else t.transpose(1, 0, 2) for n, t in enumerate(out[3:])))

    seq, whole, rows = P(("rep", "dp")), P(), P(None, "dp", None)
    return jax.shard_map(
        step,
        mesh=mesh,
        in_specs=(seq, seq) + (whole,) * 3 + (rows,) * 6,
        out_specs=(P("rep"),) * 3 + (P("rep", "dp", None),) * 6,
        check_vma=False,
    )
```

```python
import jax
import jax.numpy as jnp
from jax import lax
from jax.experimental import pallas as pl
from jax.experimental.pallas import tpu as pltpu
from jax.sharding import PartitionSpec as P

AXES = ("x", "y", "z")
STRIDE = {"x": 16, "y": 4, "z": 1}
ORDERS = (("x", "y", "z"), ("y", "z", "x"), ("z", "x", "y"))
BF, F32 = jnp.bfloat16, jnp.float32
D, FF, TOKENS = 1280, 4096, 1024
ROWS = 3840
U, SUPER = 80, 16

MIDDLE = "DADAAEAAAAA"
CUTS = (5, 9, 14, 18, 21, 24, 25, 27, 28, 31, 32, 36, 39, 42, 44, 46, 49, 53, 56, 60, 61, 62, 63)
LAYER = 24 + len(MIDDLE) + 1
ITEMS = LAYER + 27


def entries():
    rows = {"W": 80, "D": 256, "E": 128}
    items = "PWW" * 8 + MIDDLE + "X" + "PWW" * 8 + "DDE"
    made, steps, step = 0, [], 0
    while len(steps) < SUPER:
        first, last = ((0, *CUTS)[step], CUTS[step]) if step < len(CUTS) else (ITEMS, ITEMS)
        made += sum(rows.get(item, 0) for item in items[first:last])
        if made >= 3 * U * (len(steps) + 1):
            steps.append(step)
        step += 1
    return tuple(steps)


ENTRIES = entries()


def lookup(step, values):
    out = values[0]
    for i in range(1, len(values)):
        if values[i] != values[i - 1]:
            out = out + jnp.where(step >= i, values[i] - values[i - 1], 0)
    return out


def entered(step):
    return sum(jnp.where(step > entry, 1, 0) for entry in ENTRIES)


def dot(a, b, dims):
    return lax.dot_general(a, b, (dims, ((), ())), preferred_element_type=F32)


def loop(n, body, unroll=1):
    lax.fori_loop(0, n, lambda i, _: (body(i), None)[1], None, unroll=unroll)


def start(copies):
    for copy in copies:
        copy.start()


def wait(copies):
    for copy in copies:
        copy.wait()


class Refs:
    def __init__(self, operands, buffers):
        self.x, self.dy, self.wg, self.wu, self.wd, self.h, self.kept = operands
        self.a, self.d, self.ws, self.wds, self.p, self.dgu, self.da, self.out, self.sem = buffers
        self.state = self.p.at[:, FF - D :]

    def slabs(self, i):
        slot, layer = i % 2, (i // 8 + 1) // 2 % 2
        pairs = [(self.wd.at[layer, pl.ds(pl.multiple_of(i % 8 * 512, 512), 512), :], self.wds.at[slot])]
        for n in range(4):
            cols = pl.ds(pl.multiple_of(i % 8 * 512 + n // 2 * 256, 256), 256)
            pairs.append(((self.wg, self.wu)[n % 2].at[layer, :, cols], self.ws.at[slot, :, 256 * n : 256 * n + 256]))
        return [pltpu.make_async_copy(src, dst, self.sem.at[slot, n]) for n, (src, dst) in enumerate(pairs)]

    def next_slabs(self, i):
        wait(self.slabs(i))

        @pl.when(i < 31)
        def _():
            start(self.slabs(i + 1))

    def copy(self, n, src, dst):
        return [pltpu.make_async_copy(src, dst, self.sem.at[n // 6, 5 + n % 6])]

    def load_x(self, part):
        rows = pl.ds(part * TOKENS // 4, TOKENS // 4)
        return [pltpu.make_async_copy(self.x.at[rows, :], self.p.at[rows, FF - D :], self.sem.at[part // 2, 11 + part % 2])]

    def load_dy(self):
        return self.copy(1, self.dy, self.d)

    def keep_h(self):
        return self.copy(2, self.state, self.h)

    def back_h(self):
        return self.copy(3, self.h, self.state)

    def load_a(self):
        return self.copy(4, self.x, self.a)

    def keep(self, f):
        return self.copy(5 + f % 2, self.dgu.at[f % 2], self.kept.at[f])

    def back(self, f):
        return self.copy(7 + f % 2, self.kept.at[f], self.dgu.at[f % 2])

    def put(self, g, row, n, at=0, sem=0):
        return self.copy(9 + sem, self.out.at[:, :, :, pl.ds(pl.multiple_of(at, 16), n), :], g.at[:, :, :, pl.ds(pl.multiple_of(row, 16), n), :])


def normed(h):
    wide = h.astype(F32)
    return (wide * lax.rsqrt(jnp.mean(wide * wide, -1, keepdims=True) + 1e-6)).astype(BF)


def token_blocks(size, body):
    loop(TOKENS // size, lambda t: body(pl.ds(pl.multiple_of(t * size, size), size)))


def add_to(ref, rows, cols, first, more):
    ref[rows, cols] = jnp.where(first, more, ref[rows, cols] + more)


PARTS = (
    (slice(0, TOKENS), slice(0, 1024)),
    (slice(0, TOKENS // 2), slice(1024, D)),
    (slice(TOKENS // 2, TOKENS), slice(1024, D)),
)


def gate_and_up(r, rows, b, half):
    both = dot(r.a[rows, :], r.ws[b, :, 512 * half : 512 * half + 512], ((1,), (0,)))
    return both[:, :256], both[:, 256:]


def forward(r):
    for part in range(4):
        start(r.load_x(part))
    start(r.slabs(0) + r.load_dy())
    for part in range(4):
        wait(r.load_x(part))

        def norm(n):
            rows = pl.ds(pl.multiple_of(part * TOKENS // 4 + n * 128, 128), 128)
            r.a[rows, :] = normed(r.state[rows, :])

        loop(TOKENS // 512, norm)

    def task(f):
        r.next_slabs(f)
        b = f % 2

        p = []
        for half in range(2):
            gate, up = gate_and_up(r, slice(None), b, half)
            p.append((gate * jax.nn.sigmoid(gate) * up).astype(BF))
        p = jnp.concatenate(p, 1)
        for rows, cols in PARTS:
            add_to(r.da, rows, cols, f == 0, dot(p[rows], r.wds[b, :, cols], ((1,), (0,))))

    with jax.named_scope("forward"):
        loop(8, task)

    def end(rows):
        h = (r.state[rows, :].astype(F32) + r.da[rows, :].astype(BF).astype(F32)).astype(BF)
        r.state[rows, :] = h
        r.a[rows, :] = normed(h)

    token_blocks(128, end)
    start(r.keep_h())
    wait(r.load_dy())


def do_item(r, g, i):
    slot = jnp.where(i >= LAYER, 1, 0)
    at = i - LAYER * slot

    @pl.when(at < 24)
    def _():
        f, part = at // 3, at % 3

        @pl.when(part == 0)
        def _():
            @pl.when(i == 3)
            def _():
                wait(r.keep_h())

            with jax.named_scope("hidden"):
                hidden_task(r, slot, f)

        @pl.when(part > 0)
        def _():
            with jax.named_scope("columns"):
                columns_task(r, g, slot, 2 * f + part - 1)

    @pl.when(i == 24)
    def _():
        start(r.load_a())
        wait(r.keep(7))
        start(r.back(0))
        start(r.back(1))

    downs = [at for at, kind in enumerate(MIDDLE) if kind != "A"]
    t = jnp.where(slot == 1, at - 24, sum(jnp.where(at > 24 + d, 1, 0) for d in downs[:2]))
    down = (slot == 1) & (at >= 24)
    for d in downs:
        down = down | ((slot == 0) & (at == 24 + d))

    @pl.when(down & (t < 2))
    def _():
        with jax.named_scope("down512"):
            down_task(r, g, slot, t, 512)

    @pl.when(down & (t == 2))
    def _():
        with jax.named_scope("down256"):
            down_task(r, g, slot, t, 256)

    @pl.when((i >= 24) & (i < LAYER - 1) & jnp.logical_not(down))
    def _():
        with jax.named_scope("da"):
            da_task(r, at - 24 - sum(jnp.where(at > 24 + d, 1, 0) for d in downs))

    @pl.when(i == LAYER - 1)
    def _():
        with jax.named_scope("next"):
            next_layer(r)


def item_done(r, g, i):
    slot = jnp.where(i >= LAYER, 1, 0)
    at = i - LAYER * slot
    n = at // 3 * 2 + at % 3 - 1

    for m in range(3):
        @pl.when((at < 24) & (at % 3 > 0) & (n % 3 == m))
        def _():
            wait(r.put(g, 1920 * slot + 80 * n, 80, 80 * m, m))

    downs = [at for at, kind in enumerate(MIDDLE) if kind != "A"]
    for t in range(3):
        @pl.when(((slot == 0) & (at == 24 + downs[t])) | ((slot == 1) & (at == 24 + t)))
        def _():
            wait(r.put(g, 1920 * slot + 1280 + 256 * t, (256, 256, 128)[t]))


def hidden_task(r, slot, f):
    i = 8 + 16 * slot + f
    b = i % 2
    r.next_slabs(i)

    @pl.when((slot == 0) & (f > 0))
    def _():
        wait(r.keep(f - 1))

    def block(rows):
        dp = dot(r.d[rows, :], r.wds[b], ((1,), (1,))).astype(BF).astype(F32)
        for half in range(2):
            gate, up = gate_and_up(r, rows, b, half)
            sig = jax.nn.sigmoid(gate)
            silu = gate * sig
            d = dp[:, 256 * half : 256 * half + 256]
            r.p[rows, pl.ds(pl.multiple_of(f * 512 + 256 * half, 256), 256)] = (silu * up).astype(BF)
            r.dgu[b, rows, 512 * half : 512 * half + 256] = (d * up * (sig * (1 + (gate - silu)))).astype(BF)
            r.dgu[b, rows, 512 * half + 256 : 512 * half + 512] = (d * silu).astype(BF)

    block(slice(None))

    @pl.when(slot == 0)
    def _():
        start(r.keep(f))


def columns_task(r, g, slot, n):
    b, region = n // 2 % 2, n % 3
    cols = pl.ds(pl.multiple_of(n % 2 * 512, 512), 512)

    def gradients(k):
        of_both = dot(r.a[:, k * 640 : k * 640 + 640], r.dgu[b, :, cols], ((0,), (0,)))
        low = lax.broadcasted_iota(jnp.int32, (8, 128), 0) < 4
        for pair in range(16):
            row = 40 * pair
            parts = ([], [])
            for ct in range(2):
                gate, up = (of_both[row : row + 40, at + 128 * ct : at + 128 * ct + 128] for at in (0, 256))
                gm, um = gate[16:24], up[16:24]
                parts[0].extend((gate[:16], up[:16], jnp.where(low, gm, pltpu.roll(um, 4, 0))))
                parts[1].extend((gate[24:], up[24:], jnp.where(low, pltpu.roll(gm, 4, 0), um)))
            for odd in range(2):
                at = (2 * k + pair // 8, pair // 2 % 4, pair % 2 * 2 + odd)
                r.out[at + (pl.ds(pl.multiple_of(80 * region, 16), 80),)] = jnp.concatenate(parts[odd], 0).astype(BF)

    for k in range(2):
        gradients(k)
    for m in range(3):
        @pl.when(region == m)
        def _():
            start(r.put(g, 1920 * slot + 80 * n, 80, 80 * m, m))


def da_task(r, f):
    i = 16 + f
    r.next_slabs(i)
    wait(r.back(f))
    b = i % 2

    for rows, cols in PARTS:
        add_to(r.da, rows, cols, f == 0, dot(r.dgu[b, rows, :], r.ws[b, cols, :], ((1,), (1,))))

    @pl.when(f < 6)
    def _():
        start(r.back(f + 2))


def down_task(r, g, slot, t, width):
    cols = pl.ds(pl.multiple_of(t * 512, 512), width)

    for k in range(4):
        of_down = dot(r.p[:, 1024 * k : 1024 * k + 1024], r.d[:, cols], ((0,), (0,)))
        for ct in range(width // 128):
            part = of_down[:, 128 * ct : 128 * ct + 128].reshape(4, 4, 64, 128).astype(BF)
            r.out[k, :, :, 64 * ct : 64 * ct + 64, :] = part

    start(r.put(g, 1920 * slot + 1280 + 256 * t, width // 2))


def next_layer(r):
    start(r.back_h())
    wait(r.back_h())

    def block(rows):
        wide = r.state[rows, :].astype(F32)
        d = r.da[rows, :].astype(BF).astype(F32)
        scale = lax.rsqrt(jnp.mean(wide * wide, -1, keepdims=True) + 1e-6)
        along = jnp.mean(wide * d, -1, keepdims=True)
        through = (scale * d - wide * (scale * scale * scale) * along).astype(BF)
        r.d[rows, :] = (r.d[rows, :].astype(F32) + through.astype(F32)).astype(BF)

    token_blocks(128, block)
    wait(r.load_a())

    def norm(rows):
        r.a[rows, :] = normed(r.a[rows, :])

    token_blocks(128, norm)


def comm_kernel(r, g, params, moments, wall, moments_out,
                recv1, send2, recv2, own, sa, b1s, b1r, b2s, b2r, sb, c1s, c1r, c2s, c2r,
                gm, gw, gn, rows24, dm, dw, dn, wn, ssem, rsem, lsem):
    me = lax.axis_index("dp")
    pos = {"x": me // 16, "y": (me // 4) % 4, "z": me % 4}
    low = (U // 2 + 15) // 16 * 16
    halves = (pl.ds(0, 2), pl.ds(2, 2))
    row_halves = (pl.ds(0, low), pl.ds(low, U - low))

    def peer(axis, by):
        return {"dp": me + ((pos[axis] + by) % 4 - pos[axis]) * STRIDE[axis]}

    barrier = pltpu.get_barrier_semaphore()
    for axis in AXES:
        for by in (1, 3):
            pl.semaphore_signal(barrier, inc=1, device_id=peer(axis, by), device_id_type=pl.DeviceIdType.MESH)
    forward(r)
    pl.semaphore_wait(barrier, 6)

    def part(ref, fixed, rows):
        return ref.at[tuple(fixed.get(axis, slice(None)) for axis in AXES) + (rows, slice(None))]

    def remote(kind, slot, c, way, src, dst, axis):
        return pltpu.make_async_remote_copy(
            src_ref=src, dst_ref=dst, send_sem=ssem.at[kind, slot, c, way], recv_sem=rsem.at[kind, slot, c, way],
            device_id=peer(axis, (1, 3)[way]), device_id_type=pl.DeviceIdType.MESH)

    def local(kind, slot, c, src, dst):
        return pltpu.make_async_copy(src, dst, lsem.at[kind, slot, c])

    class Chunk:
        def __init__(self, c, j):
            self.c, self.slot = c, j % 2
            self.A, self.B, self.C = ORDERS[c]
            self.rest = tuple(axis for axis in AXES if axis != self.A)
            self.ib = self.rest.index(self.B)
            self.rows = pl.ds(pl.multiple_of((3 * j + c) * U, 16), U)
            self.k, self.layer = (3 * j + c) % 24, 1 - (3 * j + c) // 24
            self.a, self.b, self.c3 = (pos[axis] for axis in ORDERS[c])

        def unit(self, b, i):
            return (b, i) if self.ib == 0 else (i, b)

        def row_part(self, rows):
            return pl.ds(self.rows.start + rows.start, rows.size)

        def a1(self):
            s, c = self.slot, self.c
            return [remote(0, s, c, way, part(g, {self.A: (self.a + 2) % 4, self.rest[0]: halves[way]}, self.rows),
                           recv1.at[s, c, halves[way]], self.A) for way in (0, 1)]

        def load2(self):
            s, c = self.slot, self.c
            return [local(way, s, c, part(g, {self.A: (self.a + (1, 3)[way]) % 4}, self.rows), send2.at[s, c, way]) for way in (0, 1)]

        def load_own(self):
            return [local(2, self.slot, self.c, part(g, {self.A: self.a}, self.rows), own.at[self.slot, self.c])]

        def a2(self):
            s, c = self.slot, self.c
            return [remote(1, s, c, way, send2.at[s, c, way], recv2.at[s, c, way], self.A) for way in (0, 1)]

        def b1(self):
            s, c = self.slot, self.c
            return [remote(2, s, c, way, b1s.at[s, c, halves[way]], b1r.at[s, c, halves[way]], self.B) for way in (0, 1)]

        def b2(self):
            s, c = self.slot, self.c
            return [remote(3, s, c, way, b2s.at[s, c, way], b2r.at[s, c, way], self.B) for way in (0, 1)]

        def c1(self):
            s, c = self.slot, self.c
            return [remote(4, s, c, way, c1s.at[s, c, row_halves[way]], c1r.at[s, c, row_halves[way]], self.C) for way in (0, 1)]

        def c2(self):
            s, c = self.slot, self.c
            return [remote(5, s, c, way, c2s.at[s, c, way], c2r.at[s, c, way], self.C) for way in (0, 1)]

        def of_columns(self, out):
            s, c = self.slot, self.c
            cols = pl.ds(pl.multiple_of(self.k * 256, 256), 256)
            pairs = []
            for i in range(4):
                which = i // 2 * 3 + i % 2
                if out:
                    pairs.append((gn.at[s, c, i], moments_out[which].at[self.layer, :, cols]))
                else:
                    pairs.append((moments[which].at[:, :, cols], gm.at[s, c, i]))
            if not out:
                rows = pl.ds(pl.multiple_of(me // 2 * 40, 8), 40)
                pairs += [(params[i].at[self.layer, rows, cols], gw.at[s, c, i]) for i in range(2)]
            return [local((10 if out else 3) + i, s, c, *pair) for i, pair in enumerate(pairs)]

        def of_down(self, out, q):
            s, c = self.slot, self.c
            tile = 5 * (self.k - 16) // 4
            pairs = []
            for n, (first, rows, at) in enumerate(((16 * q, 64 - 16 * q, 0), (0, 16 + 16 * q, 64 - 16 * q))):
                cols = pl.ds(pl.multiple_of((tile + n) * 128, 128), 128)
                there, here = pl.ds(first, rows), pl.ds(at, rows)
                for i in range(2):
                    if out:
                        pairs.append((dn.at[s, c, i, here], moments_out[3 * i + 2].at[self.layer, there, cols]))
                    else:
                        pairs.append((moments[3 * i + 2].at[self.layer, there, cols], dm.at[s, c, i, here]))
                if not out:
                    mine = pl.ds(pl.multiple_of(me * 64 + first, 16), rows)
                    pairs.append((params[2].at[self.layer, mine, cols], dw.at[s, c, here]))
            return [local((10 if out else 3) + i, s, c, *pair) for i, pair in enumerate(pairs)]

        def step_copies(self, out, act):
            @pl.when(self.k < 16)
            def _():
                act(self.of_columns(out))

            for q in range(4):
                @pl.when((self.k >= 16) & (self.k % 4 == q))
                def _():
                    act(self.of_down(out, q))

        def store_new(self):
            mine = part(wall, {self.A: self.a, self.B: self.b, self.C: self.c3}, self.rows)
            return [local(9, self.slot, self.c, wn.at[self.slot, self.c], mine)]

        def gather(self, which):
            s, c = self.slot, self.c
            if which < 2:
                axis, here, fixed, kind = self.C, self.c3, {self.A: self.a, self.B: self.b}, 6
            elif which < 4:
                axis, here, fixed, kind = self.B, self.b, {self.A: self.a}, 8
            else:
                axis, here, fixed, kind = self.A, self.a, {}, 10
            if which % 2 == 0:
                block = part(wall, fixed | {axis: here}, self.rows)
                src = wn.at[s, c] if which == 0 else block
                return [remote(kind, s, c, way, src, block, axis) for way in (0, 1)]
            out = []
            for way in (0, 1):
                block = fixed | {axis: (here + (3, 1)[way]) % 4}
                rows = self.rows
                if which == 1:
                    rows = self.row_part(row_halves[way])
                elif which == 3:
                    block[self.C] = halves[way]
                else:
                    block[self.rest[0]] = halves[way]
                half = part(wall, block, rows)
                out.append(remote(kind + 1, s, c, way, half, half, axis))
            return out

    def stage0(k):
        start(k.a1())
        start(k.load2())

    def stage1(k):
        wait(k.load2())
        wait(k.a1())
        s, c = k.slot, k.c

        def body(i):
            for way in (0, 1):
                at = (s, c, 2 * way + i // 4, i % 4)
                to = (s, c, way, 2 * way + i // 4, i % 4)
                send2[to] = (send2[to].astype(F32) + recv1[at].astype(F32)).astype(BF)

        loop(8, body)
        start(k.a2())
        start(k.load_own())

    def stage2(k):
        wait(k.load_own())
        wait(k.a2())
        s, c = k.slot, k.c

        def body(i):
            at = (i // 4, i % 4)
            total = own[(s, c) + at].astype(F32) + recv2[(s, c, 0) + at].astype(F32) + recv2[(s, c, 1) + at].astype(F32)
            sa[(s, c) + at] = total

        loop(16, body)
        far = (k.b + 2) % 4

        def pack(i):
            b1s[s, c, i] = sa[(s, c) + k.unit(far, i)].astype(BF)

        loop(4, pack)
        start(k.b1())

    def stage3(k):
        wait(k.b1())
        s, c = k.slot, k.c
        near = ((k.b + 1) % 4, (k.b + 3) % 4)

        def body(i):
            for way in (0, 1):
                b2s[s, c, way, 2 * way + i] = (sa[(s, c) + k.unit(near[way], 2 * way + i)] + b1r[s, c, 2 * way + i].astype(F32)).astype(BF)
                b2s[s, c, way, 2 - 2 * way + i] = sa[(s, c) + k.unit(near[way], 2 - 2 * way + i)].astype(BF)

        loop(2, body)
        start(k.b2())

    def stage4(k):
        wait(k.b2())
        s, c = k.slot, k.c

        def body(i):
            sb[s, c, i] = sa[(s, c) + k.unit(k.b, i)] + b2r[s, c, 0, i].astype(F32) + b2r[s, c, 1, i].astype(F32)

        loop(4, body)
        c1s[s, c] = sb[s, c, (k.c3 + 2) % 4].astype(BF)
        start(k.c1())

    def stage5(k):
        wait(k.c1())
        s, c = k.slot, k.c
        near = ((k.c3 + 1) % 4, (k.c3 + 3) % 4)
        for way in (0, 1):
            add, keep = row_halves[way], row_halves[1 - way]
            c2s[s, c, way, add] = (sb[s, c, near[way], add] + c1r[s, c, add].astype(F32)).astype(BF)
            c2s[s, c, way, keep] = sb[s, c, near[way], keep].astype(BF)
        start(k.c2())
        k.step_copies(False, start)

    def adamw(old, first, second, grad):
        first = 0.9 * first + 0.1 * grad
        second = 0.95 * second + 0.05 * grad * grad
        return old - 0.02 * (first * lax.rsqrt(second + 1e-8) + 0.1 * old), first, second

    def step_columns(k, grad):
        s, c = k.slot, k.c
        low = lax.broadcasted_iota(jnp.int32, (8, 128), 0) < 4
        odd = me % 2 == 1
        unit = []
        for ct in range(2):
            tile = slice(128 * ct, 128 * ct + 128)
            mix = grad[40 * ct + 32 : 40 * ct + 40]
            turned = pltpu.roll(mix, 4, 0)
            whole, left = [], []
            for i in range(2):
                rest = jnp.where(odd, (turned, mix)[i], (mix, turned)[i])
                rows = jnp.concatenate([grad[40 * ct + 16 * i : 40 * ct + 16 * i + 16], rest], 0)
                rows = jnp.where(odd, pltpu.roll(rows, 4, 0), rows)
                pair = gw[s, c, i, :, tile].astype(F32)
                old = jnp.where(odd, pltpu.roll(pair[16:40], 20, 0), pair[0:24])
                first, second = (jnp.where(k.layer == 1, gm[s, c, n, :, 1, tile], gm[s, c, n, :, 0, tile]) for n in (i, 2 + i))
                new, first, second = adamw(old[:20], first, second, rows[:20])
                gn[s, c, i, :, tile] = first
                gn[s, c, 2 + i, :, tile] = second
                rows24[ct, i, 0:20] = new
                new = rows24[ct, i]
                new = jnp.where(odd, pltpu.roll(new, 20, 0), new)
                whole.append(new[:16])
                turn = pltpu.roll(new[16:], 4, 0)
                left.append(jnp.where(odd, (turn, new[16:])[i], (new[16:], turn)[i]))
            unit += whole + [jnp.where(low, *left)]
        wn[s, c] = jnp.concatenate(unit, 0).astype(BF)

    def stage6(k):
        k.step_copies(False, wait)
        wait(k.c2())
        s, c = k.slot, k.c
        total = sb[s, c, k.c3] + c2r[s, c, 0].astype(F32) + c2r[s, c, 1].astype(F32)
        grad = total.astype(BF).astype(F32)

        @pl.when(k.k < 16)
        def _():
            step_columns(k, grad)

        @pl.when(k.k >= 16)
        def _():
            new, dn[s, c, 0], dn[s, c, 1] = adamw(dw[s, c].astype(F32), dm[s, c, 0], dm[s, c, 1], grad)
            wn[s, c] = new.astype(BF)

        start(k.gather(0))
        start(k.store_new())
        k.step_copies(True, start)

    def stage7(k):
        wait(k.gather(0))
        start(k.gather(1))

    def stage8(k):
        wait(k.store_new())
        k.step_copies(True, wait)
        wait(k.gather(1))
        start(k.gather(2))

    def later(n):
        def stage(k):
            wait(k.gather(n - 1))
            start(k.gather(n))
        return stage

    def stage12(k):
        wait(k.gather(5))

    stages = (stage0, stage1, stage2, stage3, stage4, stage5, stage6, stage7, stage8, later(3), later(4), later(5), stage12)

    def step(now):
        first, last = lookup(now, (0, *CUTS)), lookup(now, CUTS)
        lax.fori_loop(first, last, lambda i, _: do_item(r, g, i), None)
        before = [entered(now + 1 - k) for k in range(len(stages) + 1)]
        for number in reversed(range(len(stages))):
            if number == 0:
                lax.fori_loop(first, last, lambda i, _: item_done(r, g, i), None)

            @pl.when(before[number] > before[number + 1])
            def _():
                with jax.named_scope(f"stage{number}"):
                    for c in range(3):
                        stages[number](Chunk(c, before[number + 1]))

    loop(ENTRIES[-1] + len(stages), step)


def whole_kernel(*refs):
    (x, dy), params, moments = refs[:2], refs[2:5], refs[5:11]
    wall, moments_out, g, kept = refs[11], refs[12:18], refs[18], refs[19:21]
    scratch, n = refs[21:], COMM_SCRATCH
    comm_kernel(Refs((x, dy, *params, *kept), scratch[n:]), g, params, moments, wall, moments_out, *scratch[:n])


COMM_SCRATCH = 25


def whole_step(x, dy, params, moments):
    hbm = pl.BlockSpec(memory_space=pl.ANY)
    V, two = pltpu.VMEM, (2, 3)
    comm_scratch = [
        V(two + (4, 4, U, 128), BF), V(two + (2, 4, 4, U, 128), BF), V(two + (2, 4, 4, U, 128), BF), V(two + (4, 4, U, 128), BF),
        V(two + (4, 4, U, 128), F32),
        V(two + (4, U, 128), BF), V(two + (4, U, 128), BF), V(two + (2, 4, U, 128), BF), V(two + (2, 4, U, 128), BF), V(two + (4, U, 128), F32),
        V(two + (U, 128), BF), V(two + (U, 128), BF), V(two + (2, U, 128), BF), V(two + (2, U, 128), BF),
        V(two + (4, 20, 2, 256), F32), V(two + (2, 40, 256), BF), V(two + (4, 20, 256), F32), V((2, 2, 24, 128), F32),
        V(two + (2, U, 128), F32), V(two + (U, 128), BF), V(two + (2, U, 128), F32), V(two + (U, 128), BF),
        pltpu.SemaphoreType.DMA((12, 2, 3, 2)), pltpu.SemaphoreType.DMA((12, 2, 3, 2)), pltpu.SemaphoreType.DMA((14, 2, 3)),
    ]
    assert len(comm_scratch) == COMM_SCRATCH
    task_scratch = [
        V((TOKENS, D), BF), V((TOKENS, D), BF), V((2, D, 1024), BF), V((2, 512, D), BF),
        V((TOKENS, FF), BF), V((2, TOKENS, 1024), BF), V((TOKENS, D), F32), V((4, 4, 4, 256, 128), BF), pltpu.SemaphoreType.DMA((2, 13)),
    ]
    units = jax.ShapeDtypeStruct((4, 4, 4, ROWS, 128), BF)
    outs = pl.pallas_call(
        whole_kernel,
        out_shape=(units, *(jax.ShapeDtypeStruct((2, t.size // (2 * t.shape[-1]), t.shape[-1]), F32) for t in moments), units, jax.ShapeDtypeStruct(x.shape, BF), jax.ShapeDtypeStruct((8, TOKENS, 1024), BF)),
        in_specs=[hbm] * 11,
        out_specs=(hbm,) * 10,
        scratch_shapes=comm_scratch + task_scratch,
        compiler_params=pltpu.CompilerParams(collective_id=0, has_side_effects=True, vmem_limit_bytes=67043328),
        name="whole_step",
    )(x, dy, *params, *moments)
    return outs[0].reshape(64, ROWS, 128), outs[1:7]


UNPACK, SLOTS = 4, 4


def unpack_kernel(wall, *refs):
    ins, (gate, up, down), outs = refs[:6], refs[6:9], refs[9:15]
    buf, gate_buf, up_buf, down_buf, turn, turned, plain, sem, moment_sem = refs[15:]
    low = lax.broadcasted_iota(jnp.int32, (8, 128), 0) < 4
    blocks = 64 // UNPACK

    def load(i):
        rows = pl.ds(pl.multiple_of(i // blocks * (ROWS // 2), 128), ROWS // 2)
        return [pltpu.make_async_copy(wall.at[pl.ds(i % blocks * UNPACK, UNPACK), rows, :], buf.at[i % SLOTS], sem.at[0, i % SLOTS])]

    def store(i):
        copies = []
        for n, (src, dst) in enumerate(((gate_buf, gate), (up_buf, up), (down_buf, down))):
            rows = src.shape[1]
            there = dst.at[1 - i // blocks, pl.ds(pl.multiple_of(i % blocks * rows, 16), rows), :]
            copies.append(pltpu.make_async_copy(src.at[i % SLOTS], there, sem.at[1 + n, i % SLOTS]))
        return copies

    def moments(out):
        copies = []
        for n in range(6):
            if n % 3 == 2:
                pair = (plain.at[n // 3], outs[n]) if out else (ins[n], plain.at[n // 3])
            else:
                pair = (turned.at[n // 3 * 2 + n % 3], outs[n]) if out else (ins[n], turn.at[n // 3 * 2 + n % 3])
            copies.append(pltpu.make_async_copy(*pair, moment_sem.at[n]))
        return copies

    for i in range(SLOTS - 1):
        start(load(i))
    start(moments(False))

    def block(i):
        slot = i % SLOTS
        wait(load(i))

        @pl.when(i + SLOTS - 1 < 2 * blocks)
        def _():
            start(load(i + SLOTS - 1))

        @pl.when(i >= SLOTS)
        def _():
            wait(store(i - SLOTS))

        for d in range(UNPACK):
            for ct in range(10):
                down_buf[slot, 64 * d : 64 * d + 64, ct * 128 : ct * 128 + 128] = buf[slot, d, 1280 + 64 * ct : 1344 + 64 * ct, :]

        def slab(n):
            rows = pl.ds(pl.multiple_of(80 * n, 16), 80)
            units = [buf[slot, d, rows, :].astype(F32) for d in range(UNPACK)]
            for ct in range(2):
                own = [u[40 * ct : 40 * ct + 40] for u in units]
                tile = pl.ds(pl.multiple_of(n * 256 + ct * 128, 128), 128)
                for which, out in enumerate((gate_buf, up_buf)):
                    parts = []
                    for even, odd in zip(own[::2], own[1::2], strict=True):
                        left, right = even[32:40], odd[32:40]
                        if which == 0:
                            right = pltpu.roll(right, 4, 0)
                        else:
                            left = pltpu.roll(left, 4, 0)
                        parts += [even[16 * which : 16 * which + 16], jnp.where(low, left, right), odd[16 * which : 16 * which + 16]]
                    out[slot, :, tile] = jnp.concatenate(parts, 0).astype(BF)

        loop(16, slab)
        start(store(i))

        @pl.when(i == blocks)
        def _():
            wait(moments(False))
            for n in range(4):
                for layer in range(2):
                    turned[n, :, layer, :] = turn[n, layer]
            start(moments(True))

    loop(2 * blocks, block)
    for i in range(2 * blocks - SLOTS, 2 * blocks):
        wait(store(i))
    wait(moments(True))


def unpack(wall, moments):
    shapes = ((2, D, FF), (2, D, FF), (2, FF, D))
    new = [t.shape if n % 3 == 2 else (t.shape[1], 2, t.shape[2]) for n, t in enumerate(moments)]
    hbm, V = pl.BlockSpec(memory_space=pl.ANY), pltpu.VMEM
    rows = [s[1] // 64 * UNPACK for s in shapes]
    return pl.pallas_call(
        unpack_kernel,
        out_shape=[jax.ShapeDtypeStruct(s, BF) for s in shapes] + [jax.ShapeDtypeStruct(s, F32) for s in new],
        in_specs=[hbm] * 7,
        out_specs=[hbm] * 9,
        scratch_shapes=[
            V((SLOTS, UNPACK, ROWS // 2, 128), BF), *(V((SLOTS, n, s[2]), BF) for n, s in zip(rows, shapes, strict=True)),
            V((4, *moments[0].shape), F32), V((4, *new[0]), F32), V((2, *moments[2].shape), F32),
            pltpu.SemaphoreType.DMA((4, SLOTS)), pltpu.SemaphoreType.DMA((6,)),
        ],
        compiler_params=pltpu.CompilerParams(vmem_limit_bytes=67043328),
        cost_estimate=pl.CostEstimate(flops=10**6, bytes_accessed=142 * 10**6, transcendentals=0),
        name="unpack",
    )(wall, *moments)


def solution(mesh):
    def step(x, dy, *arrays):
        turned = [t if n % 3 == 2 else t.transpose(1, 0, 2) for n, t in enumerate(arrays[3:])]
        out = unpack(*whole_step(x[0], dy[0], arrays[:3], turned))
        return (*out[:3], *(t if n % 3 == 2 else t.transpose(1, 0, 2) for n, t in enumerate(out[3:])))

    seq, whole, rows = P(("rep", "dp")), P(), P(None, "dp", None)
    return jax.shard_map(
        step,
        mesh=mesh,
        in_specs=(seq, seq) + (whole,) * 3 + (rows,) * 6,
        out_specs=(P("rep"),) * 3 + (P("rep", "dp", None),) * 6,
        check_vma=False,
    )
```

```python
import jax
import jax.numpy as jnp
from jax import lax
from jax.experimental import pallas as pl
from jax.experimental.pallas import tpu as pltpu
from jax.sharding import PartitionSpec as P

AXES = ("x", "y", "z")
STRIDE = {"x": 16, "y": 4, "z": 1}
ORDERS = (("x", "y", "z"), ("y", "z", "x"), ("z", "x", "y"))
BF, F32 = jnp.bfloat16, jnp.float32
D, FF, TOKENS = 1280, 4096, 1024
ROWS = 3840
U, SUPER = 80, 16

MIDDLE = "DADAAEAAAAA"
CUTS = (5, 9, 14, 18, 21, 24, 25, 27, 28, 31, 32, 36, 39, 42, 44, 46, 49, 53, 56, 60, 61, 62, 63)
LAYER = 24 + len(MIDDLE) + 1
ITEMS = LAYER + 27


def entries():
    rows = {"W": 80, "D": 256, "E": 128}
    items = "PWW" * 8 + MIDDLE + "X" + "PWW" * 8 + "DDE"
    made, steps, step = 0, [], 0
    while len(steps) < SUPER:
        first, last = ((0, *CUTS)[step], CUTS[step]) if step < len(CUTS) else (ITEMS, ITEMS)
        made += sum(rows.get(item, 0) for item in items[first:last])
        if made >= 3 * U * (len(steps) + 1):
            steps.append(step)
        step += 1
    return tuple(steps)


ENTRIES = entries()


def lookup(step, values):
    out = values[0]
    for i in range(1, len(values)):
        if values[i] != values[i - 1]:
            out = out + jnp.where(step >= i, values[i] - values[i - 1], 0)
    return out


def entered(step):
    return sum(jnp.where(step > entry, 1, 0) for entry in ENTRIES)


def dot(a, b, dims):
    return lax.dot_general(a, b, (dims, ((), ())), preferred_element_type=F32)


def loop(n, body, unroll=1):
    lax.fori_loop(0, n, lambda i, _: (body(i), None)[1], None, unroll=unroll)


def start(copies):
    for copy in copies:
        copy.start()


def wait(copies):
    for copy in copies:
        copy.wait()


class Refs:
    def __init__(self, operands, buffers):
        self.x, self.dy, self.wg, self.wu, self.wd, self.h, self.kept = operands
        self.a, self.d, self.ws, self.wds, self.p, self.dgu, self.da, self.out, self.sem = buffers
        self.state = self.p.at[:, FF - D :]

    def slabs(self, i):
        slot, layer = i % 2, (i // 8 + 1) // 2 % 2
        pairs = [(self.wd.at[layer, pl.ds(pl.multiple_of(i % 8 * 512, 512), 512), :], self.wds.at[slot])]
        for n in range(4):
            cols = pl.ds(pl.multiple_of(i % 8 * 512 + n // 2 * 256, 256), 256)
            pairs.append(((self.wg, self.wu)[n % 2].at[layer, :, cols], self.ws.at[slot, :, 256 * n : 256 * n + 256]))
        return [pltpu.make_async_copy(src, dst, self.sem.at[slot, n]) for n, (src, dst) in enumerate(pairs)]

    def next_slabs(self, i):
        wait(self.slabs(i))

        @pl.when(i < 31)
        def _():
            start(self.slabs(i + 1))

    def copy(self, n, src, dst):
        return [pltpu.make_async_copy(src, dst, self.sem.at[n // 6, 5 + n % 6])]

    def load_x(self, part):
        rows = pl.ds(part * TOKENS // 4, TOKENS // 4)
        return [pltpu.make_async_copy(self.x.at[rows, :], self.p.at[rows, FF - D :], self.sem.at[part // 2, 11 + part % 2])]

    def load_dy(self):
        return self.copy(1, self.dy, self.d)

    def keep_h(self):
        return self.copy(2, self.state, self.h)

    def back_h(self):
        return self.copy(3, self.h, self.state)

    def load_a(self):
        return self.copy(4, self.x, self.a)

    def keep(self, f):
        return self.copy(5 + f % 2, self.dgu.at[f % 2], self.kept.at[f])

    def back(self, f):
        return self.copy(7 + f % 2, self.kept.at[f], self.dgu.at[f % 2])

    def put(self, g, row, n, at=0, sem=0):
        return self.copy(9 + sem, self.out.at[:, :, :, pl.ds(pl.multiple_of(at, 16), n), :], g.at[:, :, :, pl.ds(pl.multiple_of(row, 16), n), :])


def normed(h):
    wide = h.astype(F32)
    return (wide * lax.rsqrt(jnp.mean(wide * wide, -1, keepdims=True) + 1e-6)).astype(BF)


def token_blocks(size, body):
    loop(TOKENS // size, lambda t: body(pl.ds(pl.multiple_of(t * size, size), size)))


def add_to(ref, rows, cols, first, more):
    ref[rows, cols] = jnp.where(first, more, ref[rows, cols] + more)


PARTS = (
    (slice(0, TOKENS), slice(0, 1024)),
    (slice(0, TOKENS // 2), slice(1024, D)),
    (slice(TOKENS // 2, TOKENS), slice(1024, D)),
)


def gate_and_up(r, rows, b, half):
    both = dot(r.a[rows, :], r.ws[b, :, 512 * half : 512 * half + 512], ((1,), (0,)))
    return both[:, :256], both[:, 256:]


def forward(r):
    for part in range(4):
        start(r.load_x(part))
    start(r.slabs(0) + r.load_dy())
    for part in range(4):
        wait(r.load_x(part))

        def norm(n):
            rows = pl.ds(pl.multiple_of(part * TOKENS // 4 + n * 128, 128), 128)
            r.a[rows, :] = normed(r.state[rows, :])

        loop(TOKENS // 512, norm)

    def task(f):
        r.next_slabs(f)
        b = f % 2

        p = []
        for half in range(2):
            gate, up = gate_and_up(r, slice(None), b, half)
            p.append((gate * jax.nn.sigmoid(gate) * up).astype(BF))
        p = jnp.concatenate(p, 1)
        for rows, cols in PARTS:
            add_to(r.da, rows, cols, f == 0, dot(p[rows], r.wds[b, :, cols], ((1,), (0,))))

    loop(8, task)

    def end(rows):
        h = (r.state[rows, :].astype(F32) + r.da[rows, :].astype(BF).astype(F32)).astype(BF)
        r.state[rows, :] = h
        r.a[rows, :] = normed(h)

    token_blocks(128, end)
    start(r.keep_h())
    wait(r.load_dy())


def do_item(r, g, i):
    slot = jnp.where(i >= LAYER, 1, 0)
    at = i - LAYER * slot

    @pl.when(at < 24)
    def _():
        f, part = at // 3, at % 3

        @pl.when(part == 0)
        def _():
            @pl.when(i == 3)
            def _():
                wait(r.keep_h())

            hidden_task(r, slot, f)

        @pl.when(part > 0)
        def _():
            columns_task(r, g, slot, 2 * f + part - 1)

    @pl.when(i == 24)
    def _():
        start(r.load_a())
        wait(r.keep(7))
        start(r.back(0))
        start(r.back(1))

    downs = [at for at, kind in enumerate(MIDDLE) if kind != "A"]
    t = jnp.where(slot == 1, at - 24, sum(jnp.where(at > 24 + d, 1, 0) for d in downs[:2]))
    down = (slot == 1) & (at >= 24)
    for d in downs:
        down = down | ((slot == 0) & (at == 24 + d))

    @pl.when(down & (t < 2))
    def _():
        down_task(r, g, slot, t, 512)

    @pl.when(down & (t == 2))
    def _():
        down_task(r, g, slot, t, 256)

    @pl.when((i >= 24) & (i < LAYER - 1) & jnp.logical_not(down))
    def _():
        da_task(r, at - 24 - sum(jnp.where(at > 24 + d, 1, 0) for d in downs))

    @pl.when(i == LAYER - 1)
    def _():
        next_layer(r)


def item_done(r, g, i):
    slot = jnp.where(i >= LAYER, 1, 0)
    at = i - LAYER * slot
    n = at // 3 * 2 + at % 3 - 1

    for m in range(3):
        @pl.when((at < 24) & (at % 3 > 0) & (n % 3 == m))
        def _():
            wait(r.put(g, 1920 * slot + 80 * n, 80, 80 * m, m))

    downs = [at for at, kind in enumerate(MIDDLE) if kind != "A"]
    for t in range(3):
        @pl.when(((slot == 0) & (at == 24 + downs[t])) | ((slot == 1) & (at == 24 + t)))
        def _():
            wait(r.put(g, 1920 * slot + 1280 + 256 * t, (256, 256, 128)[t]))


def hidden_task(r, slot, f):
    i = 8 + 16 * slot + f
    b = i % 2
    r.next_slabs(i)

    @pl.when((slot == 0) & (f > 0))
    def _():
        wait(r.keep(f - 1))

    def block(rows):
        dp = dot(r.d[rows, :], r.wds[b], ((1,), (1,))).astype(BF).astype(F32)
        for half in range(2):
            gate, up = gate_and_up(r, rows, b, half)
            sig = jax.nn.sigmoid(gate)
            silu = gate * sig
            d = dp[:, 256 * half : 256 * half + 256]
            r.p[rows, pl.ds(pl.multiple_of(f * 512 + 256 * half, 256), 256)] = (silu * up).astype(BF)
            r.dgu[b, rows, 512 * half : 512 * half + 256] = (d * up * (sig * (1 + (gate - silu)))).astype(BF)
            r.dgu[b, rows, 512 * half + 256 : 512 * half + 512] = (d * silu).astype(BF)

    block(slice(None))

    @pl.when(slot == 0)
    def _():
        start(r.keep(f))


def columns_task(r, g, slot, n):
    b, region = n // 2 % 2, n % 3
    cols = pl.ds(pl.multiple_of(n % 2 * 512, 512), 512)

    def gradients(k):
        of_both = dot(r.a[:, k * 640 : k * 640 + 640], r.dgu[b, :, cols], ((0,), (0,)))
        low = lax.broadcasted_iota(jnp.int32, (8, 128), 0) < 4
        for pair in range(16):
            row = 40 * pair
            parts = ([], [])
            for ct in range(2):
                gate, up = (of_both[row : row + 40, at + 128 * ct : at + 128 * ct + 128] for at in (0, 256))
                gm, um = gate[16:24], up[16:24]
                parts[0].extend((gate[:16], up[:16], jnp.where(low, gm, pltpu.roll(um, 4, 0))))
                parts[1].extend((gate[24:], up[24:], jnp.where(low, pltpu.roll(gm, 4, 0), um)))
            for odd in range(2):
                at = (2 * k + pair // 8, pair // 2 % 4, pair % 2 * 2 + odd)
                r.out[at + (pl.ds(pl.multiple_of(80 * region, 16), 80),)] = jnp.concatenate(parts[odd], 0).astype(BF)

    for k in range(2):
        gradients(k)
    for m in range(3):
        @pl.when(region == m)
        def _():
            start(r.put(g, 1920 * slot + 80 * n, 80, 80 * m, m))


def da_task(r, f):
    i = 16 + f
    r.next_slabs(i)
    wait(r.back(f))
    b = i % 2

    for rows, cols in PARTS:
        add_to(r.da, rows, cols, f == 0, dot(r.dgu[b, rows, :], r.ws[b, cols, :], ((1,), (1,))))

    @pl.when(f < 6)
    def _():
        start(r.back(f + 2))


def down_task(r, g, slot, t, width):
    cols = pl.ds(pl.multiple_of(t * 512, 512), width)

    for k in range(4):
        of_down = dot(r.p[:, 1024 * k : 1024 * k + 1024], r.d[:, cols], ((0,), (0,)))
        for ct in range(width // 128):
            part = of_down[:, 128 * ct : 128 * ct + 128].reshape(4, 4, 64, 128).astype(BF)
            r.out[k, :, :, 64 * ct : 64 * ct + 64, :] = part

    start(r.put(g, 1920 * slot + 1280 + 256 * t, width // 2))


def next_layer(r):
    start(r.back_h())
    wait(r.back_h())

    def block(rows):
        wide = r.state[rows, :].astype(F32)
        d = r.da[rows, :].astype(BF).astype(F32)
        scale = lax.rsqrt(jnp.mean(wide * wide, -1, keepdims=True) + 1e-6)
        along = jnp.mean(wide * d, -1, keepdims=True)
        through = (scale * d - wide * (scale * scale * scale) * along).astype(BF)
        r.d[rows, :] = (r.d[rows, :].astype(F32) + through.astype(F32)).astype(BF)

    token_blocks(128, block)
    wait(r.load_a())

    def norm(rows):
        r.a[rows, :] = normed(r.a[rows, :])

    token_blocks(128, norm)


def comm_kernel(r, g, params, moments, wall, moments_out,
                recv1, send2, recv2, own, sa, b1s, b1r, b2s, b2r, sb, c1s, c1r, c2s, c2r,
                gm, gw, gn, rows24, dm, dw, dn, wn, ssem, rsem, ssem2, rsem2, lsem):
    me = lax.axis_index("dp")
    pos = {"x": me // 16, "y": (me // 4) % 4, "z": me % 4}
    low = (U // 2 + 15) // 16 * 16
    halves = (pl.ds(0, 2), pl.ds(2, 2))
    row_halves = (pl.ds(0, low), pl.ds(low, U - low))

    def peer(axis, by):
        return {"dp": me + ((pos[axis] + by) % 4 - pos[axis]) * STRIDE[axis]}

    barrier = pltpu.get_barrier_semaphore()
    for axis in AXES:
        for by in (1, 3):
            pl.semaphore_signal(barrier, inc=1, device_id=peer(axis, by), device_id_type=pl.DeviceIdType.MESH)
    forward(r)
    pl.semaphore_wait(barrier, 6)

    def part(ref, fixed, rows):
        return ref.at[tuple(fixed.get(axis, slice(None)) for axis in AXES) + (rows, slice(None))]

    def remote(kind, slot, c, way, src, dst, axis):
        return pltpu.make_async_remote_copy(
            src_ref=src, dst_ref=dst, send_sem=ssem.at[kind, slot, c, way], recv_sem=rsem.at[kind, slot, c, way],
            device_id=peer(axis, (1, 3)[way]), device_id_type=pl.DeviceIdType.MESH)

    def local(kind, slot, c, src, dst):
        return pltpu.make_async_copy(src, dst, lsem.at[kind, slot, c])

    class Chunk:
        def __init__(self, c, j):
            self.c, self.slot, self.turn = c, j % 2, j % 3
            self.A, self.B, self.C = ORDERS[c]
            self.rest = tuple(axis for axis in AXES if axis != self.A)
            self.ib = self.rest.index(self.B)
            self.rows = pl.ds(pl.multiple_of((3 * j + c) * U, 16), U)
            self.k, self.layer = (3 * j + c) % 24, 1 - (3 * j + c) // 24
            self.a, self.b, self.c3 = (pos[axis] for axis in ORDERS[c])

        def unit(self, b, i):
            return (b, i) if self.ib == 0 else (i, b)

        def row_part(self, rows):
            return pl.ds(self.rows.start + rows.start, rows.size)

        def a1(self):
            s, c = self.slot, self.c
            return [remote(0, s, c, way, part(g, {self.A: (self.a + 2) % 4, self.rest[0]: halves[way]}, self.rows),
                           recv1.at[s, c, halves[way]], self.A) for way in (0, 1)]

        def load2(self):
            s, c = self.slot, self.c
            return [local(way, s, c, part(g, {self.A: (self.a + (1, 3)[way]) % 4}, self.rows), send2.at[s, c, way]) for way in (0, 1)]

        def load_own(self):
            return [local(2, self.slot, self.c, part(g, {self.A: self.a}, self.rows), own.at[self.slot, self.c])]

        def a2(self):
            s, c = self.slot, self.c
            return [remote(1, s, c, way, send2.at[s, c, way], recv2.at[s, c, way], self.A) for way in (0, 1)]

        def b1(self):
            s, c = self.slot, self.c
            return [remote(2, s, c, way, b1s.at[s, c, halves[way]], b1r.at[s, c, halves[way]], self.B) for way in (0, 1)]

        def b2(self):
            s, c = self.slot, self.c
            return [remote(3, s, c, way, b2s.at[s, c, way], b2r.at[s, c, way], self.B) for way in (0, 1)]

        def c1(self):
            s, c = self.slot, self.c
            return [remote(4, s, c, way, c1s.at[s, c, row_halves[way]], c1r.at[s, c, row_halves[way]], self.C) for way in (0, 1)]

        def c2(self):
            s, c = self.slot, self.c
            return [remote(5, s, c, way, c2s.at[s, c, way], c2r.at[s, c, way], self.C) for way in (0, 1)]

        def of_columns(self, out):
            s, c = self.slot, self.c
            cols = pl.ds(pl.multiple_of(self.k * 256, 256), 256)
            pairs = []
            for i in range(4):
                which = i // 2 * 3 + i % 2
                if out:
                    pairs.append((gn.at[s, c, i], moments_out[which].at[self.layer, :, cols]))
                else:
                    pairs.append((moments[which].at[:, :, cols], gm.at[s, c, i]))
            if not out:
                rows = pl.ds(pl.multiple_of(me // 2 * 40, 8), 40)
                pairs += [(params[i].at[self.layer, rows, cols], gw.at[s, c, i]) for i in range(2)]
            return [local((10 if out else 3) + i, s, c, *pair) for i, pair in enumerate(pairs)]

        def of_down(self, out, q):
            s, c = self.slot, self.c
            tile = 5 * (self.k - 16) // 4
            pairs = []
            for n, (first, rows, at) in enumerate(((16 * q, 64 - 16 * q, 0), (0, 16 + 16 * q, 64 - 16 * q))):
                cols = pl.ds(pl.multiple_of((tile + n) * 128, 128), 128)
                there, here = pl.ds(first, rows), pl.ds(at, rows)
                for i in range(2):
                    if out:
                        pairs.append((dn.at[s, c, i, here], moments_out[3 * i + 2].at[self.layer, there, cols]))
                    else:
                        pairs.append((moments[3 * i + 2].at[self.layer, there, cols], dm.at[s, c, i, here]))
                if not out:
                    mine = pl.ds(pl.multiple_of(me * 64 + first, 16), rows)
                    pairs.append((params[2].at[self.layer, mine, cols], dw.at[s, c, here]))
            return [local((10 if out else 3) + i, s, c, *pair) for i, pair in enumerate(pairs)]

        def step_copies(self, out, act):
            @pl.when(self.k < 16)
            def _():
                act(self.of_columns(out))

            for q in range(4):
                @pl.when((self.k >= 16) & (self.k % 4 == q))
                def _():
                    act(self.of_down(out, q))

        def store_new(self):
            mine = part(wall, {self.A: self.a, self.B: self.b, self.C: self.c3}, self.rows)
            return [local(9, self.slot, self.c, wn.at[self.slot, self.c], mine)]

        def gather(self, which):
            s, c = self.slot, self.c
            if which < 2:
                axis, here, fixed, kind = self.C, self.c3, {self.A: self.a, self.B: self.b}, 6
            elif which < 4:
                axis, here, fixed, kind = self.B, self.b, {self.A: self.a}, 8
            else:
                axis, here, fixed, kind = self.A, self.a, {}, 10
            if which == 4:
                blocks = [part(wall, {axis: here, self.rest[0]: halves[way]}, self.rows) for way in (0, 1)]
                return [remote(kind, s, c, way, blocks[way], blocks[way], axis) for way in (0, 1)]
            if which % 2 == 0:
                block = part(wall, fixed | {axis: here}, self.rows)
                src = wn.at[s, c] if which == 0 else block
                return [remote(kind, s, c, way, src, block, axis) for way in (0, 1)]
            out = []
            for way in (0, 1):
                block = fixed | {axis: (here + (3, 1)[way]) % 4}
                rows = self.rows
                if which == 1:
                    rows = self.row_part(row_halves[way])
                elif which == 3:
                    block[self.C] = halves[way]
                else:
                    block[self.rest[0]] = halves[way]
                half = part(wall, block, rows)
                out.append(remote(kind + 1, s, c, way, half, half, axis))
            return out

        def last_halves(self):
            out = []
            for way in (0, 1):
                half = part(wall, {self.A: self.a, self.rest[0]: halves[1 - way]}, self.rows)
                out.append(pltpu.make_async_remote_copy(
                    src_ref=half, dst_ref=half, send_sem=ssem2.at[self.turn, self.c, way], recv_sem=rsem2.at[self.turn, self.c, way],
                    device_id=peer(self.A, (1, 3)[way]), device_id_type=pl.DeviceIdType.MESH))
            return out

    def stage0(k):
        start(k.a1())
        start(k.load2())

    def stage1(k):
        wait(k.load2())
        wait(k.a1())
        s, c = k.slot, k.c

        def body(i):
            for way in (0, 1):
                at = (s, c, 2 * way + i // 4, i % 4)
                to = (s, c, way, 2 * way + i // 4, i % 4)
                send2[to] = (send2[to].astype(F32) + recv1[at].astype(F32)).astype(BF)

        loop(8, body)
        start(k.a2())
        start(k.load_own())

    def stage2(k):
        wait(k.load_own())
        wait(k.a2())
        s, c = k.slot, k.c

        def body(i):
            at = (i // 4, i % 4)
            total = own[(s, c) + at].astype(F32) + recv2[(s, c, 0) + at].astype(F32) + recv2[(s, c, 1) + at].astype(F32)
            sa[(s, c) + at] = total

        loop(16, body)
        far = (k.b + 2) % 4

        def pack(i):
            b1s[s, c, i] = sa[(s, c) + k.unit(far, i)].astype(BF)

        loop(4, pack)
        start(k.b1())

    def stage3(k):
        wait(k.b1())
        s, c = k.slot, k.c
        near = ((k.b + 1) % 4, (k.b + 3) % 4)

        def body(i):
            for way in (0, 1):
                b2s[s, c, way, 2 * way + i] = (sa[(s, c) + k.unit(near[way], 2 * way + i)] + b1r[s, c, 2 * way + i].astype(F32)).astype(BF)
                b2s[s, c, way, 2 - 2 * way + i] = sa[(s, c) + k.unit(near[way], 2 - 2 * way + i)].astype(BF)

        loop(2, body)
        start(k.b2())

    def stage4(k):
        wait(k.b2())
        s, c = k.slot, k.c

        def body(i):
            sb[s, c, i] = sa[(s, c) + k.unit(k.b, i)] + b2r[s, c, 0, i].astype(F32) + b2r[s, c, 1, i].astype(F32)

        loop(4, body)
        c1s[s, c] = sb[s, c, (k.c3 + 2) % 4].astype(BF)
        start(k.c1())

    def stage5(k):
        wait(k.c1())
        s, c = k.slot, k.c
        near = ((k.c3 + 1) % 4, (k.c3 + 3) % 4)
        for way in (0, 1):
            add, keep = row_halves[way], row_halves[1 - way]
            c2s[s, c, way, add] = (sb[s, c, near[way], add] + c1r[s, c, add].astype(F32)).astype(BF)
            c2s[s, c, way, keep] = sb[s, c, near[way], keep].astype(BF)
        start(k.c2())
        k.step_copies(False, start)

    def adamw(old, first, second, grad):
        first = 0.9 * first + 0.1 * grad
        second = 0.95 * second + 0.05 * grad * grad
        return old - 0.02 * (first * lax.rsqrt(second + 1e-8) + 0.1 * old), first, second

    def step_columns(k, grad):
        s, c = k.slot, k.c
        low = lax.broadcasted_iota(jnp.int32, (8, 128), 0) < 4
        odd = me % 2 == 1
        unit = []
        for ct in range(2):
            tile = slice(128 * ct, 128 * ct + 128)
            mix = grad[40 * ct + 32 : 40 * ct + 40]
            turned = pltpu.roll(mix, 4, 0)
            whole, left = [], []
            for i in range(2):
                rest = jnp.where(odd, (turned, mix)[i], (mix, turned)[i])
                rows = jnp.concatenate([grad[40 * ct + 16 * i : 40 * ct + 16 * i + 16], rest], 0)
                rows = jnp.where(odd, pltpu.roll(rows, 4, 0), rows)
                pair = gw[s, c, i, :, tile].astype(F32)
                old = jnp.where(odd, pltpu.roll(pair[16:40], 20, 0), pair[0:24])
                first, second = (jnp.where(k.layer == 1, gm[s, c, n, :, 1, tile], gm[s, c, n, :, 0, tile]) for n in (i, 2 + i))
                new, first, second = adamw(old[:20], first, second, rows[:20])
                gn[s, c, i, :, tile] = first
                gn[s, c, 2 + i, :, tile] = second
                rows24[ct, i, 0:20] = new
                new = rows24[ct, i]
                new = jnp.where(odd, pltpu.roll(new, 20, 0), new)
                whole.append(new[:16])
                turn = pltpu.roll(new[16:], 4, 0)
                left.append(jnp.where(odd, (turn, new[16:])[i], (new[16:], turn)[i]))
            unit += whole + [jnp.where(low, *left)]
        wn[s, c] = jnp.concatenate(unit, 0).astype(BF)

    def stage6(k):
        k.step_copies(False, wait)
        wait(k.c2())
        s, c = k.slot, k.c
        total = sb[s, c, k.c3] + c2r[s, c, 0].astype(F32) + c2r[s, c, 1].astype(F32)
        grad = total.astype(BF).astype(F32)

        @pl.when(k.k < 16)
        def _():
            step_columns(k, grad)

        @pl.when(k.k >= 16)
        def _():
            new, dn[s, c, 0], dn[s, c, 1] = adamw(dw[s, c].astype(F32), dm[s, c, 0], dm[s, c, 1], grad)
            wn[s, c] = new.astype(BF)

        start(k.gather(0))
        start(k.store_new())
        k.step_copies(True, start)

    def stage7(k):
        wait(k.gather(0))
        start(k.gather(1))

    def stage8(k):
        wait(k.store_new())
        k.step_copies(True, wait)
        wait(k.gather(1))
        start(k.gather(2))

    def later(n):
        def stage(k):
            wait(k.gather(n - 1))
            start(k.gather(n))
            if n == 4:
                start(k.last_halves())
        return stage

    def stage12(k):
        wait(k.gather(5))
        wait(k.last_halves())

    stages = (stage0, stage1, stage2, stage3, stage4, stage5, stage6, stage7, stage8, later(3), later(4), later(5), stage12)

    def step(now):
        first, last = lookup(now, (0, *CUTS)), lookup(now, CUTS)
        lax.fori_loop(first, last, lambda i, _: do_item(r, g, i), None)
        before = [entered(now + 1 - k) for k in range(len(stages) + 1)]
        for number in reversed(range(len(stages))):
            if number == 0:
                lax.fori_loop(first, last, lambda i, _: item_done(r, g, i), None)

            @pl.when(before[number] > before[number + 1])
            def _():
                for c in range(3):
                    stages[number](Chunk(c, before[number + 1]))

    loop(ENTRIES[-1] + len(stages), step)


def whole_kernel(*refs):
    (x, dy), params, moments = refs[:2], refs[2:5], refs[5:11]
    wall, moments_out, g, kept = refs[11], refs[12:18], refs[18], refs[19:21]
    scratch, n = refs[21:], COMM_SCRATCH
    comm_kernel(Refs((x, dy, *params, *kept), scratch[n:]), g, params, moments, wall, moments_out, *scratch[:n])


COMM_SCRATCH = 27


def whole_step(x, dy, params, moments):
    hbm = pl.BlockSpec(memory_space=pl.ANY)
    V, two = pltpu.VMEM, (2, 3)
    comm_scratch = [
        V(two + (4, 4, U, 128), BF), V(two + (2, 4, 4, U, 128), BF), V(two + (2, 4, 4, U, 128), BF), V(two + (4, 4, U, 128), BF),
        V(two + (4, 4, U, 128), F32),
        V(two + (4, U, 128), BF), V(two + (4, U, 128), BF), V(two + (2, 4, U, 128), BF), V(two + (2, 4, U, 128), BF), V(two + (4, U, 128), F32),
        V(two + (U, 128), BF), V(two + (U, 128), BF), V(two + (2, U, 128), BF), V(two + (2, U, 128), BF),
        V(two + (4, 20, 2, 256), F32), V(two + (2, 40, 256), BF), V(two + (4, 20, 256), F32), V((2, 2, 24, 128), F32),
        V(two + (2, U, 128), F32), V(two + (U, 128), BF), V(two + (2, U, 128), F32), V(two + (U, 128), BF),
        pltpu.SemaphoreType.DMA((12, 2, 3, 2)), pltpu.SemaphoreType.DMA((12, 2, 3, 2)), pltpu.SemaphoreType.DMA((3, 3, 2)), pltpu.SemaphoreType.DMA((3, 3, 2)), pltpu.SemaphoreType.DMA((14, 2, 3)),
    ]
    assert len(comm_scratch) == COMM_SCRATCH
    task_scratch = [
        V((TOKENS, D), BF), V((TOKENS, D), BF), V((2, D, 1024), BF), V((2, 512, D), BF),
        V((TOKENS, FF), BF), V((2, TOKENS, 1024), BF), V((TOKENS, D), F32), V((4, 4, 4, 256, 128), BF), pltpu.SemaphoreType.DMA((2, 13)),
    ]
    units = jax.ShapeDtypeStruct((4, 4, 4, ROWS, 128), BF)
    outs = pl.pallas_call(
        whole_kernel,
        out_shape=(units, *(jax.ShapeDtypeStruct((2, t.size // (2 * t.shape[-1]), t.shape[-1]), F32) for t in moments), units, jax.ShapeDtypeStruct(x.shape, BF), jax.ShapeDtypeStruct((8, TOKENS, 1024), BF)),
        in_specs=[hbm] * 11,
        out_specs=(hbm,) * 10,
        scratch_shapes=comm_scratch + task_scratch,
        compiler_params=pltpu.CompilerParams(collective_id=0, has_side_effects=True, vmem_limit_bytes=67043328),
        name="whole_step",
    )(x, dy, *params, *moments)
    return outs[0].reshape(64, ROWS, 128), outs[1:7]


UNPACK, SLOTS = 4, 4


def unpack_kernel(wall, *refs):
    ins, (gate, up, down), outs = refs[:6], refs[6:9], refs[9:15]
    buf, gate_buf, up_buf, down_buf, turn, turned, plain, sem, moment_sem = refs[15:]
    low = lax.broadcasted_iota(jnp.int32, (8, 128), 0) < 4
    blocks = 64 // UNPACK

    def load(i):
        rows = pl.ds(pl.multiple_of(i // blocks * (ROWS // 2), 128), ROWS // 2)
        return [pltpu.make_async_copy(wall.at[pl.ds(i % blocks * UNPACK, UNPACK), rows, :], buf.at[i % SLOTS], sem.at[0, i % SLOTS])]

    def store(i):
        copies = []
        for n, (src, dst) in enumerate(((gate_buf, gate), (up_buf, up), (down_buf, down))):
            rows = src.shape[1]
            there = dst.at[1 - i // blocks, pl.ds(pl.multiple_of(i % blocks * rows, 16), rows), :]
            copies.append(pltpu.make_async_copy(src.at[i % SLOTS], there, sem.at[1 + n, i % SLOTS]))
        return copies

    def moments(out):
        copies = []
        for n in range(6):
            if n % 3 == 2:
                pair = (plain.at[n // 3], outs[n]) if out else (ins[n], plain.at[n // 3])
            else:
                pair = (turned.at[n // 3 * 2 + n % 3], outs[n]) if out else (ins[n], turn.at[n // 3 * 2 + n % 3])
            copies.append(pltpu.make_async_copy(*pair, moment_sem.at[n]))
        return copies

    for i in range(SLOTS - 1):
        start(load(i))
    start(moments(False))

    def block(i):
        slot = i % SLOTS
        wait(load(i))

        @pl.when(i + SLOTS - 1 < 2 * blocks)
        def _():
            start(load(i + SLOTS - 1))

        @pl.when(i >= SLOTS)
        def _():
            wait(store(i - SLOTS))

        for d in range(UNPACK):
            for ct in range(10):
                down_buf[slot, 64 * d : 64 * d + 64, ct * 128 : ct * 128 + 128] = buf[slot, d, 1280 + 64 * ct : 1344 + 64 * ct, :]

        def slab(n):
            rows = pl.ds(pl.multiple_of(80 * n, 16), 80)
            units = [buf[slot, d, rows, :].astype(F32) for d in range(UNPACK)]
            for ct in range(2):
                own = [u[40 * ct : 40 * ct + 40] for u in units]
                tile = pl.ds(pl.multiple_of(n * 256 + ct * 128, 128), 128)
                for which, out in enumerate((gate_buf, up_buf)):
                    parts = []
                    for even, odd in zip(own[::2], own[1::2], strict=True):
                        left, right = even[32:40], odd[32:40]
                        if which == 0:
                            right = pltpu.roll(right, 4, 0)
                        else:
                            left = pltpu.roll(left, 4, 0)
                        parts += [even[16 * which : 16 * which + 16], jnp.where(low, left, right), odd[16 * which : 16 * which + 16]]
                    out[slot, :, tile] = jnp.concatenate(parts, 0).astype(BF)

        loop(16, slab)
        start(store(i))

        @pl.when(i == blocks)
        def _():
            wait(moments(False))
            for n in range(4):
                for layer in range(2):
                    turned[n, :, layer, :] = turn[n, layer]
            start(moments(True))

    loop(2 * blocks, block)
    for i in range(2 * blocks - SLOTS, 2 * blocks):
        wait(store(i))
    wait(moments(True))


def unpack(wall, moments):
    shapes = ((2, D, FF), (2, D, FF), (2, FF, D))
    new = [t.shape if n % 3 == 2 else (t.shape[1], 2, t.shape[2]) for n, t in enumerate(moments)]
    hbm, V = pl.BlockSpec(memory_space=pl.ANY), pltpu.VMEM
    rows = [s[1] // 64 * UNPACK for s in shapes]
    return pl.pallas_call(
        unpack_kernel,
        out_shape=[jax.ShapeDtypeStruct(s, BF) for s in shapes] + [jax.ShapeDtypeStruct(s, F32) for s in new],
        in_specs=[hbm] * 7,
        out_specs=[hbm] * 9,
        scratch_shapes=[
            V((SLOTS, UNPACK, ROWS // 2, 128), BF), *(V((SLOTS, n, s[2]), BF) for n, s in zip(rows, shapes, strict=True)),
            V((4, *moments[0].shape), F32), V((4, *new[0]), F32), V((2, *moments[2].shape), F32),
            pltpu.SemaphoreType.DMA((4, SLOTS)), pltpu.SemaphoreType.DMA((6,)),
        ],
        compiler_params=pltpu.CompilerParams(vmem_limit_bytes=67043328),
        cost_estimate=pl.CostEstimate(flops=10**6, bytes_accessed=142 * 10**6, transcendentals=0),
        name="unpack",
    )(wall, *moments)


def solution(mesh):
    def step(x, dy, *arrays):
        turned = [t if n % 3 == 2 else t.transpose(1, 0, 2) for n, t in enumerate(arrays[3:])]
        out = unpack(*whole_step(x[0], dy[0], arrays[:3], turned))
        return (*out[:3], *(t if n % 3 == 2 else t.transpose(1, 0, 2) for n, t in enumerate(out[3:])))

    seq, whole, rows = P(("rep", "dp")), P(), P(None, "dp", None)
    return jax.shard_map(
        step,
        mesh=mesh,
        in_specs=(seq, seq) + (whole,) * 3 + (rows,) * 6,
        out_specs=(P("rep"),) * 3 + (P("rep", "dp", None),) * 6,
        check_vma=False,
    )
```

```python
import jax
import jax.numpy as jnp
from jax import lax
from jax.experimental import pallas as pl
from jax.experimental.pallas import tpu as pltpu
from jax.sharding import PartitionSpec as P

AXES = ("x", "y", "z")
STRIDE = {"x": 16, "y": 4, "z": 1}
ORDERS = (("x", "y", "z"), ("y", "z", "x"), ("z", "x", "y"))
BF, F32 = jnp.bfloat16, jnp.float32
D, FF, TOKENS = 1280, 4096, 1024
ROWS = 3840
U, SUPER = 80, 16

MIDDLE = "DADAAEAAAAA"
CUTS = (5, 9, 14, 18, 21, 24, 25, 27, 28, 31, 32, 36, 39, 42, 44, 46, 49, 53, 56, 60, 61, 62, 63)
LAYER = 24 + len(MIDDLE) + 1
ITEMS = LAYER + 27


def entries():
    rows = {"W": 80, "D": 256, "E": 128}
    items = "PWW" * 8 + MIDDLE + "X" + "PWW" * 8 + "DDE"
    made, steps, step = 0, [], 0
    while len(steps) < SUPER:
        first, last = ((0, *CUTS)[step], CUTS[step]) if step < len(CUTS) else (ITEMS, ITEMS)
        made += sum(rows.get(item, 0) for item in items[first:last])
        if made >= 3 * U * (len(steps) + 1):
            steps.append(step)
        step += 1
    return tuple(steps)


ENTRIES = entries()


def lookup(step, values):
    out = values[0]
    for i in range(1, len(values)):
        if values[i] != values[i - 1]:
            out = out + jnp.where(step >= i, values[i] - values[i - 1], 0)
    return out


def entered(step):
    return sum(jnp.where(step > entry, 1, 0) for entry in ENTRIES)


def dot(a, b, dims):
    return lax.dot_general(a, b, (dims, ((), ())), preferred_element_type=F32)


def loop(n, body, unroll=1):
    lax.fori_loop(0, n, lambda i, _: (body(i), None)[1], None, unroll=unroll)


def start(copies):
    for copy in copies:
        copy.start()


def wait(copies):
    for copy in copies:
        copy.wait()


class Refs:
    def __init__(self, operands, buffers):
        self.x, self.dy, self.wg, self.wu, self.wd, self.h, self.kept = operands
        self.a, self.d, self.ws, self.wds, self.p, self.dgu, self.da, self.out, self.sem = buffers
        self.state = self.p.at[:, FF - D :]

    def slabs(self, i):
        slot, layer = i % 2, (i // 8 + 1) // 2 % 2
        pairs = [(self.wd.at[layer, pl.ds(pl.multiple_of(i % 8 * 512, 512), 512), :], self.wds.at[slot])]
        for n in range(4):
            cols = pl.ds(pl.multiple_of(i % 8 * 512 + n // 2 * 256, 256), 256)
            pairs.append(((self.wg, self.wu)[n % 2].at[layer, :, cols], self.ws.at[slot, :, 256 * n : 256 * n + 256]))
        return [pltpu.make_async_copy(src, dst, self.sem.at[slot, n]) for n, (src, dst) in enumerate(pairs)]

    def next_slabs(self, i):
        wait(self.slabs(i))

        @pl.when(i < 31)
        def _():
            start(self.slabs(i + 1))

    def copy(self, n, src, dst):
        return [pltpu.make_async_copy(src, dst, self.sem.at[n // 6, 5 + n % 6])]

    def load_x(self, part):
        rows = pl.ds(part * TOKENS // 4, TOKENS // 4)
        return [pltpu.make_async_copy(self.x.at[rows, :], self.p.at[rows, FF - D :], self.sem.at[part // 2, 11 + part % 2])]

    def load_dy(self):
        return self.copy(1, self.dy, self.d)

    def keep_h(self):
        return self.copy(2, self.state, self.h)

    def back_h(self):
        return self.copy(3, self.h, self.state)

    def load_a(self):
        return self.copy(4, self.x, self.a)

    def keep(self, f):
        return self.copy(5 + f % 2, self.dgu.at[f % 2], self.kept.at[f])

    def back(self, f):
        return self.copy(7 + f % 2, self.kept.at[f], self.dgu.at[f % 2])

    def put(self, g, row, n, at=0, sem=0):
        return self.copy(9 + sem, self.out.at[:, :, :, pl.ds(pl.multiple_of(at, 16), n), :], g.at[:, :, :, pl.ds(pl.multiple_of(row, 16), n), :])


def normed(h):
    wide = h.astype(F32)
    return (wide * lax.rsqrt(jnp.mean(wide * wide, -1, keepdims=True) + 1e-6)).astype(BF)


def token_blocks(size, body):
    loop(TOKENS // size, lambda t: body(pl.ds(pl.multiple_of(t * size, size), size)))


def add_to(ref, rows, cols, first, more):
    ref[rows, cols] = jnp.where(first, more, ref[rows, cols] + more)


PARTS = (
    (slice(0, TOKENS), slice(0, 1024)),
    (slice(0, TOKENS // 2), slice(1024, D)),
    (slice(TOKENS // 2, TOKENS), slice(1024, D)),
)


def gate_and_up(r, rows, b, half):
    both = dot(r.a[rows, :], r.ws[b, :, 512 * half : 512 * half + 512], ((1,), (0,)))
    return both[:, :256], both[:, 256:]


def forward(r):
    for part in range(4):
        start(r.load_x(part))
    start(r.slabs(0) + r.load_dy())
    for part in range(4):
        wait(r.load_x(part))

        def norm(n):
            rows = pl.ds(pl.multiple_of(part * TOKENS // 4 + n * 128, 128), 128)
            r.a[rows, :] = normed(r.state[rows, :])

        loop(TOKENS // 512, norm)

    def task(f):
        r.next_slabs(f)
        b = f % 2

        p = []
        for half in range(2):
            gate, up = gate_and_up(r, slice(None), b, half)
            p.append((gate * jax.nn.sigmoid(gate) * up).astype(BF))
        p = jnp.concatenate(p, 1)
        for rows, cols in PARTS:
            add_to(r.da, rows, cols, f == 0, dot(p[rows], r.wds[b, :, cols], ((1,), (0,))))

    loop(8, task)

    def end(rows):
        h = (r.state[rows, :].astype(F32) + r.da[rows, :].astype(BF).astype(F32)).astype(BF)
        r.state[rows, :] = h
        r.a[rows, :] = normed(h)

    token_blocks(128, end)
    start(r.keep_h())
    wait(r.load_dy())


def do_item(r, g, i):
    slot = jnp.where(i >= LAYER, 1, 0)
    at = i - LAYER * slot

    @pl.when(at < 24)
    def _():
        f, part = at // 3, at % 3

        @pl.when(part == 0)
        def _():
            @pl.when(i == 3)
            def _():
                wait(r.keep_h())

            hidden_task(r, slot, f)

        @pl.when(part > 0)
        def _():
            columns_task(r, g, slot, 2 * f + part - 1)

    @pl.when(i == 24)
    def _():
        start(r.load_a())
        wait(r.keep(7))
        start(r.back(0))
        start(r.back(1))

    downs = [at for at, kind in enumerate(MIDDLE) if kind != "A"]
    t = jnp.where(slot == 1, at - 24, sum(jnp.where(at > 24 + d, 1, 0) for d in downs[:2]))
    down = (slot == 1) & (at >= 24)
    for d in downs:
        down = down | ((slot == 0) & (at == 24 + d))

    @pl.when(down & (t < 2))
    def _():
        down_task(r, g, slot, t, 512)

    @pl.when(down & (t == 2))
    def _():
        down_task(r, g, slot, t, 256)

    @pl.when((i >= 24) & (i < LAYER - 1) & jnp.logical_not(down))
    def _():
        da_task(r, at - 24 - sum(jnp.where(at > 24 + d, 1, 0) for d in downs))

    @pl.when(i == LAYER - 1)
    def _():
        next_layer(r)


def item_done(r, g, i):
    slot = jnp.where(i >= LAYER, 1, 0)
    at = i - LAYER * slot
    n = at // 3 * 2 + at % 3 - 1

    for m in range(3):
        @pl.when((at < 24) & (at % 3 > 0) & (n % 3 == m))
        def _():
            wait(r.put(g, 1920 * slot + 80 * n, 80, 80 * m, m))

    downs = [at for at, kind in enumerate(MIDDLE) if kind != "A"]
    for t in range(3):
        @pl.when(((slot == 0) & (at == 24 + downs[t])) | ((slot == 1) & (at == 24 + t)))
        def _():
            wait(r.put(g, 1920 * slot + 1280 + 256 * t, (256, 256, 128)[t]))


def hidden_task(r, slot, f):
    i = 8 + 16 * slot + f
    b = i % 2
    r.next_slabs(i)

    @pl.when((slot == 0) & (f > 0))
    def _():
        wait(r.keep(f - 1))

    def block(rows):
        dp = dot(r.d[rows, :], r.wds[b], ((1,), (1,))).astype(BF).astype(F32)
        for half in range(2):
            gate, up = gate_and_up(r, rows, b, half)
            sig = jax.nn.sigmoid(gate)
            silu = gate * sig
            d = dp[:, 256 * half : 256 * half + 256]
            r.p[rows, pl.ds(pl.multiple_of(f * 512 + 256 * half, 256), 256)] = (silu * up).astype(BF)
            r.dgu[b, rows, 512 * half : 512 * half + 256] = (d * up * (sig * (1 + (gate - silu)))).astype(BF)
            r.dgu[b, rows, 512 * half + 256 : 512 * half + 512] = (d * silu).astype(BF)

    for t in range(2):
        block(slice(TOKENS // 2 * t, TOKENS // 2 * (t + 1)))

    @pl.when(slot == 0)
    def _():
        start(r.keep(f))


def columns_task(r, g, slot, n):
    b, region = n // 2 % 2, n % 3
    cols = pl.ds(pl.multiple_of(n % 2 * 512, 512), 512)

    def gradients(k):
        of_both = dot(r.a[:, k * 640 : k * 640 + 640], r.dgu[b, :, cols], ((0,), (0,)))
        low = lax.broadcasted_iota(jnp.int32, (8, 128), 0) < 4
        for pair in range(16):
            row = 40 * pair
            parts = ([], [])
            for ct in range(2):
                gate, up = (of_both[row : row + 40, at + 128 * ct : at + 128 * ct + 128] for at in (0, 256))
                gm, um = gate[16:24], up[16:24]
                parts[0].extend((gate[:16], up[:16], jnp.where(low, gm, pltpu.roll(um, 4, 0))))
                parts[1].extend((gate[24:], up[24:], jnp.where(low, pltpu.roll(gm, 4, 0), um)))
            for odd in range(2):
                at = (2 * k + pair // 8, pair // 2 % 4, pair % 2 * 2 + odd)
                r.out[at + (pl.ds(pl.multiple_of(80 * region, 16), 80),)] = jnp.concatenate(parts[odd], 0).astype(BF)

    for k in range(2):
        gradients(k)
    for m in range(3):
        @pl.when(region == m)
        def _():
            start(r.put(g, 1920 * slot + 80 * n, 80, 80 * m, m))


def da_task(r, f):
    i = 16 + f
    r.next_slabs(i)
    wait(r.back(f))
    b = i % 2

    for rows, cols in PARTS:
        add_to(r.da, rows, cols, f == 0, dot(r.dgu[b, rows, :], r.ws[b, cols, :], ((1,), (1,))))

    @pl.when(f < 6)
    def _():
        start(r.back(f + 2))


def down_task(r, g, slot, t, width):
    cols = pl.ds(pl.multiple_of(t * 512, 512), width)

    for k in range(4):
        of_down = dot(r.p[:, 1024 * k : 1024 * k + 1024], r.d[:, cols], ((0,), (0,)))
        for ct in range(width // 128):
            part = of_down[:, 128 * ct : 128 * ct + 128].reshape(4, 4, 64, 128).astype(BF)
            r.out[k, :, :, 64 * ct : 64 * ct + 64, :] = part

    start(r.put(g, 1920 * slot + 1280 + 256 * t, width // 2))


def next_layer(r):
    start(r.back_h())
    wait(r.back_h())

    def block(rows):
        wide = r.state[rows, :].astype(F32)
        d = r.da[rows, :].astype(BF).astype(F32)
        scale = lax.rsqrt(jnp.mean(wide * wide, -1, keepdims=True) + 1e-6)
        along = jnp.mean(wide * d, -1, keepdims=True)
        through = (scale * d - wide * (scale * scale * scale) * along).astype(BF)
        r.d[rows, :] = (r.d[rows, :].astype(F32) + through.astype(F32)).astype(BF)

    token_blocks(128, block)
    wait(r.load_a())

    def norm(rows):
        r.a[rows, :] = normed(r.a[rows, :])

    token_blocks(128, norm)


def comm_kernel(r, g, params, moments, wall, moments_out,
                recv1, send2, recv2, own, sa, b1s, b1r, b2s, b2r, sb, c1s, c1r, c2s, c2r,
                gm, gw, gn, rows24, dm, dw, dn, wn, ssem, rsem, ssem2, rsem2, lsem):
    me = lax.axis_index("dp")
    pos = {"x": me // 16, "y": (me // 4) % 4, "z": me % 4}
    low = (U // 2 + 15) // 16 * 16
    halves = (pl.ds(0, 2), pl.ds(2, 2))
    row_halves = (pl.ds(0, low), pl.ds(low, U - low))

    def peer(axis, by):
        return {"dp": me + ((pos[axis] + by) % 4 - pos[axis]) * STRIDE[axis]}

    barrier = pltpu.get_barrier_semaphore()
    for axis in AXES:
        for by in (1, 3):
            pl.semaphore_signal(barrier, inc=1, device_id=peer(axis, by), device_id_type=pl.DeviceIdType.MESH)
    forward(r)
    pl.semaphore_wait(barrier, 6)

    def part(ref, fixed, rows):
        return ref.at[tuple(fixed.get(axis, slice(None)) for axis in AXES) + (rows, slice(None))]

    def remote(kind, slot, c, way, src, dst, axis):
        return pltpu.make_async_remote_copy(
            src_ref=src, dst_ref=dst, send_sem=ssem.at[kind, slot, c, way], recv_sem=rsem.at[kind, slot, c, way],
            device_id=peer(axis, (1, 3)[way]), device_id_type=pl.DeviceIdType.MESH)

    def local(kind, slot, c, src, dst):
        return pltpu.make_async_copy(src, dst, lsem.at[kind, slot, c])

    class Chunk:
        def __init__(self, c, j):
            self.c, self.slot, self.turn = c, j % 2, j % 3
            self.A, self.B, self.C = ORDERS[c]
            self.rest = tuple(axis for axis in AXES if axis != self.A)
            self.ib = self.rest.index(self.B)
            self.rows = pl.ds(pl.multiple_of((3 * j + c) * U, 16), U)
            self.k, self.layer = (3 * j + c) % 24, 1 - (3 * j + c) // 24
            self.a, self.b, self.c3 = (pos[axis] for axis in ORDERS[c])

        def unit(self, b, i):
            return (b, i) if self.ib == 0 else (i, b)

        def row_part(self, rows):
            return pl.ds(self.rows.start + rows.start, rows.size)

        def a1(self):
            s, c = self.slot, self.c
            return [remote(0, s, c, way, part(g, {self.A: (self.a + 2) % 4, self.rest[0]: halves[way]}, self.rows),
                           recv1.at[s, c, halves[way]], self.A) for way in (0, 1)]

        def load2(self):
            s, c = self.slot, self.c
            return [local(way, s, c, part(g, {self.A: (self.a + (1, 3)[way]) % 4}, self.rows), send2.at[s, c, way]) for way in (0, 1)]

        def load_own(self):
            return [local(2, self.slot, self.c, part(g, {self.A: self.a}, self.rows), own.at[self.slot, self.c])]

        def a2(self):
            s, c = self.slot, self.c
            return [remote(1, s, c, way, send2.at[s, c, way], recv2.at[s, c, way], self.A) for way in (0, 1)]

        def b1(self):
            s, c = self.slot, self.c
            return [remote(2, s, c, way, b1s.at[s, c, halves[way]], b1r.at[s, c, halves[way]], self.B) for way in (0, 1)]

        def b2(self):
            s, c = self.slot, self.c
            return [remote(3, s, c, way, b2s.at[s, c, way], b2r.at[s, c, way], self.B) for way in (0, 1)]

        def c1(self):
            s, c = self.slot, self.c
            return [remote(4, s, c, way, c1s.at[s, c, row_halves[way]], c1r.at[s, c, row_halves[way]], self.C) for way in (0, 1)]

        def c2(self):
            s, c = self.slot, self.c
            return [remote(5, s, c, way, c2s.at[s, c, way], c2r.at[s, c, way], self.C) for way in (0, 1)]

        def of_columns(self, out):
            s, c = self.slot, self.c
            cols = pl.ds(pl.multiple_of(self.k * 256, 256), 256)
            pairs = []
            for i in range(4):
                which = i // 2 * 3 + i % 2
                if out:
                    pairs.append((gn.at[s, c, i], moments_out[which].at[self.layer, :, cols]))
                else:
                    pairs.append((moments[which].at[:, :, cols], gm.at[s, c, i]))
            if not out:
                rows = pl.ds(pl.multiple_of(me // 2 * 40, 8), 40)
                pairs += [(params[i].at[self.layer, rows, cols], gw.at[s, c, i]) for i in range(2)]
            return [local((10 if out else 3) + i, s, c, *pair) for i, pair in enumerate(pairs)]

        def of_down(self, out, q):
            s, c = self.slot, self.c
            tile = 5 * (self.k - 16) // 4
            pairs = []
            for n, (first, rows, at) in enumerate(((16 * q, 64 - 16 * q, 0), (0, 16 + 16 * q, 64 - 16 * q))):
                cols = pl.ds(pl.multiple_of((tile + n) * 128, 128), 128)
                there, here = pl.ds(first, rows), pl.ds(at, rows)
                for i in range(2):
                    if out:
                        pairs.append((dn.at[s, c, i, here], moments_out[3 * i + 2].at[self.layer, there, cols]))
                    else:
                        pairs.append((moments[3 * i + 2].at[self.layer, there, cols], dm.at[s, c, i, here]))
                if not out:
                    mine = pl.ds(pl.multiple_of(me * 64 + first, 16), rows)
                    pairs.append((params[2].at[self.layer, mine, cols], dw.at[s, c, here]))
            return [local((10 if out else 3) + i, s, c, *pair) for i, pair in enumerate(pairs)]

        def step_copies(self, out, act):
            @pl.when(self.k < 16)
            def _():
                act(self.of_columns(out))

            for q in range(4):
                @pl.when((self.k >= 16) & (self.k % 4 == q))
                def _():
                    act(self.of_down(out, q))

        def store_new(self):
            mine = part(wall, {self.A: self.a, self.B: self.b, self.C: self.c3}, self.rows)
            return [local(9, self.slot, self.c, wn.at[self.slot, self.c], mine)]

        def gather(self, which):
            s, c = self.slot, self.c
            if which < 2:
                axis, here, fixed, kind = self.C, self.c3, {self.A: self.a, self.B: self.b}, 6
            elif which < 4:
                axis, here, fixed, kind = self.B, self.b, {self.A: self.a}, 8
            else:
                axis, here, fixed, kind = self.A, self.a, {}, 10
            if which == 4:
                blocks = [part(wall, {axis: here, self.rest[0]: halves[way]}, self.rows) for way in (0, 1)]
                return [remote(kind, s, c, way, blocks[way], blocks[way], axis) for way in (0, 1)]
            if which % 2 == 0:
                block = part(wall, fixed | {axis: here}, self.rows)
                src = wn.at[s, c] if which == 0 else block
                return [remote(kind, s, c, way, src, block, axis) for way in (0, 1)]
            out = []
            for way in (0, 1):
                block = fixed | {axis: (here + (3, 1)[way]) % 4}
                rows = self.rows
                if which == 1:
                    rows = self.row_part(row_halves[way])
                elif which == 3:
                    block[self.C] = halves[way]
                else:
                    block[self.rest[0]] = halves[way]
                half = part(wall, block, rows)
                out.append(remote(kind + 1, s, c, way, half, half, axis))
            return out

        def last_halves(self):
            out = []
            for way in (0, 1):
                half = part(wall, {self.A: self.a, self.rest[0]: halves[1 - way]}, self.rows)
                out.append(pltpu.make_async_remote_copy(
                    src_ref=half, dst_ref=half, send_sem=ssem2.at[self.turn, self.c, way], recv_sem=rsem2.at[self.turn, self.c, way],
                    device_id=peer(self.A, (1, 3)[way]), device_id_type=pl.DeviceIdType.MESH))
            return out

    def stage0(k):
        start(k.a1())
        start(k.load2())

    def stage1(k):
        wait(k.load2())
        wait(k.a1())
        s, c = k.slot, k.c

        def body(i):
            for way in (0, 1):
                at = (s, c, 2 * way + i // 4, i % 4)
                to = (s, c, way, 2 * way + i // 4, i % 4)
                send2[to] = (send2[to].astype(F32) + recv1[at].astype(F32)).astype(BF)

        loop(8, body)
        start(k.a2())
        start(k.load_own())

    def stage2(k):
        wait(k.load_own())
        wait(k.a2())
        s, c = k.slot, k.c

        def body(i):
            at = (i // 4, i % 4)
            total = own[(s, c) + at].astype(F32) + recv2[(s, c, 0) + at].astype(F32) + recv2[(s, c, 1) + at].astype(F32)
            sa[(s, c) + at] = total

        loop(16, body)
        far = (k.b + 2) % 4

        def pack(i):
            b1s[s, c, i] = sa[(s, c) + k.unit(far, i)].astype(BF)

        loop(4, pack)
        start(k.b1())

    def stage3(k):
        wait(k.b1())
        s, c = k.slot, k.c
        near = ((k.b + 1) % 4, (k.b + 3) % 4)

        def body(i):
            for way in (0, 1):
                b2s[s, c, way, 2 * way + i] = (sa[(s, c) + k.unit(near[way], 2 * way + i)] + b1r[s, c, 2 * way + i].astype(F32)).astype(BF)
                b2s[s, c, way, 2 - 2 * way + i] = sa[(s, c) + k.unit(near[way], 2 - 2 * way + i)].astype(BF)

        loop(2, body)
        start(k.b2())

    def stage4(k):
        wait(k.b2())
        s, c = k.slot, k.c

        def body(i):
            sb[s, c, i] = sa[(s, c) + k.unit(k.b, i)] + b2r[s, c, 0, i].astype(F32) + b2r[s, c, 1, i].astype(F32)

        loop(4, body)
        c1s[s, c] = sb[s, c, (k.c3 + 2) % 4].astype(BF)
        start(k.c1())

    def stage5(k):
        wait(k.c1())
        s, c = k.slot, k.c
        near = ((k.c3 + 1) % 4, (k.c3 + 3) % 4)
        for way in (0, 1):
            add, keep = row_halves[way], row_halves[1 - way]
            c2s[s, c, way, add] = (sb[s, c, near[way], add] + c1r[s, c, add].astype(F32)).astype(BF)
            c2s[s, c, way, keep] = sb[s, c, near[way], keep].astype(BF)
        start(k.c2())
        k.step_copies(False, start)

    def adamw(old, first, second, grad):
        first = 0.9 * first + 0.1 * grad
        second = 0.95 * second + 0.05 * grad * grad
        return old - 0.02 * (first * lax.rsqrt(second + 1e-8) + 0.1 * old), first, second

    def step_columns(k, grad):
        s, c = k.slot, k.c
        low = lax.broadcasted_iota(jnp.int32, (8, 128), 0) < 4
        odd = me % 2 == 1
        unit = []
        for ct in range(2):
            tile = slice(128 * ct, 128 * ct + 128)
            mix = grad[40 * ct + 32 : 40 * ct + 40]
            turned = pltpu.roll(mix, 4, 0)
            whole, left = [], []
            for i in range(2):
                rest = jnp.where(odd, (turned, mix)[i], (mix, turned)[i])
                rows = jnp.concatenate([grad[40 * ct + 16 * i : 40 * ct + 16 * i + 16], rest], 0)
                rows = jnp.where(odd, pltpu.roll(rows, 4, 0), rows)
                pair = gw[s, c, i, :, tile].astype(F32)
                old = jnp.where(odd, pltpu.roll(pair[16:40], 20, 0), pair[0:24])
                first, second = (jnp.where(k.layer == 1, gm[s, c, n, :, 1, tile], gm[s, c, n, :, 0, tile]) for n in (i, 2 + i))
                new, first, second = adamw(old[:20], first, second, rows[:20])
                gn[s, c, i, :, tile] = first
                gn[s, c, 2 + i, :, tile] = second
                rows24[ct, i, 0:20] = new
                new = rows24[ct, i]
                new = jnp.where(odd, pltpu.roll(new, 20, 0), new)
                whole.append(new[:16])
                turn = pltpu.roll(new[16:], 4, 0)
                left.append(jnp.where(odd, (turn, new[16:])[i], (new[16:], turn)[i]))
            unit += whole + [jnp.where(low, *left)]
        wn[s, c] = jnp.concatenate(unit, 0).astype(BF)

    def stage6(k):
        k.step_copies(False, wait)
        wait(k.c2())
        s, c = k.slot, k.c
        total = sb[s, c, k.c3] + c2r[s, c, 0].astype(F32) + c2r[s, c, 1].astype(F32)
        grad = total.astype(BF).astype(F32)

        @pl.when(k.k < 16)
        def _():
            step_columns(k, grad)

        @pl.when(k.k >= 16)
        def _():
            new, dn[s, c, 0], dn[s, c, 1] = adamw(dw[s, c].astype(F32), dm[s, c, 0], dm[s, c, 1], grad)
            wn[s, c] = new.astype(BF)

        start(k.gather(0))
        start(k.store_new())
        k.step_copies(True, start)

    def stage7(k):
        wait(k.gather(0))
        start(k.gather(1))

    def stage8(k):
        wait(k.store_new())
        k.step_copies(True, wait)
        wait(k.gather(1))
        start(k.gather(2))

    def later(n):
        def stage(k):
            wait(k.gather(n - 1))
            start(k.gather(n))
            if n == 4:
                start(k.last_halves())
        return stage

    def stage12(k):
        wait(k.gather(5))
        wait(k.last_halves())

    stages = (stage0, stage1, stage2, stage3, stage4, stage5, stage6, stage7, stage8, later(3), later(4), later(5), stage12)

    def step(now):
        first, last = lookup(now, (0, *CUTS)), lookup(now, CUTS)
        lax.fori_loop(first, last, lambda i, _: do_item(r, g, i), None)
        before = [entered(now + 1 - k) for k in range(len(stages) + 1)]
        for number in reversed(range(len(stages))):
            if number == 0:
                lax.fori_loop(first, last, lambda i, _: item_done(r, g, i), None)

            @pl.when(before[number] > before[number + 1])
            def _():
                for c in range(3):
                    stages[number](Chunk(c, before[number + 1]))

    loop(ENTRIES[-1] + len(stages), step)


def whole_kernel(*refs):
    (x, dy), params, moments = refs[:2], refs[2:5], refs[5:11]
    wall, moments_out, g, kept = refs[11], refs[12:18], refs[18], refs[19:21]
    scratch, n = refs[21:], COMM_SCRATCH
    comm_kernel(Refs((x, dy, *params, *kept), scratch[n:]), g, params, moments, wall, moments_out, *scratch[:n])


COMM_SCRATCH = 27


def whole_step(x, dy, params, moments):
    hbm = pl.BlockSpec(memory_space=pl.ANY)
    V, two = pltpu.VMEM, (2, 3)
    comm_scratch = [
        V(two + (4, 4, U, 128), BF), V(two + (2, 4, 4, U, 128), BF), V(two + (2, 4, 4, U, 128), BF), V(two + (4, 4, U, 128), BF),
        V(two + (4, 4, U, 128), F32),
        V(two + (4, U, 128), BF), V(two + (4, U, 128), BF), V(two + (2, 4, U, 128), BF), V(two + (2, 4, U, 128), BF), V(two + (4, U, 128), F32),
        V(two + (U, 128), BF), V(two + (U, 128), BF), V(two + (2, U, 128), BF), V(two + (2, U, 128), BF),
        V(two + (4, 20, 2, 256), F32), V(two + (2, 40, 256), BF), V(two + (4, 20, 256), F32), V((2, 2, 24, 128), F32),
        V(two + (2, U, 128), F32), V(two + (U, 128), BF), V(two + (2, U, 128), F32), V(two + (U, 128), BF),
        pltpu.SemaphoreType.DMA((12, 2, 3, 2)), pltpu.SemaphoreType.DMA((12, 2, 3, 2)), pltpu.SemaphoreType.DMA((3, 3, 2)), pltpu.SemaphoreType.DMA((3, 3, 2)), pltpu.SemaphoreType.DMA((14, 2, 3)),
    ]
    assert len(comm_scratch) == COMM_SCRATCH
    task_scratch = [
        V((TOKENS, D), BF), V((TOKENS, D), BF), V((2, D, 1024), BF), V((2, 512, D), BF),
        V((TOKENS, FF), BF), V((2, TOKENS, 1024), BF), V((TOKENS, D), F32), V((4, 4, 4, 256, 128), BF), pltpu.SemaphoreType.DMA((2, 13)),
    ]
    units = jax.ShapeDtypeStruct((4, 4, 4, ROWS, 128), BF)
    outs = pl.pallas_call(
        whole_kernel,
        out_shape=(units, *(jax.ShapeDtypeStruct((2, t.size // (2 * t.shape[-1]), t.shape[-1]), F32) for t in moments), units, jax.ShapeDtypeStruct(x.shape, BF), jax.ShapeDtypeStruct((8, TOKENS, 1024), BF)),
        in_specs=[hbm] * 11,
        out_specs=(hbm,) * 10,
        scratch_shapes=comm_scratch + task_scratch,
        compiler_params=pltpu.CompilerParams(collective_id=0, has_side_effects=True, vmem_limit_bytes=67043328),
        name="whole_step",
    )(x, dy, *params, *moments)
    return outs[0].reshape(64, ROWS, 128), outs[1:7]


UNPACK, SLOTS = 4, 6


def unpack_kernel(wall, *refs):
    ins, (gate, up, down), outs = refs[:6], refs[6:9], refs[9:15]
    buf, gate_buf, up_buf, down_buf, turn, turned, plain, sem, moment_sem = refs[15:]
    low = lax.broadcasted_iota(jnp.int32, (8, 128), 0) < 4
    blocks = 64 // UNPACK

    def load(i):
        rows = pl.ds(pl.multiple_of(i // blocks * (ROWS // 2), 128), ROWS // 2)
        return [pltpu.make_async_copy(wall.at[pl.ds(i % blocks * UNPACK, UNPACK), rows, :], buf.at[i % SLOTS], sem.at[0, i % SLOTS])]

    def store(i):
        copies = []
        for n, (src, dst) in enumerate(((gate_buf, gate), (up_buf, up), (down_buf, down))):
            rows = src.shape[1]
            there = dst.at[1 - i // blocks, pl.ds(pl.multiple_of(i % blocks * rows, 16), rows), :]
            copies.append(pltpu.make_async_copy(src.at[i % SLOTS], there, sem.at[1 + n, i % SLOTS]))
        return copies

    def moments(out):
        copies = []
        for n in range(6):
            if n % 3 == 2:
                pair = (plain.at[n // 3], outs[n]) if out else (ins[n], plain.at[n // 3])
            else:
                pair = (turned.at[n // 3 * 2 + n % 3], outs[n]) if out else (ins[n], turn.at[n // 3 * 2 + n % 3])
            copies.append(pltpu.make_async_copy(*pair, moment_sem.at[n]))
        return copies

    for i in range(SLOTS - 1):
        start(load(i))
    start(moments(False))

    def block(i):
        slot = i % SLOTS
        wait(load(i))

        @pl.when(i + SLOTS - 1 < 2 * blocks)
        def _():
            start(load(i + SLOTS - 1))

        @pl.when(i >= SLOTS)
        def _():
            wait(store(i - SLOTS))

        for d in range(UNPACK):
            for ct in range(10):
                down_buf[slot, 64 * d : 64 * d + 64, ct * 128 : ct * 128 + 128] = buf[slot, d, 1280 + 64 * ct : 1344 + 64 * ct, :]

        def slab(n):
            rows = pl.ds(pl.multiple_of(80 * n, 16), 80)
            units = [buf[slot, d, rows, :].astype(F32) for d in range(UNPACK)]
            for ct in range(2):
                own = [u[40 * ct : 40 * ct + 40] for u in units]
                tile = pl.ds(pl.multiple_of(n * 256 + ct * 128, 128), 128)
                for which, out in enumerate((gate_buf, up_buf)):
                    parts = []
                    for even, odd in zip(own[::2], own[1::2], strict=True):
                        left, right = even[32:40], odd[32:40]
                        if which == 0:
                            right = pltpu.roll(right, 4, 0)
                        else:
                            left = pltpu.roll(left, 4, 0)
                        parts += [even[16 * which : 16 * which + 16], jnp.where(low, left, right), odd[16 * which : 16 * which + 16]]
                    out[slot, :, tile] = jnp.concatenate(parts, 0).astype(BF)

        loop(16, slab)
        start(store(i))

        @pl.when(i == blocks)
        def _():
            wait(moments(False))
            for n in range(4):
                for layer in range(2):
                    turned[n, :, layer, :] = turn[n, layer]
            start(moments(True))

    loop(2 * blocks, block)
    for i in range(2 * blocks - SLOTS, 2 * blocks):
        wait(store(i))
    wait(moments(True))


def unpack(wall, moments):
    shapes = ((2, D, FF), (2, D, FF), (2, FF, D))
    new = [t.shape if n % 3 == 2 else (t.shape[1], 2, t.shape[2]) for n, t in enumerate(moments)]
    hbm, V = pl.BlockSpec(memory_space=pl.ANY), pltpu.VMEM
    rows = [s[1] // 64 * UNPACK for s in shapes]
    return pl.pallas_call(
        unpack_kernel,
        out_shape=[jax.ShapeDtypeStruct(s, BF) for s in shapes] + [jax.ShapeDtypeStruct(s, F32) for s in new],
        in_specs=[hbm] * 7,
        out_specs=[hbm] * 9,
        scratch_shapes=[
            V((SLOTS, UNPACK, ROWS // 2, 128), BF), *(V((SLOTS, n, s[2]), BF) for n, s in zip(rows, shapes, strict=True)),
            V((4, *moments[0].shape), F32), V((4, *new[0]), F32), V((2, *moments[2].shape), F32),
            pltpu.SemaphoreType.DMA((4, SLOTS)), pltpu.SemaphoreType.DMA((6,)),
        ],
        compiler_params=pltpu.CompilerParams(vmem_limit_bytes=67043328),
        cost_estimate=pl.CostEstimate(flops=10**6, bytes_accessed=142 * 10**6, transcendentals=0),
        name="unpack",
    )(wall, *moments)


def solution(mesh):
    def step(x, dy, *arrays):
        turned = [t if n % 3 == 2 else t.transpose(1, 0, 2) for n, t in enumerate(arrays[3:])]
        out = unpack(*whole_step(x[0], dy[0], arrays[:3], turned))
        return (*out[:3], *(t if n % 3 == 2 else t.transpose(1, 0, 2) for n, t in enumerate(out[3:])))

    seq, whole, rows = P(("rep", "dp")), P(), P(None, "dp", None)
    return jax.shard_map(
        step,
        mesh=mesh,
        in_specs=(seq, seq) + (whole,) * 3 + (rows,) * 6,
        out_specs=(P("rep"),) * 3 + (P("rep", "dp", None),) * 6,
        check_vma=False,
    )
```
